32 devices in a mesh: replica: 8 (over z, x), shard: 4 (over y, core).
Axes of the slice: x: 2, y: 2, z: 4, core: 2. Of those that a mesh axis runs over, the one named last changes fastest.
Arguments:
- tokens_in: bfloat16 [32, 256, 2048], P(('replica', 'shard')), may hold values from -6 to 6
- cotangent: bfloat16 [32, 256, 2048], P(('replica', 'shard')), may hold values from -6 to 6
- segment_ids: int32 [32, 256], P(('replica', 'shard')), may hold values from 0 to 3, never falling along the last dimension, each value on 1 to 128 neighbouring positions
- attn_gain: bfloat16 [2048], P('shard'), may hold values from 0.5 to 1.5
- w_query: bfloat16 [2048, 1024], P('shard'), may hold values from -0.125 to 0.125
- w_key: bfloat16 [2048, 256], P('shard'), may hold values from -0.125 to 0.125
- w_value: bfloat16 [2048, 256], P('shard'), may hold values from -0.125 to 0.125
- w_output: bfloat16 [1024, 2048], P('shard'), may hold values from -1.5 to 1.5
- mlp_gain: bfloat16 [2048], P('shard'), may hold values from 0.5 to 1.5
- w_gate: bfloat16 [2048, 4096], P('shard'), may hold values from -0.125 to 0.125
- w_up: bfloat16 [2048, 4096], P('shard'), may hold values from -0.125 to 0.125
- w_down: bfloat16 [4096, 2048], P('shard'), may hold values from -0.09375 to 0.09375
Outputs:
- tokens_out: bfloat16 [32, 256, 2048], P(('replica', 'shard'))
- grad_tokens: bfloat16 [32, 256, 2048], P(('replica', 'shard'))
- grad_attn_gain: float32 [2048], P('shard')
- grad_query: float32 [2048, 1024], P('shard')
- grad_key: float32 [2048, 256], P('shard')
- grad_value: float32 [2048, 256], P('shard')
- grad_output: float32 [1024, 2048], P('shard')
- grad_mlp_gain: float32 [2048], P('shard')
- grad_gate: float32 [2048, 4096], P('shard')
- grad_up: float32 [2048, 4096], P('shard')
- grad_down: float32 [4096, 2048], P('shard')
The draws below stay inside these ranges and needn't reach their ends.
Inputs may be any that keep to these rules, and one draw needn't show every extreme that they name: `segment_ids`: in each sequence segment numbers never fall, each segment holds 1 to 128 tokens, and some segment exactly that many.
All inputs are finite; a program needn't handle non-finite values.
Results may differ from the reference program's by a relative error of at most 0.02.
Values may be sent and summed in bfloat16 or wider, within the bound.
A program may use at most 384 MiB of HBM per device.

```python
import math
import jax
import jax.numpy as jnp
import numpy as np
from jax import lax

D = 2048
HQ = 16
KV = 4
HD = 64
FF = 4096
SEQ = 256
SEQS = 32


def steps_of(own_key, shape, cuts, smallest, top_value):
    loudness = 1.0
    for dim, shards_of in cuts:
        steps = jax.random.uniform(jax.random.fold_in(jax.random.fold_in(own_key, 6), dim), (shards_of,), jnp.float32, smallest / len(cuts), top_value / len(cuts))
        loudness = loudness * jnp.repeat(jnp.exp(steps), shape[dim] // shards_of).reshape((-1,) + (1,) * (len(shape) - 1 - dim))
    return loudness


def length_profile(number_of, total, most, lean):
    loads = [(1 << 20) // math.isqrt(standing ** lean) + 1 for standing in range(2, number_of + 1)]
    spare, holding = total - most - (number_of - 1), [1] * (number_of - 1)
    while spare > 0:
        free = [i for i in range(number_of - 1) if holding[i] < most]
        whole, left = sum([loads[i] for i in free]), spare
        for i in free:
            addition = min(most - holding[i], max(1, left * loads[i] // whole), spare)
            holding[i] = holding[i] + addition
            spare = spare - addition
    return np.array([most] + holding)


def uneven_parts(rng, count, total, bound, slope):
    if count == 2:
        one = jax.random.randint(rng, (), max(1, total - bound), min(bound, total - 1) + 1)
        return jnp.stack([one, total - one])
    tallies = jnp.asarray(length_profile(count, total, bound, slope), jnp.int32)
    couples = (count - 1) // 2
    giver, receiver = tallies[1:1 + 2 * couples:2], tallies[2:2 + 2 * couples:2]
    room = jnp.minimum(giver - 1, bound - receiver)
    moved = jax.random.randint(jax.random.fold_in(rng, 1), (couples,), 0, 1 << 20) % (room + 1)
    tallies = tallies.at[1:1 + 2 * couples:2].set(giver - moved).at[2:2 + 2 * couples:2].set(receiver + moved)
    return tallies[jax.random.permutation(jax.random.fold_in(rng, 2), count)]


def centred(key, extent, scale, limit, pieces=(), kind=jnp.bfloat16):
    entries = jax.random.normal(key, extent, jnp.float32) * scale
    if len(pieces) > 0:
        entries = steps_of(key, extent, pieces, -0.22, 0.18) * entries
    return jnp.clip(entries, min=-limit, max=limit).astype(kind)


def setup_inputs(seed: int = 0) -> dict:
    seeds = jax.random.split(jax.random.key(seed), 13)
    return {
        "tokens_in": centred(seeds[0], (SEQS, SEQ, D), 1.0, 6.0, ((0, 32),)),
        "cotangent": centred(seeds[1], (SEQS, SEQ, D), 1.0, 6.0, ((0, 32),)),
        "segment_ids": jax.vmap(lambda own: jnp.searchsorted(jnp.cumsum(uneven_parts(own, 4, SEQ, SEQ // 2, 1)), jnp.arange(SEQ), side="right"))(jax.random.split(seeds[2], SEQS)).reshape((SEQS, SEQ)).astype(jnp.int32),
        "attn_gain": jnp.clip(1.0 + 0.1 * jax.random.normal(seeds[3], (D,), jnp.float32), 0.5, 1.5).astype(jnp.bfloat16),
        "w_query": centred(seeds[4], (D, HQ * HD), D ** -0.5, 0.125, ((0, 4),)),
        "w_key": centred(seeds[5], (D, KV * HD), D ** -0.5, 0.125, ((0, 4),)),
        "w_value": centred(seeds[6], (D, KV * HD), D ** -0.5, 0.125, ((0, 4),)),
        "w_output": centred(seeds[7], (HQ * HD, D), (HQ * HD // 64) ** -0.5, 1.5, ((0, 4),)),
        "mlp_gain": jnp.clip(1.0 + 0.1 * jax.random.normal(seeds[8], (D,), jnp.float32), 0.5, 1.5).astype(jnp.bfloat16),
        "w_gate": centred(seeds[9], (D, FF), D ** -0.5, 0.125, ((0, 4),)),
        "w_up": centred(seeds[10], (D, FF), D ** -0.5, 0.125, ((0, 4),)),
        "w_down": centred(seeds[11], (FF, D), FF ** -0.5, 0.09375, ((0, 4),)),
    }


epsilon = 1e-05
theta_base = 500000.0
neg_large = -1e+30

def contract(form, left_arr, right_arr):
    return jnp.einsum(form, left_arr.astype(jnp.float32), right_arr.astype(jnp.float32))

def matmul(left_arr, right_arr):
    return jnp.dot(left_arr, right_arr, preferred_element_type=jnp.float32)

def positions_of(segment_ids):
    column = lax.broadcasted_iota(jnp.int32, segment_ids.shape, 1)
    starts = jnp.concatenate([jnp.ones_like(segment_ids[:, :1]), (segment_ids[:, 1:] != segment_ids[:, :-1]).astype(jnp.int32)], axis=1)
    seg_start = lax.cummax(jnp.where(starts > 0, column, jnp.zeros_like(column)), axis=1)
    return column - seg_start

def rotary_tables(segment_ids, head_dim):
    positions = positions_of(segment_ids).astype(jnp.float32)
    half_dim = head_dim // 2
    exponent = jnp.arange(half_dim).astype(jnp.float32) * (2.0 / head_dim)
    inverse = theta_base ** (-exponent)
    angles = positions[:, :, None] * inverse[None, None, :]
    return (jnp.cos(angles)[:, :, None, :], jnp.sin(angles)[:, :, None, :])

def rotate(field_in, cosine, sine_tab):
    half_dim = field_in.shape[-1] // 2
    front_half = field_in[..., :half_dim]
    back_half = field_in[..., half_dim:]
    return jnp.concatenate([front_half * cosine - back_half * sine_tab, front_half * sine_tab + back_half * cosine], axis=-1)

def rotate_back(field_in, cosine, sine_tab):
    half_dim = field_in.shape[-1] // 2
    front_half = field_in[..., :half_dim]
    back_half = field_in[..., half_dim:]
    return jnp.concatenate([front_half * cosine + back_half * sine_tab, back_half * cosine - front_half * sine_tab], axis=-1)

def mask_of(segment_ids):
    length = segment_ids.shape[1]
    same_doc = segment_ids[:, :, None] == segment_ids[:, None, :]
    row_idx = lax.broadcasted_iota(jnp.int32, (length, length), 0)
    col_idx = lax.broadcasted_iota(jnp.int32, (length, length), 1)
    return (same_doc & (row_idx >= col_idx)[None])[:, None, None, :, :]

def forward_pass(tokens_in, segment_ids, weights, head_dim, kv_heads):
    attn_gain, w_query, w_key, w_value, w_output, mlp_gain, w_gate, w_up, w_down = weights
    batches, length, model_width = tokens_in.shape
    query_heads = w_query.shape[1] // head_dim
    group_size = query_heads // kv_heads
    scaling = 1.0 / math.sqrt(head_dim)
    flat_in = tokens_in.reshape(batches * length, model_width).astype(jnp.float32)
    inv_attn = lax.rsqrt(lax.optimization_barrier(jnp.mean(flat_in * flat_in, axis=1, keepdims=True)) + epsilon)
    normed_one = (flat_in * inv_attn * attn_gain.astype(jnp.float32)).astype(jnp.bfloat16)
    cosine, sine_tab = rotary_tables(segment_ids, head_dim)
    query_raw = matmul(normed_one, w_query).reshape(batches, length, query_heads, head_dim)
    key_raw = matmul(normed_one, w_key).reshape(batches, length, kv_heads, head_dim)
    query_rot = rotate(query_raw, cosine, sine_tab).astype(jnp.bfloat16).reshape(batches, length, kv_heads, group_size, head_dim)
    key_rot = rotate(key_raw, cosine, sine_tab).astype(jnp.bfloat16)
    value_rows = matmul(normed_one, w_value).astype(jnp.bfloat16).reshape(batches, length, kv_heads, head_dim)
    attn_mask = mask_of(segment_ids)
    scores = jnp.where(attn_mask, contract('bqkgd,bskd->bkgqs', query_rot, key_rot) * scaling, neg_large)
    row_max = lax.optimization_barrier(jnp.max(scores, axis=-1, keepdims=True))
    exp_scores = jnp.exp(scores - row_max)
    row_total = lax.optimization_barrier(jnp.sum(exp_scores, axis=-1, keepdims=True))
    log_sum = row_max + jnp.log(row_total)
    attn_probs = (exp_scores / row_total).astype(jnp.bfloat16)
    context = contract('bkgqs,bskd->bqkgd', attn_probs, value_rows).astype(jnp.bfloat16).reshape(batches * length, query_heads * head_dim)
    hidden = flat_in + matmul(context, w_output)
    inv_mlp = lax.rsqrt(lax.optimization_barrier(jnp.mean(hidden * hidden, axis=1, keepdims=True)) + epsilon)
    normed_two = (hidden * inv_mlp * mlp_gain.astype(jnp.float32)).astype(jnp.bfloat16)
    gate_pre = matmul(normed_two, w_gate)
    up_pre = matmul(normed_two, w_up)
    activated = (jax.nn.silu(gate_pre) * up_pre).astype(jnp.bfloat16)
    tokens_out = (hidden + matmul(activated, w_down)).astype(jnp.bfloat16).reshape(batches, length, model_width)
    stored = (flat_in, inv_attn, normed_one, query_rot, key_rot, value_rows, cosine, sine_tab, attn_mask, log_sum, context, hidden, inv_mlp, normed_two, gate_pre, up_pre, activated)
    return (tokens_out, stored)

def backward_pass(cotangent, stored, weights, head_dim, kv_heads):
    attn_gain, w_query, w_key, w_value, w_output, mlp_gain, w_gate, w_up, w_down = weights
    flat_in, inv_attn, normed_one, query_rot, key_rot, value_rows, cosine, sine_tab, attn_mask, log_sum, context, hidden, inv_mlp, normed_two, gate_pre, up_pre, activated = stored
    batches, length, model_width = cotangent.shape
    query_heads = w_query.shape[1] // head_dim
    group_size = query_heads // kv_heads
    scaling = 1.0 / math.sqrt(head_dim)
    grad_out = cotangent.reshape(batches * length, model_width)
    grad_down = matmul(activated.T, grad_out)
    grad_act = matmul(grad_out, w_down.T)
    sigmoid_gate = jax.nn.sigmoid(gate_pre)
    silu_gate = gate_pre * sigmoid_gate
    grad_gate_pre = (grad_act * up_pre * sigmoid_gate * (1.0 + gate_pre * (1.0 - sigmoid_gate))).astype(jnp.bfloat16)
    grad_up_pre = (grad_act * silu_gate).astype(jnp.bfloat16)
    grad_gate = matmul(normed_two.T, grad_gate_pre)
    grad_up = matmul(normed_two.T, grad_up_pre)
    grad_two = matmul(grad_gate_pre, w_gate.T) + matmul(grad_up_pre, w_up.T)
    grad_mlp_gain = lax.optimization_barrier(jnp.sum(grad_two * hidden * inv_mlp, axis=0))
    scaled_two = grad_two * mlp_gain.astype(jnp.float32)
    grad_hidden = grad_out.astype(jnp.float32) + inv_mlp * (scaled_two - hidden * inv_mlp * inv_mlp * lax.optimization_barrier(jnp.mean(scaled_two * hidden, axis=1, keepdims=True)))
    grad_hid_bf = grad_hidden.astype(jnp.bfloat16)
    grad_output = matmul(context.T, grad_hid_bf)
    grad_context = matmul(grad_hid_bf, w_output.T).astype(jnp.bfloat16).reshape(batches, length, kv_heads, group_size, head_dim)
    scores = jnp.where(attn_mask, contract('bqkgd,bskd->bkgqs', query_rot, key_rot) * scaling, neg_large)
    probs_full = jnp.exp(scores - log_sum)
    grad_value_rows = contract('bkgqs,bqkgd->bskd', probs_full.astype(jnp.bfloat16), grad_context)
    grad_probs = contract('bqkgd,bskd->bkgqs', grad_context, value_rows)
    context_five = context.reshape(batches, length, kv_heads, group_size, head_dim).astype(jnp.float32)
    row_dot = lax.optimization_barrier(jnp.sum(grad_context.astype(jnp.float32) * context_five, axis=-1))
    row_dot = jnp.transpose(row_dot, (0, 2, 3, 1))[..., None]
    grad_scores = (probs_full * (grad_probs - row_dot) * scaling).astype(jnp.bfloat16)
    grad_q_rot = contract('bkgqs,bskd->bqkgd', grad_scores, key_rot).reshape(batches, length, query_heads, head_dim)
    grad_k_rot = contract('bkgqs,bqkgd->bskd', grad_scores, query_rot)
    grad_q_in = rotate_back(grad_q_rot, cosine, sine_tab).astype(jnp.bfloat16).reshape(batches * length, query_heads * head_dim)
    grad_k_in = rotate_back(grad_k_rot, cosine, sine_tab).astype(jnp.bfloat16).reshape(batches * length, kv_heads * head_dim)
    grad_v_in = grad_value_rows.astype(jnp.bfloat16).reshape(batches * length, kv_heads * head_dim)
    grad_query = matmul(normed_one.T, grad_q_in)
    grad_key = matmul(normed_one.T, grad_k_in)
    grad_value = matmul(normed_one.T, grad_v_in)
    grad_one = matmul(grad_q_in, w_query.T) + matmul(grad_k_in, w_key.T) + matmul(grad_v_in, w_value.T)
    grad_attn_gain = lax.optimization_barrier(jnp.sum(grad_one * flat_in * inv_attn, axis=0))
    scaled_one = grad_one * attn_gain.astype(jnp.float32)
    grad_tokens = grad_hidden + inv_attn * (scaled_one - flat_in * inv_attn * inv_attn * lax.optimization_barrier(jnp.mean(scaled_one * flat_in, axis=1, keepdims=True)))
    grad_tokens = grad_tokens.astype(jnp.bfloat16).reshape(batches, length, model_width)
    return (grad_tokens, (grad_attn_gain, grad_query, grad_key, grad_value, grad_output, grad_mlp_gain, grad_gate, grad_up, grad_down))

def reference(tokens_in, cotangent, segment_ids, attn_gain, w_query, w_key, w_value, w_output, mlp_gain, w_gate, w_up, w_down):
    weights = (attn_gain, w_query, w_key, w_value, w_output, mlp_gain, w_gate, w_up, w_down)
    per_block = math.gcd(SEQS, 16)
    blocks = SEQS // per_block

    def one_block(running, block_items):
        block_in, block_cot, block_seg = block_items
        block_out, stored = forward_pass(block_in, block_seg, weights, HD, KV)
        block_grad, grads = backward_pass(block_cot, stored, weights, HD, KV)
        running = tuple((earlier + addend for earlier, addend in zip(running, grads)))
        return (running, (block_out, block_grad))
    zeros_init = tuple((jnp.zeros(weight_arr.shape, jnp.float32) for weight_arr in weights))
    sums, (outputs, input_grads) = lax.scan(one_block, zeros_init, (tokens_in.reshape(blocks, per_block, SEQ, D), cotangent.reshape(blocks, per_block, SEQ, D), segment_ids.reshape(blocks, per_block, SEQ)))
    tokens_out = outputs.reshape(SEQS, SEQ, D)
    grad_tokens = input_grads.reshape(SEQS, SEQ, D)
    return (tokens_out, grad_tokens, sums[0], sums[1], sums[2], sums[3], sums[4], sums[5], sums[6], sums[7], sums[8])
```

```python
import math

import jax
import jax.numpy as jnp
from jax import lax
from jax.sharding import PartitionSpec as P

KV = 4
HD = 64

epsilon = 1e-05
theta_base = 500000.0
neg_large = -1e30


AXES = ("replica", "shard")
f32 = jnp.float32
bf16 = jnp.bfloat16


def contract(form, left_arr, right_arr):
    return jnp.einsum(form, left_arr, right_arr, preferred_element_type=f32)


def matmul(left_arr, right_arr):
    return jnp.dot(left_arr, right_arr, preferred_element_type=f32)


def matmul_nt(left_arr, right_arr):
    return lax.dot_general(
        left_arr, right_arr, (((1,), (1,)), ((), ())), preferred_element_type=f32
    )


def matmul_tn(left_arr, right_arr):
    return lax.dot_general(
        left_arr, right_arr, (((0,), (0,)), ((), ())), preferred_element_type=f32
    )


def positions_of(segment_ids):
    column = lax.broadcasted_iota(jnp.int32, segment_ids.shape, 1)
    starts = jnp.concatenate(
        [
            jnp.ones_like(segment_ids[:, :1]),
            (segment_ids[:, 1:] != segment_ids[:, :-1]).astype(jnp.int32),
        ],
        axis=1,
    )
    seg_start = lax.cummax(jnp.where(starts > 0, column, jnp.zeros_like(column)), axis=1)
    return column - seg_start


def rotary_tables(segment_ids, head_dim):
    positions = positions_of(segment_ids).astype(f32)
    half_dim = head_dim // 2
    exponent = jnp.arange(half_dim).astype(f32) * (2.0 / head_dim)
    inverse = theta_base ** (-exponent)
    angles = positions[:, :, None] * inverse[None, None, :]
    return (jnp.cos(angles)[:, :, None, :], jnp.sin(angles)[:, :, None, :])


def rotate(field_in, cosine, sine_tab):
    half_dim = field_in.shape[-1] // 2
    front_half = field_in[..., :half_dim]
    back_half = field_in[..., half_dim:]
    return jnp.concatenate(
        [front_half * cosine - back_half * sine_tab, front_half * sine_tab + back_half * cosine],
        axis=-1,
    )


def rotate_back(field_in, cosine, sine_tab):
    half_dim = field_in.shape[-1] // 2
    front_half = field_in[..., :half_dim]
    back_half = field_in[..., half_dim:]
    return jnp.concatenate(
        [front_half * cosine + back_half * sine_tab, back_half * cosine - front_half * sine_tab],
        axis=-1,
    )


def mask_of(segment_ids):
    length = segment_ids.shape[1]
    same_doc = segment_ids[:, :, None] == segment_ids[:, None, :]
    row_idx = lax.broadcasted_iota(jnp.int32, (length, length), 0)
    col_idx = lax.broadcasted_iota(jnp.int32, (length, length), 1)
    return (same_doc & (row_idx >= col_idx)[None])[:, None, None, :, :]


def cut(arr, start, size, axis=0):
    return lax.dynamic_slice_in_dim(arr, start, size, axis)


def put(arr, part, start, axis=0):
    return lax.dynamic_update_slice_in_dim(arr, part, start, axis)


class Fabric:
    def __init__(self, mesh):
        self.R = mesh.shape["replica"]
        self.S = mesh.shape["shard"]
        self.n = self.R // 2
        assert self.S == 4 and self.R % 4 == 0, "unsupported mesh"

    def place(self):
        r = lax.axis_index("replica")
        s = lax.axis_index("shard")
        self.s = s
        self.c = lax.rem(s, 2)
        self.x = lax.rem(r, 2)
        self.z = lax.div(r, 2)
        self.high = (self.z >= self.n // 2).astype(jnp.int32)

    def move(self, arr, to):
        pairs = []
        for r in range(self.R):
            for s in range(self.S):
                there = to(r, s)
                if there is not None:
                    pairs.append((r * self.S + s, there[0] * self.S + there[1]))
        return lax.ppermute(arr, AXES, pairs)

    def core(self, arr):
        return self.move(arr, lambda r, s: (r, s ^ 1))

    def row(self, arr):
        return self.move(arr, lambda r, s: (r, s ^ 2))

    def diagonal(self, arr):
        return self.move(arr, lambda r, s: (r, s ^ 3))

    def column(self, arr):
        return self.move(arr, lambda r, s: (r ^ 1, s))

    def column_mid(self, arr):
        mid = (self.n // 2 - 1, self.n // 2)
        return self.move(arr, lambda r, s: (r ^ 1, s) if r // 2 in mid else None)

    def line_mid(self, arr):
        lo, hi = self.n // 2 - 1, self.n // 2
        other = {lo: hi, hi: lo}
        return self.move(
            arr, lambda r, s: (other[r // 2] * 2 + r % 2, s) if r // 2 in other else None
        )

    def inward(self, arr, i):
        step = {i: i + 1, self.n - 1 - i: self.n - 2 - i}
        return self.move(
            arr, lambda r, s: (step[r // 2] * 2 + r % 2, s) if r // 2 in step else None
        )

    def outward(self, arr, i):
        step = {i + 1: i, self.n - 2 - i: self.n - 1 - i}
        return self.move(
            arr, lambda r, s: (step[r // 2] * 2 + r % 2, s) if r // 2 in step else None
        )

    def ordered(self, own, other, flag, axis=0):
        return jnp.where(
            flag == 0,
            jnp.concatenate([own, other], axis),
            jnp.concatenate([other, own], axis),
        )


    def gather_rows(self, block):
        m = block.shape[0]
        h = m // 2
        s, x = self.s, self.x
        near = self.core(block)
        a = self.row(cut(block, x * h, h))
        b = self.column(a)
        ac = self.core(a)
        bc = self.core(b)
        whole = jnp.zeros((self.S * m,) + block.shape[1:], block.dtype)
        whole = put(whole, block, s * m)
        whole = put(whole, near, (s ^ 1) * m)
        whole = put(whole, a, (s ^ 2) * m + x * h)
        whole = put(whole, ac, (s ^ 3) * m + x * h)
        whole = put(whole, b, (s ^ 2) * m + (1 - x) * h)
        whole = put(whole, bc, (s ^ 3) * m + (1 - x) * h)
        return whole

    def exchange_columns(self, part_for, m):
        h = m // 2
        s, x = self.s, self.x
        own = part_for(s)
        near = self.core(part_for(s ^ 1))
        a = self.row(cut(part_for(s ^ 2), x * h, h))
        ad = self.diagonal(cut(part_for(s ^ 3), x * h, h))
        b = self.column(a)
        bd = self.column(ad)
        whole = jnp.zeros((self.S * m, own.shape[1]), own.dtype)
        whole = put(whole, own, s * m)
        whole = put(whole, near, (s ^ 1) * m)
        whole = put(whole, a, (s ^ 2) * m + x * h)
        whole = put(whole, ad, (s ^ 3) * m + x * h)
        whole = put(whole, b, (s ^ 2) * m + (1 - x) * h)
        whole = put(whole, bd, (s ^ 3) * m + (1 - x) * h)
        return whole


    def gather_tokens(self, own):
        near = self.core(own)
        far = self.row(own)
        far_near = self.core(far)
        return self.ordered(own, near, self.c), self.ordered(far, far_near, self.c)

    def exchange_tokens(self, part_for):
        own = part_for(self.s)
        near = self.core(part_for(self.s ^ 1))
        far = self.row(part_for(self.s ^ 2))
        far_near = self.diagonal(part_for(self.s ^ 3))
        return self.ordered(own, near, self.c), self.ordered(far, far_near, self.c)

    def scatter_tokens(self, part_a, part_b):
        m = part_a.shape[0] // 2
        c = self.c
        other_b = self.core(cut(part_b, (1 - c) * m, m).astype(bf16))
        sum_b = (cut(part_b, c * m, m) + other_b.astype(f32)).astype(bf16)
        far = self.row(sum_b)
        other_a = self.core(cut(part_a, (1 - c) * m, m).astype(bf16))
        return cut(part_a, c * m, m) + other_a.astype(f32) + far.astype(f32)


    def sum_by_column(self, chunk):
        h = chunk.shape[0] // 2
        q = h // 2
        x, high, z = self.x, self.high, self.z
        got = self.column(cut(chunk, (1 - x) * h, h))
        a = add(cut(chunk, x * h, h), got)
        for i in range(self.n // 2 - 1):
            a = add(a, self.inward(a, i))
        got = self.line_mid(cut(a, (1 - high) * q, q))
        b = add(cut(a, high * q, q), got)
        half = self.ordered(b, self.line_mid(b), high)
        for i in reversed(range(self.n // 2 - 1)):
            got = self.outward(half, i)
            half = jnp.where((z == i) | (z == self.n - 1 - i), got, half)
        return half, self.column(half)

    def sum_by_line(self, chunk):
        h = chunk.shape[0] // 2
        q = h // 2
        x, high, z = self.x, self.high, self.z
        a = chunk
        for i in range(self.n // 2 - 1):
            a = add(a, self.inward(a, i))
        got = self.line_mid(cut(a, (1 - high) * h, h))
        a = add(cut(a, high * h, h), got)
        got = self.column_mid(cut(a, (1 - x) * q, q))
        b = add(cut(a, x * q, q), got)
        half = self.ordered(b, self.column_mid(b), x)
        whole = self.ordered(half, self.line_mid(half), high)
        for i in reversed(range(self.n // 2 - 1)):
            got = self.outward(whole, i)
            whole = jnp.where((z == i) | (z == self.n - 1 - i), got, whole)
        return whole

    def sum_chunks(self, chunks):
        pass

    def sum_all(self, arr):
        for bit in (1, 2):
            arr = arr + self.move(arr, lambda r, s: (r, s ^ bit))
        if self.R & (self.R - 1):
            return lax.psum(arr, "replica")
        bit = 1
        while bit < self.R:
            arr = arr + self.move(arr, lambda r, s: (r ^ bit, s))
            bit *= 2
        return arr


def add(one, two):
    return (one.astype(f32) + two.astype(f32)).astype(bf16)


class Sums:
    def __init__(self, fabric, shape):
        self.fabric = fabric
        self.out = jnp.zeros(shape, f32)

    def take(self, chunk, row, column, kind):
        fabric = self.fabric
        if kind == 0:
            h = chunk.shape[0] // 2
            own, other = fabric.sum_by_column(chunk)
            self.write(own, row + fabric.x * h, column)
            self.write(other, row + (1 - fabric.x) * h, column)
        else:
            self.write(fabric.sum_by_line(chunk), row, column)

    def write(self, part, row, column):
        self.out = lax.dynamic_update_slice(self.out, part.astype(f32), (row, column))


def per_device(
    fabric,
    tokens_in,
    cotangent,
    segment_ids,
    attn_gain,
    w_query,
    w_key,
    w_value,
    w_output,
    mlp_gain,
    w_gate,
    w_up,
    w_down,
):
    fabric.place()
    s, S = fabric.s, fabric.S
    batches, length, width = tokens_in.shape
    tokens = batches * length
    rows = w_query.shape[0]
    q_cols, kv_cols = w_query.shape[1], w_key.shape[1]
    head_rows = w_output.shape[0]
    ff_rows = w_down.shape[0]
    query_heads = q_cols // HD
    group_size = query_heads // KV
    scaling = 1.0 / math.sqrt(HD)

    w_qkv = fabric.gather_rows(jnp.concatenate([w_query, w_key, w_value], axis=1))
    w_out = fabric.gather_rows(w_output)
    gains = jnp.concatenate([attn_gain[None], mlp_gain[None]], axis=0)
    gains = lax.all_gather(gains, "shard", axis=1, tiled=True).astype(f32)
    gain_one, gain_two = gains[0], gains[1]
    w_gu = fabric.exchange_columns(
        lambda t: jnp.concatenate(
            [cut(w_gate, t * ff_rows, ff_rows, 1), cut(w_up, t * ff_rows, ff_rows, 1)], axis=1
        ),
        rows,
    )
    grad_out = cotangent.reshape(tokens, width)
    cot_a, cot_b = fabric.gather_tokens(grad_out)

    flat_in = tokens_in.reshape(tokens, width).astype(f32)
    inv_attn = lax.rsqrt(jnp.mean(flat_in * flat_in, axis=1, keepdims=True) + epsilon)
    normed_one = (flat_in * inv_attn * gain_one).astype(bf16)
    cosine, sine_tab = rotary_tables(segment_ids, HD)
    qkv = matmul(normed_one, w_qkv)
    query_raw = qkv[:, :q_cols].reshape(batches, length, query_heads, HD)
    key_raw = qkv[:, q_cols : q_cols + kv_cols].reshape(batches, length, KV, HD)
    value_rows = qkv[:, q_cols + kv_cols :].astype(bf16).reshape(batches, length, KV, HD)
    query_rot = (
        rotate(query_raw, cosine, sine_tab)
        .astype(bf16)
        .reshape(batches, length, KV, group_size, HD)
    )
    key_rot = rotate(key_raw, cosine, sine_tab).astype(bf16)
    attn_mask = mask_of(segment_ids)
    scores = jnp.where(
        attn_mask, contract("bqkgd,bskd->bkgqs", query_rot, key_rot) * scaling, neg_large
    )
    row_max = jnp.max(scores, axis=-1, keepdims=True)
    exp_scores = jnp.exp(scores - row_max)
    row_total = jnp.sum(exp_scores, axis=-1, keepdims=True)
    log_sum = row_max + jnp.log(row_total)
    attn_probs = (exp_scores / row_total).astype(bf16)
    context = (
        contract("bkgqs,bskd->bqkgd", attn_probs, value_rows).astype(bf16).reshape(tokens, q_cols)
    )
    hidden = flat_in + matmul(context, w_out)
    inv_mlp = lax.rsqrt(jnp.mean(hidden * hidden, axis=1, keepdims=True) + epsilon)
    normed_two = (hidden * inv_mlp * gain_two).astype(bf16)

    two_a, two_b = fabric.gather_tokens(normed_two)

    def hidden_units(two):
        gu = matmul(two, w_gu)
        gate_pre, up_pre = gu[:, :ff_rows], gu[:, ff_rows:]
        return gate_pre, up_pre, (jax.nn.silu(gate_pre) * up_pre).astype(bf16)

    gate_a, up_a, act_a = hidden_units(two_a)
    gate_b, up_b, act_b = hidden_units(two_b)
    act = jnp.concatenate([act_a, act_b], axis=0)
    cot = jnp.concatenate([cot_a, cot_b], axis=0)

    down = Sums(fabric, w_down.shape)
    pieces = 4
    step = ff_rows // pieces
    for k in range(pieces):
        chunk = matmul_tn(act[:, k * step : (k + 1) * step], cot).astype(bf16)
        down.take(chunk, k * step, 0, k % 2)

    def grads_of(gate_pre, up_pre, cot_half):
        grad_act = matmul_nt(cot_half, w_down)
        sigmoid_gate = jax.nn.sigmoid(gate_pre)
        grad_gate = (
            grad_act * up_pre * sigmoid_gate * (1.0 + gate_pre * (1.0 - sigmoid_gate))
        ).astype(bf16)
        grad_up = (grad_act * (gate_pre * sigmoid_gate)).astype(bf16)
        return grad_gate, grad_up

    gg_a, gu_a = grads_of(gate_a, up_a, cot_a)
    gg_b, gu_b = grads_of(gate_b, up_b, cot_b)
    w_g, w_u = w_gu[:, :ff_rows], w_gu[:, ff_rows:]
    two_part_a = matmul_nt(gg_a, w_g) + matmul_nt(gu_a, w_u)
    two_part_b = matmul_nt(gg_b, w_g) + matmul_nt(gu_b, w_u)
    grad_two = fabric.scatter_tokens(two_part_a, two_part_b)

    own_a = cut(two_a, s * rows, rows, 1)
    own_b = cut(two_b, s * rows, rows, 1)
    two_near = jnp.concatenate([own_a, own_b], axis=0)
    two_far = jnp.concatenate([own_b, own_a], axis=0)
    gg = jnp.concatenate([gg_a, gg_b], axis=0)
    gu = jnp.concatenate([gu_a, gu_b], axis=0)
    gg_row, gu_row = fabric.row(gg), fabric.row(gu)
    gate_sum, up_sum = Sums(fabric, w_gate.shape), Sums(fabric, w_up.shape)
    gate_in = (gg, fabric.core(gg), gg_row, fabric.core(gg_row))
    up_in = (gu, fabric.core(gu), gu_row, fabric.core(gu_row))
    for j in range(S):
        left = two_near if j < 2 else two_far
        for sums, source, kind in ((gate_sum, gate_in, 0), (up_sum, up_in, 1)):
            chunk = matmul_tn(left, source[j]).astype(bf16)
            sums.take(chunk, 0, (s ^ j) * ff_rows, kind)

    out_part_a = matmul(act_a, w_down)
    out_part_b = matmul(act_b, w_down)
    tokens_out = (hidden + fabric.scatter_tokens(out_part_a, out_part_b)).astype(bf16)

    part_mlp_gain = jnp.sum(grad_two * hidden * inv_mlp, axis=0)
    scaled_two = grad_two * gain_two
    grad_hidden = grad_out.astype(f32) + inv_mlp * (
        scaled_two
        - hidden * inv_mlp * inv_mlp * jnp.mean(scaled_two * hidden, axis=1, keepdims=True)
    )
    grad_hid_bf = grad_hidden.astype(bf16)
    gh_a, gh_b = fabric.gather_tokens(grad_hid_bf)
    ctx_a, ctx_b = fabric.exchange_tokens(lambda t: cut(context, t * head_rows, head_rows, 1))
    out_sum = Sums(fabric, w_output.shape)
    chunk = matmul_tn(
        jnp.concatenate([ctx_a, ctx_b], axis=0), jnp.concatenate([gh_a, gh_b], axis=0)
    )
    out_sum.take(chunk.astype(bf16), 0, 0, 0)

    grad_context = (
        matmul_nt(grad_hid_bf, w_out).astype(bf16).reshape(batches, length, KV, group_size, HD)
    )
    scores = jnp.where(
        attn_mask, contract("bqkgd,bskd->bkgqs", query_rot, key_rot) * scaling, neg_large
    )
    probs_full = jnp.exp(scores - log_sum)
    grad_value_rows = contract("bkgqs,bqkgd->bskd", probs_full.astype(bf16), grad_context)
    grad_probs = contract("bqkgd,bskd->bkgqs", grad_context, value_rows)
    context_five = context.reshape(batches, length, KV, group_size, HD).astype(f32)
    row_dot = jnp.sum(grad_context.astype(f32) * context_five, axis=-1)
    row_dot = jnp.transpose(row_dot, (0, 2, 3, 1))[..., None]
    grad_scores = (probs_full * (grad_probs - row_dot) * scaling).astype(bf16)
    grad_q_rot = contract("bkgqs,bskd->bqkgd", grad_scores, key_rot).reshape(
        batches, length, query_heads, HD
    )
    grad_k_rot = contract("bkgqs,bqkgd->bskd", grad_scores, query_rot)
    grad_q_in = rotate_back(grad_q_rot, cosine, sine_tab).astype(bf16).reshape(tokens, q_cols)
    grad_k_in = rotate_back(grad_k_rot, cosine, sine_tab).astype(bf16).reshape(tokens, kv_cols)
    grad_v_in = grad_value_rows.astype(bf16).reshape(tokens, kv_cols)
    grad_qkv = jnp.concatenate([grad_q_in, grad_k_in, grad_v_in], axis=1)

    gq_a, gq_b = fabric.gather_tokens(grad_qkv)
    one_a, one_b = fabric.exchange_tokens(lambda t: cut(normed_one, t * rows, rows, 1))
    qkv_sum = Sums(fabric, (rows, q_cols + 2 * kv_cols))
    chunk = matmul_tn(
        jnp.concatenate([one_a, one_b], axis=0), jnp.concatenate([gq_a, gq_b], axis=0)
    )
    qkv_sum.take(chunk.astype(bf16), 0, 0, 1)

    grad_one = matmul_nt(grad_qkv, w_qkv)
    part_attn_gain = jnp.sum(grad_one * flat_in * inv_attn, axis=0)
    scaled_one = grad_one * gain_one
    grad_tokens = grad_hidden + inv_attn * (
        scaled_one
        - flat_in * inv_attn * inv_attn * jnp.mean(scaled_one * flat_in, axis=1, keepdims=True)
    )
    gain_sums = fabric.sum_all(jnp.stack([part_attn_gain, part_mlp_gain]))
    gain_sums = cut(gain_sums, s * rows, rows, 1)

    return (
        tokens_out.reshape(tokens_in.shape),
        grad_tokens.astype(bf16).reshape(tokens_in.shape),
        gain_sums[0],
        qkv_sum.out[:, :q_cols],
        qkv_sum.out[:, q_cols : q_cols + kv_cols],
        qkv_sum.out[:, q_cols + kv_cols :],
        out_sum.out,
        gain_sums[1],
        gate_sum.out,
        up_sum.out,
        down.out,
    )


def solution(mesh):
    fabric = Fabric(mesh)
    data = P(AXES, None, None)
    rowwise = P("shard", None)
    flat = P("shard")
    return jax.shard_map(
        lambda *args: per_device(fabric, *args),
        mesh=mesh,
        in_specs=(
            (data, data, P(AXES, None), flat)
            + (rowwise,) * 4
            + (flat,)
            + (rowwise,) * 3
        ),
        out_specs=(data, data, flat) + (rowwise,) * 4 + (flat,) + (rowwise,) * 3,
        check_vma=False,
    )
```

```python
import functools
import math

import jax
import jax.numpy as jnp
from jax import lax
from jax.experimental import pallas as pl
from jax.experimental.pallas import tpu as pltpu
from jax.sharding import PartitionSpec as P

KV = 4
HD = 64

epsilon = 1e-05
theta_base = 500000.0
neg_large = -1e30


AXES = ("replica", "shard")
f32 = jnp.float32
bf16 = jnp.bfloat16


def contract(form, left_arr, right_arr):
    return jnp.einsum(form, left_arr, right_arr, preferred_element_type=f32)


def matmul(left_arr, right_arr):
    return jnp.dot(left_arr, right_arr, preferred_element_type=f32)


def matmul_nt(left_arr, right_arr):
    return lax.dot_general(
        left_arr, right_arr, (((1,), (1,)), ((), ())), preferred_element_type=f32
    )


def matmul_tn(left_arr, right_arr):
    return lax.dot_general(
        left_arr, right_arr, (((0,), (0,)), ((), ())), preferred_element_type=f32
    )


def positions_of(segment_ids):
    column = lax.broadcasted_iota(jnp.int32, segment_ids.shape, 1)
    starts = jnp.concatenate(
        [
            jnp.ones_like(segment_ids[:, :1]),
            (segment_ids[:, 1:] != segment_ids[:, :-1]).astype(jnp.int32),
        ],
        axis=1,
    )
    seg_start = lax.cummax(jnp.where(starts > 0, column, jnp.zeros_like(column)), axis=1)
    return column - seg_start


def rotary_tables(segment_ids, head_dim):
    positions = positions_of(segment_ids).astype(f32)
    half_dim = head_dim // 2
    exponent = jnp.arange(half_dim).astype(f32) * (2.0 / head_dim)
    inverse = theta_base ** (-exponent)
    angles = positions[:, :, None] * inverse[None, None, :]
    return (jnp.cos(angles)[:, :, None, :], jnp.sin(angles)[:, :, None, :])


def rotate(field_in, cosine, sine_tab):
    half_dim = field_in.shape[-1] // 2
    front_half = field_in[..., :half_dim]
    back_half = field_in[..., half_dim:]
    return jnp.concatenate(
        [front_half * cosine - back_half * sine_tab, front_half * sine_tab + back_half * cosine],
        axis=-1,
    )


def rotate_back(field_in, cosine, sine_tab):
    half_dim = field_in.shape[-1] // 2
    front_half = field_in[..., :half_dim]
    back_half = field_in[..., half_dim:]
    return jnp.concatenate(
        [front_half * cosine + back_half * sine_tab, back_half * cosine - front_half * sine_tab],
        axis=-1,
    )


def mask_of(segment_ids):
    length = segment_ids.shape[1]
    same_doc = segment_ids[:, :, None] == segment_ids[:, None, :]
    row_idx = lax.broadcasted_iota(jnp.int32, (length, length), 0)
    col_idx = lax.broadcasted_iota(jnp.int32, (length, length), 1)
    return (same_doc & (row_idx >= col_idx)[None])[:, None, None, :, :]


def cut(arr, start, size, axis=0):
    return lax.dynamic_slice_in_dim(arr, start, size, axis)


def put(arr, part, start, axis=0):
    return lax.dynamic_update_slice_in_dim(arr, part, start, axis)


class Fabric:
    def __init__(self, mesh):
        self.R = mesh.shape["replica"]
        self.S = mesh.shape["shard"]
        self.n = self.R // 2
        assert self.S == 4 and self.R % 4 == 0, "unsupported mesh"

    def place(self):
        r = lax.axis_index("replica")
        s = lax.axis_index("shard")
        self.s = s
        self.c = lax.rem(s, 2)
        self.x = lax.rem(r, 2)
        self.z = lax.div(r, 2)
        self.high = (self.z >= self.n // 2).astype(jnp.int32)

    def move(self, arr, to):
        pairs = []
        for r in range(self.R):
            for s in range(self.S):
                there = to(r, s)
                if there is not None:
                    pairs.append((r * self.S + s, there[0] * self.S + there[1]))
        return lax.ppermute(arr, AXES, pairs)

    def core(self, arr):
        return self.move(arr, lambda r, s: (r, s ^ 1))

    def row(self, arr):
        return self.move(arr, lambda r, s: (r, s ^ 2))

    def diagonal(self, arr):
        return self.move(arr, lambda r, s: (r, s ^ 3))

    def column(self, arr):
        return self.move(arr, lambda r, s: (r ^ 1, s))

    def column_mid(self, arr):
        mid = (self.n // 2 - 1, self.n // 2)
        return self.move(arr, lambda r, s: (r ^ 1, s) if r // 2 in mid else None)

    def line_mid(self, arr):
        lo, hi = self.n // 2 - 1, self.n // 2
        other = {lo: hi, hi: lo}
        return self.move(
            arr, lambda r, s: (other[r // 2] * 2 + r % 2, s) if r // 2 in other else None
        )

    def inward(self, arr, i):
        step = {i: i + 1, self.n - 1 - i: self.n - 2 - i}
        return self.move(
            arr, lambda r, s: (step[r // 2] * 2 + r % 2, s) if r // 2 in step else None
        )

    def outward(self, arr, i):
        step = {i + 1: i, self.n - 2 - i: self.n - 1 - i}
        return self.move(
            arr, lambda r, s: (step[r // 2] * 2 + r % 2, s) if r // 2 in step else None
        )

    def ordered(self, own, other, flag, axis=0):
        return jnp.where(
            flag == 0,
            jnp.concatenate([own, other], axis),
            jnp.concatenate([other, own], axis),
        )


    def gather_rows(self, block):
        m = block.shape[0]
        h = m // 2
        s, x = self.s, self.x
        near = self.core(block)
        a = self.row(cut(block, x * h, h))
        b = self.column(a)
        ac = self.core(a)
        bc = self.core(b)
        whole = jnp.zeros((self.S * m,) + block.shape[1:], block.dtype)
        whole = put(whole, block, s * m)
        whole = put(whole, near, (s ^ 1) * m)
        whole = put(whole, a, (s ^ 2) * m + x * h)
        whole = put(whole, ac, (s ^ 3) * m + x * h)
        whole = put(whole, b, (s ^ 2) * m + (1 - x) * h)
        whole = put(whole, bc, (s ^ 3) * m + (1 - x) * h)
        return whole

    def exchange_columns(self, part_for, m):
        h = m // 2
        s, x = self.s, self.x
        own = part_for(s)
        near = self.core(part_for(s ^ 1))
        a = self.row(cut(part_for(s ^ 2), x * h, h))
        ad = self.diagonal(cut(part_for(s ^ 3), x * h, h))
        b = self.column(a)
        bd = self.column(ad)
        whole = jnp.zeros((self.S * m, own.shape[1]), own.dtype)
        whole = put(whole, own, s * m)
        whole = put(whole, near, (s ^ 1) * m)
        whole = put(whole, a, (s ^ 2) * m + x * h)
        whole = put(whole, ad, (s ^ 3) * m + x * h)
        whole = put(whole, b, (s ^ 2) * m + (1 - x) * h)
        whole = put(whole, bd, (s ^ 3) * m + (1 - x) * h)
        return whole

    def gather_gains(self, own):
        whole = put(jnp.zeros((own.shape[0], self.S * own.shape[1]), f32), own, self.s * own.shape[1], 1)
        for bit in (1, 2):
            whole = whole + self.move(whole, lambda r, s: (r, s ^ bit))
        return whole


    def gather_tokens(self, own):
        near = self.core(own)
        far = self.row(own)
        far_near = self.core(far)
        return self.ordered(own, near, self.c), self.ordered(far, far_near, self.c)

    def exchange_tokens(self, part_for):
        own = part_for(self.s)
        near = self.core(part_for(self.s ^ 1))
        far = self.row(part_for(self.s ^ 2))
        far_near = self.diagonal(part_for(self.s ^ 3))
        return self.ordered(own, near, self.c), self.ordered(far, far_near, self.c)

    def scatter_tokens(self, part_a, part_b):
        m = part_a.shape[0] // 2
        c = self.c
        other_b = self.core(cut(part_b, (1 - c) * m, m).astype(bf16))
        sum_b = (cut(part_b, c * m, m) + other_b.astype(f32)).astype(bf16)
        far = self.row(sum_b)
        other_a = self.core(cut(part_a, (1 - c) * m, m).astype(bf16))
        return cut(part_a, c * m, m) + other_a.astype(f32) + far.astype(f32)


class Copies:
    def __init__(self, send, recv):
        self.send, self.recv, self.count, self.open = send, recv, 0, []

    def start(self, src, dst, device):
        copy = pltpu.make_async_remote_copy(
            src_ref=src,
            dst_ref=dst,
            send_sem=self.send.at[self.count],
            recv_sem=self.recv.at[self.count],
            device_id=device,
            device_id_type=pl.DeviceIdType.MESH,
        )
        self.count += 1
        copy.start()
        self.open.append(copy)
        return self.count - 1

    def arrived(self, number, landed):
        pltpu.make_async_copy(landed, landed, self.recv.at[number]).wait()

    def finish(self):
        for copy in self.open:
            copy.wait_send()


def meet(devices):
    barrier = pltpu.get_barrier_semaphore()
    for device in devices:
        pl.semaphore_signal(
            barrier, inc=1, device_id=device, device_id_type=pl.DeviceIdType.MESH
        )
    pl.semaphore_wait(barrier, len(devices))


def fetch_kernel(
    w_qkv, w_o, w_gate, w_up, cot, all_qkv, all_o, all_gu, all_cot, send, recv, local, *stages
):
    r, s = lax.axis_index("replica"), lax.axis_index("shard")
    c, y = lax.rem(s, 2), lax.div(s, 2)
    x = lax.rem(r, 2)
    w = lax.rem(lax.div(r, 2), 2)
    near, row = 2 * y + 1 - c, 2 * (1 - y) + c
    diagonal = 2 * (1 - y) + 1 - c
    r_x = r + 1 - 2 * x
    r_z = r + 2 - 4 * w
    core_dev, row_dev, diag_dev = (r, near), (r, row), (r, diagonal)
    x_dev, z_dev = (r_x, s), (r_z, s)
    meet([core_dev, row_dev, diag_dev, x_dev, z_dev])
    copies = Copies(send, recv)

    m_q, m_o, m_g = w_qkv.shape[0], w_o.shape[0], w_gate.shape[0]
    ff, tok = all_gu.shape[1] // 2, cot.shape[0]

    def rows_of(ref, start, size):
        return ref.at[pl.ds(pl.multiple_of(start, 16), size)]

    def region(ref, m, owner, quarter):
        return rows_of(ref, owner * m + quarter * (m // 4), m // 4)

    def columns_of(ref, start, rows, shard):
        return ref.at[
            pl.ds(pl.multiple_of(start, 16), rows), pl.ds(pl.multiple_of(shard * ff, 128), ff)
        ]

    def quarter(flip_x, flip_z):
        at_x = (1 - x) if flip_x else x
        at_z = (1 - w) if flip_z else w
        return 2 * at_z + at_x

    here = quarter(0, 0)
    q_g = m_g // 4

    def gu_part(owner, start, rows):
        return [
            all_gu.at[pl.ds(pl.multiple_of(owner * m_g + start, 16), rows), pl.ds(k * ff, ff)]
            for k in (0, 1)
        ]

    first = []
    first.append([copies.start(rows_of(w_qkv, here * (m_q // 4), m_q // 4), region(all_qkv, m_q, s, here), row_dev)])
    first.append([copies.start(rows_of(w_o, here * (m_o // 4), m_o // 4), region(all_o, m_o, s, here), row_dev)])
    for shard, device in ((row, row_dev), (diagonal, diag_dev)):
        first.append(
            [
                copies.start(columns_of(ref, here * q_g, q_g, shard), part, device)
                for ref, part in zip((w_gate, w_up), gu_part(s, here * q_g, q_g))
            ]
        )
    cot_far = copies.start(cot, rows_of(all_cot, 2 * tok + c * tok, tok), row_dev)

    core_q = copies.start(w_qkv, rows_of(all_qkv, s * m_q, m_q), core_dev)
    core_o = copies.start(w_o, rows_of(all_o, s * m_o, m_o), core_dev)
    core_g = [
        copies.start(columns_of(ref, 0, m_g, near), part, core_dev)
        for ref, part in zip((w_gate, w_up), gu_part(s, 0, m_g))
    ]
    core_c = copies.start(cot, rows_of(all_cot, c * tok, tok), core_dev)
    own = [
        (w_qkv, rows_of(all_qkv, s * m_q, m_q)),
        (w_o, rows_of(all_o, s * m_o, m_o)),
        (columns_of(w_gate, 0, m_g, s), gu_part(s, 0, m_g)[0]),
        (columns_of(w_up, 0, m_g, s), gu_part(s, 0, m_g)[1]),
        (cot, rows_of(all_cot, c * tok, tok)),
    ]
    staged = [
        pltpu.make_async_copy(source, stage, local.at[i])
        for i, ((source, _), stage) in enumerate(zip(own, stages))
    ]
    for copy in staged:
        copy.start()
    for copy in staged:
        copy.wait()
    own = [
        pltpu.make_async_copy(stage, there, local.at[i])
        for i, ((_, there), stage) in enumerate(zip(own, stages))
    ]
    for copy in own:
        copy.start()

    flows = [
        (all_qkv, m_q, row, True, False),
        (all_o, m_o, row, True, True),
        (all_gu, m_g, row, False, False),
        (all_gu, m_g, diagonal, False, True),
    ]
    forwarded, second, third = [], {}, {}

    def landed_first(i):
        ref, m, owner, to_core, line_first = flows[i]
        if len(first[i]) == 1:
            copies.arrived(first[i][0], region(ref, m, owner, here))
        else:
            for number, part in zip(first[i], gu_part(owner, here * q_g, q_g)):
                copies.arrived(number, part)
        piece = region(ref, m, owner, here)
        second[i] = copies.start(piece, piece, z_dev if line_first else x_dev)
        if to_core:
            forwarded.append((copies.start(piece, piece, core_dev), i, (0, 0)))

    def landed_second(i):
        ref, m, owner, to_core, line_first = flows[i]
        flip = (0, 1) if line_first else (1, 0)
        other = region(ref, m, owner, quarter(*flip))
        copies.arrived(second[i], other)
        third[i] = []
        for part, spot in ((region(ref, m, owner, here), (0, 0)), (other, flip)):
            third[i].append((copies.start(part, part, x_dev if line_first else z_dev), spot))
        if to_core:
            forwarded.append((copies.start(other, other, core_dev), i, flip))

    def landed_third(i):
        ref, m, owner, to_core, line_first = flows[i]
        for number, (fx, fz) in third[i]:
            spot = (1 - fx, fz) if line_first else (fx, 1 - fz)
            part = region(ref, m, owner, quarter(*spot))
            copies.arrived(number, part)
            if to_core:
                forwarded.append((copies.start(part, part, core_dev), i, spot))

    for i in range(len(flows) + 2):
        if i < len(flows):
            landed_first(i)
        if 0 <= i - 1 < len(flows):
            landed_second(i - 1)
        if i >= 2:
            landed_third(i - 2)
    part = rows_of(all_cot, 2 * tok + c * tok, tok)
    copies.arrived(cot_far, part)
    last = copies.start(part, part, core_dev)

    other = diagonal
    copies.arrived(core_q, rows_of(all_qkv, near * m_q, m_q))
    copies.arrived(core_o, rows_of(all_o, near * m_o, m_o))
    for number, part in zip(core_g, gu_part(near, 0, m_g)):
        copies.arrived(number, part)
    copies.arrived(core_c, rows_of(all_cot, (1 - c) * tok, tok))
    for number, i, spot in forwarded:
        ref, m = flows[i][:2]
        copies.arrived(number, region(ref, m, other, quarter(*spot)))
    copies.arrived(last, rows_of(all_cot, 2 * tok + (1 - c) * tok, tok))
    copies.finish()
    for copy in own:
        copy.wait()


def fetch(w_qkv, w_o, w_gate, w_up, cot, shards):
    ff = w_gate.shape[1] // shards
    shapes = [
        (shards * w_qkv.shape[0], w_qkv.shape[1]),
        (shards * w_o.shape[0], w_o.shape[1]),
        (shards * w_gate.shape[0], 2 * ff),
        (shards * cot.shape[0], cot.shape[1]),
    ]
    return pl.pallas_call(
        fetch_kernel,
        out_shape=[jax.ShapeDtypeStruct(shape, bf16) for shape in shapes],
        in_specs=[pl.BlockSpec(memory_space=pl.ANY)] * 5,
        out_specs=[pl.BlockSpec(memory_space=pl.ANY)] * 4,
        scratch_shapes=[
            pltpu.SemaphoreType.DMA((40,)),
            pltpu.SemaphoreType.DMA((40,)),
            pltpu.SemaphoreType.DMA((5,)),
        ]
        + [pltpu.VMEM(a.shape, bf16) for a in (w_qkv, w_o)]
        + [pltpu.VMEM((w_gate.shape[0], ff), bf16)] * 2
        + [pltpu.VMEM(cot.shape, bf16)],
        compiler_params=pltpu.CompilerParams(collective_id=1, has_side_effects=True),
        name="fetch",
    )(w_qkv, w_o, w_gate, w_up, cot)


def slice_shape(shape, parts):
    rows, cols = shape
    down = min(parts, rows // 16)
    across = parts // down
    assert rows % down == 0 and cols % (128 * across) == 0, "unsupported sizes"
    return rows // down, cols // across, across


def halves_of(ref):
    w = ref.shape[1] // 2
    return ref.at[:, pl.ds(0, w)], ref.at[:, pl.ds(w, w)]


class Ring:
    def __init__(self, R, chunks, outs, slots, sums, spread, sent, kept):
        self.R, self.chunks, self.outs, self.slots = R, chunks, outs, slots
        self.sums, self.spread, self.sent, self.kept = sums, spread, sent, kept
        r, self.s = lax.axis_index("replica"), lax.axis_index("shard")
        z, x = lax.div(r, 2), lax.rem(r, 2)
        self.place = z * (1 - x) + (R - 1 - z) * x
        self.peers = [self.replica_at(self.place + 1), self.replica_at(self.place + R - 1)]

    def replica_at(self, place):
        R = self.R
        place = lax.rem(place, R)
        back = lax.div(place, R // 2)
        return (1 - back) * 2 * place + back * (2 * (R - 1 - place) + 1)

    def part(self, halves, way, step):
        R, ref = self.R, halves[way]
        number = lax.rem(self.place + (R - step if way == 0 else step), R)
        h, w, across = slice_shape(ref.shape, R)
        return ref.at[
            pl.ds(pl.multiple_of(lax.div(number, across) * h, 16), h),
            pl.ds(pl.multiple_of(lax.rem(number, across) * w, 128), w),
        ]

    def copy(self, a, way, step, src, dst, arrival):
        return pltpu.make_async_remote_copy(
            src_ref=src,
            dst_ref=dst,
            send_sem=self.sent.at[a, way, lax.rem(step, 2)],
            recv_sem=arrival,
            device_id=(self.peers[way], self.s),
            device_id_type=pl.DeviceIdType.MESH,
        )

    def send(self, a, way, step, src, dst, arrival, free=True):
        copy = self.copy(a, way, step, src, dst, arrival)
        if free:
            copy.wait_send()
        copy.start()

    def start(self, a):
        for way in (0, 1):
            src = self.part(self.chunks[a], way, 0)
            self.send(a, way, 0, src, self.slots[a].at[way, 0], self.sums.at[a, way, 0], False)

    def sum_step(self, a, k, last=False, first=False):
        for way in (0, 1):
            slot = self.slots[a].at[way, k - 1]
            self.copy(a, way, 0, slot, slot, self.sums.at[a, way, k - 1]).wait_recv()
            own = self.part(self.chunks[a], way, k)
            slot[...] = (slot[...].astype(f32) + own[...].astype(f32)).astype(bf16)
            if last:
                dst = self.part(self.outs[a], way, k)
                self.send(a, way, k, slot, dst, self.spread.at[a, way, 0])
                pltpu.make_async_copy(slot, dst, self.kept.at[a, way]).start()
            else:
                self.send(a, way, k, slot, self.slots[a].at[way, k], self.sums.at[a, way, k], not first)

    def spread_step(self, a, k, last=False):
        for way in (0, 1):
            dst = self.part(self.outs[a], way, lax.rem(k + self.R - 1, self.R))
            self.copy(a, way, 0, dst, dst, self.spread.at[a, way, k - 1]).wait_recv()
            if not last:
                self.send(a, way, k + self.R - 1, dst, dst, self.spread.at[a, way, k])

    def finish(self, a):
        for way in (0, 1):
            slot = self.slots[a].at[way, self.R - 2]
            for step in (0, 1):
                self.copy(a, way, step, slot, slot, self.sums.at[a, way, 0]).wait_send()
            dst = self.part(self.outs[a], way, self.R - 1)
            pltpu.make_async_copy(slot, dst, self.kept.at[a, way]).wait()


class Product:
    def __init__(self, left, right, out, tile=256):
        self.left, self.right, self.out, self.tile = left, right, out, tile
        self.tiles = out.shape[1] // tile

    def do(self, i):
        columns = pl.ds(pl.multiple_of(i * self.tile, 128), self.tile)
        self.out[:, columns] = jnp.dot(
            self.left[...], self.right[:, columns], preferred_element_type=f32
        ).astype(bf16)

    def do_all(self):
        @pl.loop(0, self.tiles)
        def _(i):
            self.do(i)

    def do_some(self, k, steps):
        each = -(-self.tiles // steps)
        for j in range(each):
            i = (k - 1) * each + j

            @pl.when(i < self.tiles)
            def _():
                self.do(i)


def finish_kernel(
    R, down, near_t, far_t, gu_own, gh, ctx_t, one_t, gq, gains,
    out_gate, out_up, out_o, out_qkv, out_down, out_gains,
    chunk0, chunk1, chunk2, chunk3, chunk_o, chunk_q,
    slot0, slot1, slot2, slot3, slot_o, slot_q, slot_d0, slot_d1,
    gu_near, gu_row, gu_diag, all_gh, all_ctx, all_one, all_gq, gain_in, gain_all,
    sums, spread, sent, kept, send, recv, gain_send, gain_recv,
):
    r, s = lax.axis_index("replica"), lax.axis_index("shard")
    c, y = lax.rem(s, 2), lax.div(s, 2)
    near, row = 2 * y + 1 - c, 2 * (1 - y) + c
    diagonal = 2 * (1 - y) + 1 - c
    shard_of = (s, near, row, diagonal)
    core_dev, row_dev, diag_dev = (r, near), (r, row), (r, diagonal)
    ff = gu_own.shape[1] // 2
    units = [pl.ds(pl.multiple_of(shard_of[j] * ff, 128), ff) for j in range(4)]
    half_d = down.shape[0] // 2
    outs = [(out_gate.at[:, cols], out_up.at[:, cols]) for cols in units]
    outs += [halves_of(ref) for ref in (out_o, out_qkv)]
    outs += [halves_of(out_down.at[pl.ds(k * half_d, half_d)]) for k in (0, 1)]
    chunks = [halves_of(ref) for ref in (chunk0, chunk1, chunk2, chunk3, chunk_o, chunk_q)]
    chunks += [halves_of(down.at[pl.ds(k * half_d, half_d)]) for k in (0, 1)]
    ring = Ring(
        R, chunks, outs, [slot0, slot1, slot2, slot3, slot_o, slot_q, slot_d0, slot_d1],
        sums, spread, sent, kept,
    )

    barrier = pltpu.get_barrier_semaphore()
    for other in (near, row, diagonal):
        pl.semaphore_signal(
            barrier, inc=1, device_id=(r, other), device_id_type=pl.DeviceIdType.MESH
        )

    @pl.loop(1, R)
    def _(d):
        pl.semaphore_signal(
            barrier, inc=1, device_id=(lax.rem(r + d, R), s), device_id_type=pl.DeviceIdType.MESH
        )

    pl.semaphore_wait(barrier, R + 2)

    copies = Copies(send, recv)
    tok, rows, head_rows = gh.shape[0], near_t.shape[0], chunk_o.shape[0]

    def block(ref, j):
        return ref.at[pl.ds(j * tok, tok)]

    def columns(ref, j):
        return ref.at[:, pl.ds(j * tok, tok)]

    def strip(ref, shard, size):
        return ref.at[pl.ds(pl.multiple_of(shard * size, 16), size)]

    core_gu = copies.start(gu_own, gu_near, core_dev)
    row_gh = copies.start(gh, block(all_gh, 2), row_dev)
    row_gq = copies.start(gq, block(all_gq, 2), row_dev)
    small = []
    for j, device in ((2, row_dev), (3, diag_dev), (1, core_dev)):
        small.append((copies.start(strip(ctx_t, shard_of[j], head_rows), columns(all_ctx, j), device), columns(all_ctx, j)))
        small.append((copies.start(strip(one_t, shard_of[j], rows), columns(all_one, j), device), columns(all_one, j)))
        mine = gains.at[:, pl.ds(pl.multiple_of(shard_of[j] * rows, 128), rows)]
        small.append((copies.start(mine, gain_in.at[j], device), gain_in.at[j]))
    near_gh = copies.start(gh, block(all_gh, 1), core_dev)
    near_gq = copies.start(gq, block(all_gq, 1), core_dev)
    row_gu = copies.start(gu_own, gu_row, row_dev)

    products = [
        Product(near_t, gu_own, chunk0),
        Product(near_t, gu_near, chunk1),
        Product(far_t, gu_row, chunk2),
        Product(far_t, gu_diag, chunk3),
        Product(all_ctx, all_gh, chunk_o),
        Product(all_one, all_gq, chunk_q),
    ]
    for a in (6, 7):
        ring.start(a)

    block(all_gh, 0)[...] = gh[...]
    block(all_gq, 0)[...] = gq[...]
    all_ctx[:, 0:tok] = strip(ctx_t, s, head_rows)[...]
    all_one[:, 0:tok] = strip(one_t, s, rows)[...]

    def sum_phase(pair):
        for a in pair:
            ring.sum_step(a, 1, first=True)

        @pl.loop(2, R - 1)
        def _(k):
            for a in pair:
                ring.sum_step(a, k)

        for a in pair:
            ring.sum_step(a, R - 1, last=True)

    def spread_phase(pair, following):
        @pl.loop(1, R - 1)
        def _(k):
            for a in pair:
                ring.spread_step(a, k)
            for a in following:
                products[a].do_some(k, R - 2)

        for a in following:
            ring.start(a)
        for a in pair:
            ring.spread_step(a, R - 1, last=True)

    sum_phase((6, 7))
    copies.arrived(core_gu, gu_near)
    spread_phase((6, 7), (0, 1))
    sum_phase((0, 1))

    copies.arrived(row_gh, block(all_gh, 2))
    far_gh = copies.start(block(all_gh, 2), block(all_gh, 3), core_dev)
    copies.arrived(row_gq, block(all_gq, 2))
    far_gq = copies.start(block(all_gq, 2), block(all_gq, 3), core_dev)
    for number, landed in small:
        copies.arrived(number, landed)
    mine = gains[:, pl.ds(pl.multiple_of(s * rows, 128), rows)]
    gain_all[r] = mine + gain_in[1] + (gain_in[2] + gain_in[3])

    def gain_copy(d):
        return pltpu.make_async_remote_copy(
            src_ref=gain_all.at[r],
            dst_ref=gain_all.at[r],
            send_sem=gain_send.at[d],
            recv_sem=gain_recv.at[d],
            device_id=(lax.rem(r + d, R), s),
            device_id_type=pl.DeviceIdType.MESH,
        )

    @pl.loop(1, R)
    def _(d):
        gain_copy(d).start()

    copies.arrived(near_gh, block(all_gh, 1))
    copies.arrived(near_gq, block(all_gq, 1))
    copies.arrived(far_gh, block(all_gh, 3))
    copies.arrived(far_gq, block(all_gq, 3))
    spread_phase((0, 1), (4, 5))
    copies.arrived(row_gu, gu_row)
    diag_gu = copies.start(gu_row, gu_diag, core_dev)
    sum_phase((4, 5))
    copies.arrived(diag_gu, gu_diag)
    spread_phase((4, 5), (2, 3))
    sum_phase((2, 3))
    spread_phase((2, 3), ())

    @pl.loop(1, R)
    def _(d):
        source = lax.rem(r + R - d, R)
        landed = gain_all.at[source]
        pltpu.make_async_copy(landed, landed, gain_recv.at[d]).wait()
        gain_copy(d).wait_send()

    total = gain_all[0]
    for q in range(1, R):
        total = total + gain_all[q]
    out_gains[...] = total
    for a in range(8):
        ring.finish(a)
    copies.finish()


def finish(R, down, near_t, far_t, gu_own, gh, ctx_t, one_t, gq, gains):
    rows, tokens = near_t.shape
    tok, width = gh.shape
    S = tokens // tok
    head_rows = ctx_t.shape[0] // S
    chunk = (rows, gu_own.shape[1])
    chunk_o, chunk_q = (head_rows, width), (rows, gq.shape[1])
    shapes = [chunk] * 4 + [chunk_o, chunk_q]
    part_d = (down.shape[0] // 2, down.shape[1])
    slots = [
        (2, R - 1) + slice_shape((shape[0], shape[1] // 2), R)[:2] for shape in shapes + [part_d] * 2
    ]
    full = (rows, S * chunk[1] // 2)
    vmem = lambda shape, dtype=bf16: pltpu.VMEM(shape, dtype)
    dma = pltpu.SemaphoreType.DMA
    return pl.pallas_call(
        functools.partial(finish_kernel, R),
        out_shape=[jax.ShapeDtypeStruct(shape, bf16) for shape in (full, full, chunk_o, chunk_q, down.shape)]
        + [jax.ShapeDtypeStruct((2, rows), f32)],
        in_specs=[pl.BlockSpec(memory_space=pltpu.VMEM)] * 9,
        out_specs=[pl.BlockSpec(memory_space=pl.ANY)] * 5
        + [pl.BlockSpec(memory_space=pltpu.VMEM)],
        scratch_shapes=[vmem(shape) for shape in shapes]
        + [vmem(shape) for shape in slots]
        + [
            vmem(gu_own.shape),
            vmem(gu_own.shape),
            vmem(gu_own.shape),
            vmem((tokens, width)),
            vmem((head_rows, tokens)),
            vmem((rows, tokens)),
            vmem((tokens, gq.shape[1])),
            vmem((S, 2, rows), f32),
            vmem((R, 2, rows), f32),
            dma((8, 2, R - 1)),
            dma((8, 2, R - 1)),
            dma((8, 2, 2)),
            dma((8, 2)),
            dma((20,)),
            dma((20,)),
            dma((R,)),
            dma((R,)),
        ],
        compiler_params=pltpu.CompilerParams(
            collective_id=2, has_side_effects=True, vmem_limit_bytes=62 * 2**20
        ),
        name="finish",
    )(down, near_t, far_t, gu_own, gh, ctx_t, one_t, gq, gains)


def per_device(
    fabric,
    tokens_in,
    cotangent,
    segment_ids,
    attn_gain,
    w_query,
    w_key,
    w_value,
    w_output,
    mlp_gain,
    w_gate,
    w_up,
    w_down,
):
    fabric.place()
    s, S = fabric.s, fabric.S
    batches, length, width = tokens_in.shape
    tokens = batches * length
    rows = w_query.shape[0]
    q_cols, kv_cols = w_query.shape[1], w_key.shape[1]
    head_rows = w_output.shape[0]
    ff_rows = w_down.shape[0]
    query_heads = q_cols // HD
    group_size = query_heads // KV
    scaling = 1.0 / math.sqrt(HD)

    grad_out = cotangent.reshape(tokens, width)
    w_qkv, w_out, w_gu, cot = fetch(
        jnp.concatenate([w_query, w_key, w_value], axis=1), w_output, w_gate, w_up, grad_out, S
    )
    gains = jnp.stack([attn_gain, mlp_gain]).astype(f32)
    gains = fabric.gather_gains(gains)
    gain_one, gain_two = gains[0], gains[1]

    flat_in = tokens_in.reshape(tokens, width).astype(f32)
    inv_attn = lax.rsqrt(jnp.mean(flat_in * flat_in, axis=1, keepdims=True) + epsilon)
    normed_one = (flat_in * inv_attn * gain_one).astype(bf16)
    cosine, sine_tab = rotary_tables(segment_ids, HD)
    qkv = matmul(normed_one, w_qkv)
    query_raw = qkv[:, :q_cols].reshape(batches, length, query_heads, HD)
    key_raw = qkv[:, q_cols : q_cols + kv_cols].reshape(batches, length, KV, HD)
    value_rows = qkv[:, q_cols + kv_cols :].astype(bf16).reshape(batches, length, KV, HD)
    query_rot = (
        rotate(query_raw, cosine, sine_tab)
        .astype(bf16)
        .reshape(batches, length, KV, group_size, HD)
    )
    key_rot = rotate(key_raw, cosine, sine_tab).astype(bf16)
    attn_mask = mask_of(segment_ids)
    scores = jnp.where(
        attn_mask, contract("bqkgd,bskd->bkgqs", query_rot, key_rot) * scaling, neg_large
    )
    row_max = jnp.max(scores, axis=-1, keepdims=True)
    exp_scores = jnp.exp(scores - row_max)
    row_total = jnp.sum(exp_scores, axis=-1, keepdims=True)
    log_sum = row_max + jnp.log(row_total)
    attn_probs = (exp_scores / row_total).astype(bf16)
    context = (
        contract("bkgqs,bskd->bqkgd", attn_probs, value_rows).astype(bf16).reshape(tokens, q_cols)
    )
    hidden = flat_in + matmul(context, w_out)
    inv_mlp = lax.rsqrt(jnp.mean(hidden * hidden, axis=1, keepdims=True) + epsilon)
    normed_two = (hidden * inv_mlp * gain_two).astype(bf16)

    two_a, two_b = fabric.gather_tokens(normed_two)

    def hidden_units(two):
        gu = matmul(two, w_gu)
        gate_pre, up_pre = gu[:, :ff_rows], gu[:, ff_rows:]
        return gate_pre, up_pre, (jax.nn.silu(gate_pre) * up_pre).astype(bf16)

    gate_a, up_a, act_a = hidden_units(two_a)
    gate_b, up_b, act_b = hidden_units(two_b)
    act = jnp.concatenate([act_a, act_b], axis=0)
    half = cot.shape[0] // 2

    grad_down = matmul_tn(act, cot).astype(bf16)
    half_rows = ff_rows // 2
    down_first = lax.psum(grad_down[:half_rows], "replica")

    def grads_of(gate_pre, up_pre, cot_half):
        grad_act = matmul_nt(cot_half, w_down)
        sigmoid_gate = jax.nn.sigmoid(gate_pre)
        grad_gate = (
            grad_act * up_pre * sigmoid_gate * (1.0 + gate_pre * (1.0 - sigmoid_gate))
        ).astype(bf16)
        grad_up = (grad_act * (gate_pre * sigmoid_gate)).astype(bf16)
        return jnp.concatenate([grad_gate, grad_up], axis=1)

    gu_a = grads_of(gate_a, up_a, cot[:half])
    gu_b = grads_of(gate_b, up_b, cot[half:])
    grad_two = fabric.scatter_tokens(matmul_nt(gu_a, w_gu), matmul_nt(gu_b, w_gu))
    gu_own = jnp.concatenate([gu_a, gu_b], axis=0)

    own_a = cut(two_a, s * rows, rows, 1).T
    own_b = cut(two_b, s * rows, rows, 1).T
    near_t = jnp.concatenate([own_a, own_b], axis=1)
    far_t = jnp.concatenate([own_b, own_a], axis=1)

    out_part_a = matmul(act_a, w_down)
    out_part_b = matmul(act_b, w_down)
    tokens_out = (hidden + fabric.scatter_tokens(out_part_a, out_part_b)).astype(bf16)

    part_mlp_gain = jnp.sum(grad_two * hidden * inv_mlp, axis=0)
    scaled_two = grad_two * gain_two
    grad_hidden = grad_out.astype(f32) + inv_mlp * (
        scaled_two
        - hidden * inv_mlp * inv_mlp * jnp.mean(scaled_two * hidden, axis=1, keepdims=True)
    )
    grad_hid_bf = grad_hidden.astype(bf16)
    grad_context = (
        matmul_nt(grad_hid_bf, w_out).astype(bf16).reshape(batches, length, KV, group_size, HD)
    )
    scores = jnp.where(
        attn_mask, contract("bqkgd,bskd->bkgqs", query_rot, key_rot) * scaling, neg_large
    )
    probs_full = jnp.exp(scores - log_sum)
    grad_value_rows = contract("bkgqs,bqkgd->bskd", probs_full.astype(bf16), grad_context)
    grad_probs = contract("bqkgd,bskd->bkgqs", grad_context, value_rows)
    context_five = context.reshape(batches, length, KV, group_size, HD).astype(f32)
    row_dot = jnp.sum(grad_context.astype(f32) * context_five, axis=-1)
    row_dot = jnp.transpose(row_dot, (0, 2, 3, 1))[..., None]
    grad_scores = (probs_full * (grad_probs - row_dot) * scaling).astype(bf16)
    grad_q_rot = contract("bkgqs,bskd->bqkgd", grad_scores, key_rot).reshape(
        batches, length, query_heads, HD
    )
    grad_k_rot = contract("bkgqs,bqkgd->bskd", grad_scores, query_rot)
    grad_q_in = rotate_back(grad_q_rot, cosine, sine_tab).astype(bf16).reshape(tokens, q_cols)
    grad_k_in = rotate_back(grad_k_rot, cosine, sine_tab).astype(bf16).reshape(tokens, kv_cols)
    grad_v_in = grad_value_rows.astype(bf16).reshape(tokens, kv_cols)
    grad_qkv = jnp.concatenate([grad_q_in, grad_k_in, grad_v_in], axis=1)

    grad_one = matmul_nt(grad_qkv, w_qkv)
    part_attn_gain = jnp.sum(grad_one * flat_in * inv_attn, axis=0)
    scaled_one = grad_one * gain_one
    grad_tokens = grad_hidden + inv_attn * (
        scaled_one
        - flat_in * inv_attn * inv_attn * jnp.mean(scaled_one * flat_in, axis=1, keepdims=True)
    )
    grad_gate, grad_up, grad_o, sum_qkv, down_last, gain_sums = finish(
        fabric.R,
        grad_down[half_rows:],
        near_t,
        far_t,
        gu_own,
        grad_hid_bf,
        context.T,
        normed_one.T,
        grad_qkv,
        jnp.stack([part_attn_gain, part_mlp_gain]),
    )

    return (
        tokens_out.reshape(tokens_in.shape),
        grad_tokens.astype(bf16).reshape(tokens_in.shape),
        gain_sums[0],
        sum_qkv[:, :q_cols].astype(f32),
        sum_qkv[:, q_cols : q_cols + kv_cols].astype(f32),
        sum_qkv[:, q_cols + kv_cols :].astype(f32),
        grad_o.astype(f32),
        gain_sums[1],
        grad_gate.astype(f32),
        grad_up.astype(f32),
        jnp.concatenate([down_first, down_last], axis=0).astype(f32),
    )


def solution(mesh):
    fabric = Fabric(mesh)
    data = P(AXES, None, None)
    rowwise = P("shard", None)
    flat = P("shard")
    return jax.shard_map(
        lambda *args: per_device(fabric, *args),
        mesh=mesh,
        in_specs=(
            (data, data, P(AXES, None), flat)
            + (rowwise,) * 4
            + (flat,)
            + (rowwise,) * 3
        ),
        out_specs=(data, data, flat) + (rowwise,) * 4 + (flat,) + (rowwise,) * 3,
        check_vma=False,
    )
```

```python
import functools
import math
import types

import jax
import jax.numpy as jnp
from jax import lax
from jax.experimental import pallas as pl
from jax.experimental.pallas import tpu as pltpu
from jax.sharding import PartitionSpec as P

KV = 4
HD = 64

epsilon = 1e-05
theta_base = 500000.0
neg_large = -1e30


AXES = ("replica", "shard")
f32 = jnp.float32
bf16 = jnp.bfloat16


def matmul(left_arr, right_arr):
    return jnp.dot(left_arr, right_arr, preferred_element_type=f32)


def matmul_nt(left_arr, right_arr):
    return lax.dot_general(
        left_arr, right_arr, (((1,), (1,)), ((), ())), preferred_element_type=f32
    )


def matmul_tn(left_arr, right_arr):
    return lax.dot_general(
        left_arr, right_arr, (((0,), (0,)), ((), ())), preferred_element_type=f32
    )


class Copies:
    def __init__(self, send, recv):
        self.send, self.recv, self.count, self.open = send, recv, 0, []

    def start(self, src, dst, device):
        copy = pltpu.make_async_remote_copy(
            src_ref=src,
            dst_ref=dst,
            send_sem=self.send.at[self.count],
            recv_sem=self.recv.at[self.count],
            device_id=device,
            device_id_type=pl.DeviceIdType.MESH,
        )
        self.count += 1
        copy.start()
        self.open.append(copy)
        return self.count - 1

    def arrived(self, number, landed):
        pltpu.make_async_copy(landed, landed, self.recv.at[number]).wait()

    def finish(self):
        for copy in self.open:
            copy.wait_send()
        self.open = []


def meet(devices):
    barrier = pltpu.get_barrier_semaphore()
    for device in devices:
        pl.semaphore_signal(
            barrier, inc=1, device_id=device, device_id_type=pl.DeviceIdType.MESH
        )
    pl.semaphore_wait(barrier, len(devices))


def forward_kernel(keys, *refs):
    given = iter(refs)
    h, o, v = (types.SimpleNamespace(**{key: next(given) for key in group}) for group in keys)
    r, s = lax.axis_index("replica"), lax.axis_index("shard")
    c, y = lax.rem(s, 2), lax.div(s, 2)
    x = lax.rem(r, 2)
    w = lax.rem(lax.div(r, 2), 2)
    near, row = 2 * y + 1 - c, 2 * (1 - y) + c
    diagonal = 2 * (1 - y) + 1 - c
    core_dev, row_dev, diag_dev = (r, near), (r, row), (r, diagonal)
    x_dev, z_dev = (r + 1 - 2 * x, s), (r + 2 - 4 * w, s)
    copies = Copies(v.send, v.recv)
    loads, saves = [], []

    def move(source, into, kind, sems):
        copy = pltpu.make_async_copy(source, into, sems.at[len(kind)])
        kind.append(copy)
        copy.start()
        return copy

    def load(source, into):
        return move(source, into, loads, v.loaded)

    def save(source, into):
        return move(source, into, saves, v.saved)

    tok, width = h.x.shape
    ff = v.all_gu.shape[1] // 2
    q_cols, kv_cols = v.q.shape[1], v.all_kv.shape[1] // 2
    m_g = h.w_gate.shape[0]
    q_g = m_g // 4

    def rows_of(ref, start, size):
        return ref.at[pl.ds(pl.multiple_of(start, 16), size)]

    def region(ref, m, owner, spot):
        return rows_of(ref, owner * m + spot * (m // 4), m // 4)

    def columns_of(ref, start, size, shard):
        return ref.at[
            pl.ds(pl.multiple_of(start, 16), size), pl.ds(pl.multiple_of(shard * ff, 128), ff)
        ]

    def quarter(flip_x, flip_z):
        at_x = (1 - x) if flip_x else x
        at_z = (1 - w) if flip_z else w
        return 2 * at_z + at_x

    here = quarter(0, 0)

    def gu_part(owner, start, size):
        return [
            v.all_gu.at[pl.ds(pl.multiple_of(owner * m_g + start, 16), size), pl.ds(k * ff, ff)]
            for k in (0, 1)
        ]

    load_x = load(h.x, v.x_in)
    load_gain = load(h.gain, v.gain.at[:, pl.ds(pl.multiple_of(s * m_g, 128), m_g)])
    plain = [(h.w_q, v.all_q, True), (h.w_kv, v.all_kv, False), (h.w_o, v.all_o, True)]
    load_own = [load(a, rows_of(b, s * a.shape[0], a.shape[0])) for a, b, _ in plain]
    load_small = [load(h.segments, v.segments), load(h.speed, v.speed)]
    own_cot = rows_of(v.all_cot, c * tok, tok)
    load_gu = [
        load(columns_of(a, 0, m_g, s), part)
        for a, part in zip((h.w_gate, h.w_up), gu_part(s, 0, m_g))
    ]
    load_gu += [load(h.cot, own_cot), load(h.w_down, v.w_down)]

    meet([core_dev, row_dev, diag_dev, x_dev, z_dev])

    flows, first = [], []
    for a, b, x_first in plain:
        m = a.shape[0]
        part = rows_of(a, here * (m // 4), m // 4)
        first.append([copies.start(part, region(b, m, s, here), row_dev)])
        flows.append((b, m, row, True, x_first))
    gain_parts = []
    for device, owner in ((core_dev, near), (row_dev, row), (diag_dev, diagonal)):
        mine = v.gain.at[:, pl.ds(pl.multiple_of(s * m_g, 128), m_g)]
        landed = v.gain.at[:, pl.ds(pl.multiple_of(owner * m_g, 128), m_g)]
        gain_parts.append((copies.start(h.gain, mine, device), landed))
    for shard, device, x_first in ((row, row_dev, True), (diagonal, diag_dev, False)):
        first.append(
            [
                copies.start(columns_of(a, here * q_g, q_g, shard), part, device)
                for a, part in zip((h.w_gate, h.w_up), gu_part(s, here * q_g, q_g))
            ]
        )
        flows.append((v.all_gu, m_g, shard, False, x_first))
    far_cot = rows_of(v.all_cot, 2 * tok + c * tok, tok)
    row_cot = copies.start(h.cot, far_cot, row_dev)

    core_plain = []
    for a, b, _ in plain:
        m = a.shape[0]
        core_plain.append((copies.start(a, rows_of(b, s * m, m), core_dev), rows_of(b, near * m, m)))
    core_gu = [
        (copies.start(columns_of(a, 0, m_g, near), part, core_dev), landed)
        for a, part, landed in zip(
            (h.w_gate, h.w_up), gu_part(s, 0, m_g), gu_part(near, 0, m_g)
        )
    ]
    core_gu.append(
        (copies.start(h.cot, own_cot, core_dev), rows_of(v.all_cot, (1 - c) * tok, tok))
    )

    second, third = {}, {}
    forwarded = {i: [] for i in range(len(flows))}

    def to_core(i, part, spot):
        if flows[i][3]:
            forwarded[i].append((copies.start(part, part, core_dev), spot))

    def stage(i, number):
        ref, m, owner, _, x_first = flows[i]
        flip = (1, 0) if x_first else (0, 1)
        one, two = (x_dev, z_dev) if x_first else (z_dev, x_dev)
        if number == 1:
            piece = region(ref, m, owner, here)
            if len(first[i]) == 1:
                copies.arrived(first[i][0], piece)
            else:
                for sent, part in zip(first[i], gu_part(owner, here * q_g, q_g)):
                    copies.arrived(sent, part)
            second[i] = copies.start(piece, piece, one)
            to_core(i, piece, (0, 0))
        elif number == 2:
            piece, other = region(ref, m, owner, here), region(ref, m, owner, quarter(*flip))
            copies.arrived(second[i], other)
            third[i] = [
                (copies.start(part, part, two), spot)
                for part, spot in ((piece, (0, 0)), (other, flip))
            ]
            to_core(i, other, flip)
        elif number == 3:
            for sent, (fx, fz) in third[i]:
                spot = (fx, 1 - fz) if x_first else (1 - fx, fz)
                part = region(ref, m, owner, quarter(*spot))
                copies.arrived(sent, part)
                to_core(i, part, spot)
        else:
            for sent, spot in forwarded[i]:
                copies.arrived(sent, region(ref, m, diagonal, quarter(*spot)))

    step = 32

    def at_rows(i):
        return pl.ds(pl.multiple_of(i * step, step), step)

    def norm(source, which, into):
        @pl.loop(0, tok // step)
        def _(i):
            b = at_rows(i)
            values = source[b].astype(f32)
            inv = lax.rsqrt(jnp.mean(values * values, axis=1, keepdims=True) + epsilon)
            into[b] = (values * inv * v.gain[which : which + 1]).astype(bf16)

    load_x.wait()
    load_gain.wait()
    for sent, landed in gain_parts:
        copies.arrived(sent, landed)
    norm(v.x_in, 0, v.one)
    save(v.one, o.one)
    for copy in load_own + load_small:
        copy.wait()

    along = jnp.broadcast_to(v.segments[...], (tok, tok))
    query_at = lax.broadcasted_iota(jnp.int32, (tok, tok), 0)
    key_at = lax.broadcasted_iota(jnp.int32, (tok, tok), 1)
    allowed = (along.T == along) & (query_at >= key_at)
    v.mask[...] = jnp.where(allowed, 1.0, 0.0)
    position = jnp.sum(v.mask[...], axis=1, keepdims=True) - 1.0
    angle = position * v.speed[...]
    lane = lax.broadcasted_iota(jnp.int32, (tok, 2 * HD), 1)
    front = lane < HD
    lower = lax.rem(lane, HD) < HD // 2
    v.cos[...] = jnp.cos(angle)
    sine = jnp.sin(angle)
    v.sin[...] = jnp.where(lower, sine, -sine)
    save(v.mask, o.mask)
    save(v.cos, o.cos)
    save(v.sin, o.sin)
    stage(0, 1)
    stage(1, 1)
    stage(0, 2)
    stage(1, 2)
    stage(2, 1)
    stage(1, 3)
    stage(0, 3)
    for sent, landed in core_plain:
        copies.arrived(sent, landed)
    stage(3, 1)
    stage(2, 2)
    stage(0, 4)
    stage(1, 4)

    def turn(part):
        other = jnp.where(lower, pltpu.roll(part, 2 * HD - HD // 2, 1), pltpu.roll(part, HD // 2, 1))
        return part * v.cos[...] - other * v.sin[...]

    def lanes_of(i):
        return pl.ds(pl.multiple_of(i * 2 * HD, 128), 2 * HD)

    @pl.loop(0, q_cols // 256)
    def _(i):
        part = matmul(v.one[...], v.all_q[:, pl.ds(pl.multiple_of(i * 256, 128), 256)])
        for j in (0, 1):
            half = part[:, j * 2 * HD : (j + 1) * 2 * HD]
            v.q[:, lanes_of(2 * i + j)] = turn(half).astype(bf16)

    for which, into in ((0, v.k), (1, v.v)):
        part = matmul(v.one[...], v.all_kv[:, which * kv_cols : (which + 1) * kv_cols])
        for j in range(kv_cols // (2 * HD)):
            half = part[:, j * 2 * HD : (j + 1) * 2 * HD]
            half = turn(half) if which == 0 else half
            swapped = pltpu.roll(half, HD, 1)
            into[2 * j] = jnp.where(front, half, swapped).astype(bf16)
            into[2 * j + 1] = jnp.where(front, swapped, half).astype(bf16)
    save(v.q, o.q)
    save(v.k, o.k)
    save(v.v, o.v)
    save(v.all_q, o.w_qkv.at[:, pl.ds(0, q_cols)])
    save(v.all_kv, o.w_qkv.at[:, pl.ds(q_cols, 2 * kv_cols)])
    stage(4, 1)

    group = q_cols // kv_cols
    scaling = 1.0 / math.sqrt(HD)

    def head_pair(u):
        kv = lax.div(2 * u, group)
        query, keys, values = v.q[:, lanes_of(u)], v.k[kv], v.v[kv]
        allowed = v.mask[...] > 0
        zero = jnp.zeros_like(query)
        context = jnp.zeros((tok, 2 * HD), f32)
        for e in (0, 1):
            own = front if e == 0 else jnp.logical_not(front)
            scores = jnp.where(
                allowed, matmul_nt(jnp.where(own, query, zero), keys) * scaling, neg_large
            )
            top = jnp.max(scores, axis=1, keepdims=True)
            weight = jnp.exp(scores - top)
            probs = (weight / jnp.sum(weight, axis=1, keepdims=True)).astype(bf16)
            context += matmul(probs, jnp.where(own, values, zero))
        v.ctx[:, lanes_of(u)] = context.astype(bf16)

    pairs = q_cols // (2 * HD)

    @pl.loop(0, pairs // 2)
    def _(u):
        head_pair(u)

    stage(3, 2)

    @pl.loop(pairs // 2, pairs)
    def _(u):
        head_pair(u)

    save(v.ctx, o.ctx)
    stage(2, 3)
    stage(2, 4)
    save(v.all_o, o.w_o)

    @pl.loop(0, width // 256)
    def _(i):
        columns = pl.ds(pl.multiple_of(i * 256, 128), 256)
        v.hid[:, columns] = v.x_in[:, columns].astype(f32) + matmul(v.ctx[...], v.all_o[:, columns])

    stage(4, 2)
    own_two = rows_of(v.two, c * tok, tok)
    norm(v.hid, 1, own_two)
    far_two = rows_of(v.two, 2 * tok + c * tok, tok)
    near_two = copies.start(own_two, own_two, core_dev)
    row_two = copies.start(own_two, far_two, row_dev)
    save(v.hid, o.hid)
    save(v.gain, o.gain)

    for copy in load_gu:
        copy.wait()
    for sent, landed in core_gu:
        copies.arrived(sent, landed)
    stage(3, 3)
    stage(4, 3)
    copies.arrived(near_two, rows_of(v.two, (1 - c) * tok, tok))

    def units(end):
        tokens = pl.ds(end * 2 * tok, 2 * tok)

        @pl.loop(0, ff // 256)
        def _(i):
            columns = pl.ds(pl.multiple_of(i * 256, 128), 256)
            ups = pl.ds(pl.multiple_of(ff + i * 256, 128), 256)
            gate = matmul(v.two[tokens], v.all_gu[:, columns])
            up = matmul(v.two[tokens], v.all_gu[:, ups])
            grad_act = matmul_nt(v.all_cot[tokens], v.w_down[pl.ds(pl.multiple_of(i * 256, 128), 256)])
            sigmoid = jax.nn.sigmoid(gate)
            silu = gate * sigmoid
            v.act[tokens, columns] = (silu * up).astype(bf16)
            v.gu[tokens, columns] = (
                grad_act * up * sigmoid * (1.0 + gate * (1.0 - sigmoid))
            ).astype(bf16)
            v.gu[tokens, ups] = (grad_act * silu).astype(bf16)

    def partial(end):
        tokens = pl.ds(end * 2 * tok, 2 * tok)

        @pl.loop(0, width // 256)
        def _(i):
            columns = pl.ds(pl.multiple_of(i * 256, 128), 256)
            v.part[tokens, columns] = matmul_nt(
                v.gu[tokens], v.all_gu[pl.ds(pl.multiple_of(i * 256, 128), 256)]
            ).astype(bf16)

    def down(end):
        tokens = pl.ds(end * 2 * tok, 2 * tok)

        @pl.loop(0, ff // 256)
        def _(i):
            units_at = pl.ds(pl.multiple_of(i * 256, 128), 256)
            turned = v.act[tokens, units_at].T

            @pl.loop(0, width // 512)
            def _(j):
                columns = pl.ds(pl.multiple_of(j * 512, 128), 512)
                part = matmul(turned, v.all_cot[tokens, columns])
                if end == 0:
                    v.sums[units_at, columns] = part
                else:
                    v.down[units_at, columns] = (v.sums[units_at, columns] + part).astype(bf16)

    def save_rows(end, *names):
        tokens = pl.ds(end * 2 * tok, 2 * tok)
        for a, b in names:
            save(a.at[tokens], b.at[tokens])

    units(0)
    copies.arrived(row_cot, far_cot)
    last_cot = copies.start(far_cot, far_cot, core_dev)
    partial(0)
    save_rows(0, (v.act, o.act), (v.gu, o.gu), (v.part, o.part), (v.two, o.two))
    down(0)
    copies.arrived(row_two, far_two)
    last_two = copies.start(far_two, far_two, core_dev)
    there = 2 * tok + (1 - c) * tok
    copies.arrived(last_cot, rows_of(v.all_cot, there, tok))
    copies.arrived(last_two, rows_of(v.two, there, tok))
    units(1)
    save_rows(1, (v.two, o.two), (v.act, o.act), (v.gu, o.gu))
    down(1)
    save(v.down, o.down)
    partial(1)
    save_rows(1, (v.part, o.part))
    copies.finish()
    for copy in saves:
        copy.wait()


def forward(S, **given):
    h = types.SimpleNamespace(**given)
    tok, width = h.x.shape
    ff, q_cols, kv_cols = h.w_down.shape[0], h.w_q.shape[1], h.w_kv.shape[1] // 2
    V = lambda shape, dtype=bf16: pltpu.VMEM(shape, dtype)
    dma = pltpu.SemaphoreType.DMA
    heads = (kv_cols // HD, tok, 2 * HD)
    many = S * tok
    outs = dict(
        w_qkv=(S * h.w_q.shape[0], q_cols + 2 * kv_cols),
        w_o=(S * h.w_o.shape[0], width),
        gain=(2, width),
        one=(tok, width),
        q=(tok, q_cols),
        k=heads,
        v=heads,
        ctx=(tok, q_cols),
        hid=(tok, width),
        two=(many, width),
        act=(many, ff),
        gu=(many, 2 * ff),
        part=(many, width),
        down=(ff, width),
        mask=(tok, tok),
        cos=(tok, 2 * HD),
        sin=(tok, 2 * HD),
    )
    scratch = dict(
        x_in=V((tok, width)),
        gain=V((2, width), f32),
        all_q=V((S * h.w_q.shape[0], q_cols)),
        all_kv=V((S * h.w_q.shape[0], 2 * kv_cols)),
        all_o=V((S * h.w_o.shape[0], width)),
        all_gu=V((S * h.w_gate.shape[0], 2 * ff)),
        all_cot=V((many, width)),
        w_down=V(h.w_down.shape),
        segments=V(h.segments.shape, h.segments.dtype),
        speed=V(h.speed.shape, f32),
        cos=V((tok, 2 * HD), f32),
        sin=V((tok, 2 * HD), f32),
        mask=V((tok, tok), f32),
        sums=V((ff, width), f32),
        down=V((ff, width)),
        one=V((tok, width)),
        q=V((tok, q_cols)),
        k=V(heads),
        v=V(heads),
        ctx=V((tok, q_cols)),
        hid=V((tok, width), f32),
        two=V((many, width)),
        act=V((many, ff)),
        gu=V((many, 2 * ff)),
        part=V((many, width)),
        send=dma((56,)),
        recv=dma((56,)),
        loaded=dma((24,)),
        saved=dma((32,)),
    )
    wide = ("hid", "gain", "mask", "cos", "sin")
    out = pl.pallas_call(
        functools.partial(forward_kernel, (tuple(given), tuple(outs), tuple(scratch))),
        out_shape=[
            jax.ShapeDtypeStruct(shape, f32 if name in wide else bf16)
            for name, shape in outs.items()
        ],
        in_specs=[pl.BlockSpec(memory_space=pl.ANY)] * len(given),
        out_specs=[pl.BlockSpec(memory_space=pl.ANY)] * len(outs),
        scratch_shapes=list(scratch.values()),
        compiler_params=pltpu.CompilerParams(
            collective_id=1, has_side_effects=True, vmem_limit_bytes=67043328
        ),
        name="forward",
    )(*given.values())
    return types.SimpleNamespace(**dict(zip(outs, out)))


def slice_shape(shape, parts):
    rows, cols = shape
    down = min(parts, rows // 16)
    across = parts // down
    assert rows % down == 0 and cols % (128 * across) == 0, "unsupported sizes"
    return rows // down, cols // across, across


def halves_of(ref):
    w = ref.shape[1] // 2
    return ref.at[:, pl.ds(0, w)], ref.at[:, pl.ds(w, w)]


class Ring:
    def __init__(self, R, chunks, outs, slots, sums, spread, sent, kept):
        self.R, self.chunks, self.outs, self.slots = R, chunks, outs, slots
        self.sums, self.spread, self.sent, self.kept = sums, spread, sent, kept
        r, self.s = lax.axis_index("replica"), lax.axis_index("shard")
        z, x = lax.div(r, 2), lax.rem(r, 2)
        self.place = z * (1 - x) + (R - 1 - z) * x
        self.peers = [self.replica_at(self.place + 1), self.replica_at(self.place + R - 1)]

    def replica_at(self, place):
        R = self.R
        place = lax.rem(place, R)
        back = lax.div(place, R // 2)
        return (1 - back) * 2 * place + back * (2 * (R - 1 - place) + 1)

    def part(self, halves, way, step):
        R, ref = self.R, halves[way]
        number = lax.rem(self.place + (R - step if way == 0 else step), R)
        h, w, across = slice_shape(ref.shape, R)
        return ref.at[
            pl.ds(pl.multiple_of(lax.div(number, across) * h, 16), h),
            pl.ds(pl.multiple_of(lax.rem(number, across) * w, 128), w),
        ]

    def slot(self, a, way, step):
        h, w, _ = slice_shape(self.chunks[a][0].shape, self.R)
        return self.slots[a].at[way, step, pl.ds(0, h), pl.ds(0, w)]

    def copy(self, a, way, step, src, dst, arrival):
        return pltpu.make_async_remote_copy(
            src_ref=src,
            dst_ref=dst,
            send_sem=self.sent.at[a, way, lax.rem(step, 2)],
            recv_sem=arrival,
            device_id=(self.peers[way], self.s),
            device_id_type=pl.DeviceIdType.MESH,
        )

    def start(self, a):
        for way in (0, 1):
            src = self.part(self.chunks[a], way, 0)
            self.copy(a, way, 0, src, self.slot(a, way, 0), self.sums.at[a, way, 0]).start()

    def sum_step(self, a, k):
        last = k == self.R - 1
        for way in (0, 1):
            slot = self.slot(a, way, k - 1)
            self.copy(a, way, 0, slot, slot, self.sums.at[a, way, k - 1]).wait_recv()
            own = self.part(self.chunks[a], way, k)
            slot[...] = (slot[...].astype(f32) + own[...].astype(f32)).astype(bf16)
            dst = self.part(self.outs[a], way, k)
            onward = self.copy(a, way, k, slot, dst, self.spread.at[a, way, 0])

            @pl.when(k >= 2)
            def _():
                self.copy(a, way, k, slot, slot, self.sums.at[a, way, 0]).wait_send()

            @pl.when(last)
            def _():
                onward.start()
                pltpu.make_async_copy(slot, dst, self.kept.at[a, way]).start()

            @pl.when(jnp.logical_not(last))
            def _():
                there = lax.rem(k, self.R - 1)
                self.copy(
                    a, way, k, slot, self.slot(a, way, there), self.sums.at[a, way, there]
                ).start()

    def spread_step(self, a, k, last=False):
        for way in (0, 1):
            dst = self.part(self.outs[a], way, lax.rem(k + self.R - 1, self.R))
            self.copy(a, way, 0, dst, dst, self.spread.at[a, way, k - 1]).wait_recv()
            if not last:
                onward = self.copy(a, way, k + self.R - 1, dst, dst, self.spread.at[a, way, k])
                onward.wait_send()
                onward.start()

    def finish(self, a):
        for way in (0, 1):
            slot = self.slot(a, way, self.R - 2)
            for step in (0, 1):
                self.copy(a, way, step, slot, slot, self.sums.at[a, way, 0]).wait_send()
            dst = self.part(self.outs[a], way, self.R - 1)
            pltpu.make_async_copy(slot, dst, self.kept.at[a, way]).wait()


def product(left, right, out, crossed=False, tile=256):
    half = right.shape[0] // 2

    def make(i):
        columns = pl.ds(pl.multiple_of(i * tile, 128), tile)
        if crossed:
            one = matmul(left[:, 0:half], right[pl.ds(half, half), columns])
            out[:, columns] = (one + matmul(left[:, half:], right[pl.ds(0, half), columns])).astype(bf16)
        else:
            out[:, columns] = matmul(left[...], right[:, columns]).astype(bf16)

    return out.shape[1] // tile, make


def backward_kernel(R, keys, *refs):
    given = iter(refs)
    h, o, v = (types.SimpleNamespace(**{key: next(given) for key in group}) for group in keys)
    r, s = lax.axis_index("replica"), lax.axis_index("shard")
    c, y = lax.rem(s, 2), lax.div(s, 2)
    near, row = 2 * y + 1 - c, 2 * (1 - y) + c
    diagonal = 2 * (1 - y) + 1 - c
    shard_of = (s, near, row, diagonal)
    core_dev, row_dev, diag_dev = (r, near), (r, row), (r, diagonal)

    barrier = pltpu.get_barrier_semaphore()
    for other in (near, row, diagonal):
        pl.semaphore_signal(
            barrier, inc=1, device_id=(r, other), device_id_type=pl.DeviceIdType.MESH
        )

    @pl.loop(1, R)
    def _(d):
        pl.semaphore_signal(
            barrier, inc=1, device_id=(lax.rem(r + d, R), s), device_id_type=pl.DeviceIdType.MESH
        )

    loads = []

    def load(source, into):
        copy = pltpu.make_async_copy(source, into, v.loaded.at[len(loads)])
        loads.append(copy)
        copy.start()
        return copy

    down, set_one, slots_a, slots_b = v.down, v.set_one, v.slots_a, v.slots_b
    gu_own, gu_near, gu_row = v.gu_own, v.gu_near, v.gu_row
    all_gh, all_gq, all_ctx, all_one = v.all_gh, v.all_gq, v.all_ctx, v.all_one
    mine_a, mine_b, got_a, got_b, got_far = v.mine_a, v.mine_b, v.got_a, v.got_b, v.got_far
    hid, x_in, cot, grad_hid = v.hid, v.x_in, v.cot, v.grad_hid
    weights, q_tiles = v.weights, v.q_tiles
    tok, width = x_in.shape
    ff = gu_own.shape[1] // 2
    rows, head_rows = v.near_t.shape[0], weights.shape[0] // len(shard_of)
    q_cols = v.q.shape[1]
    qkv_cols = all_gq.shape[1]
    kv_cols = (qkv_cols - q_cols) // 2
    half_d = down.shape[0] // 2
    scaling = 1.0 / math.sqrt(HD)

    def rows_of(a, start, size):
        return a.at[pl.ds(pl.multiple_of(start, 16), size)]

    def block(a, j):
        return a.at[pl.ds(j * tok, tok)]

    def columns(a, j, size):
        return a.at[:, pl.ds(pl.multiple_of(j * size, 128), size)]

    load_down = load(h.down, down)
    load_b = load(rows_of(h.part, 2 * tok + c * tok, tok), mine_b)
    tokens = gu_own.shape[0]
    load_gu = load(h.gu, gu_own)
    own_two = all_gq.at[:, pl.ds(0, rows)]
    load_near = load(h.two.at[:, pl.ds(pl.multiple_of(s * rows, 128), rows)], own_two)
    load_a = load(rows_of(h.part, c * tok, tok), mine_a)
    later = [
        load(source, into)
        for source, into in ((h.hid, hid), (h.x, x_in), (h.cot, cot), (h.gain, v.gain))
    ]
    load_w = load(h.w_o, weights)
    attention = [
        load(source, into)
        for source, into in (
            (h.q, v.q), (h.k, v.k), (h.v, v.v), (h.ctx, v.ctx),
            (h.mask, v.mask), (h.cos, v.cos), (h.sin, v.sin),
        )
    ]

    units = [pl.ds(pl.multiple_of(shard_of[j] * ff, 128), ff) for j in range(4)]
    outs = [(o.gate.at[:, cols], o.up.at[:, cols]) for cols in units]
    outs += [halves_of(o.o), halves_of(o.qkv)]
    outs += [halves_of(rows_of(o.down, k * half_d, half_d)) for k in (0, 1)]
    chunk = [set_one.at[0], set_one.at[1], set_one.at[0], set_one.at[1]]
    chunk += [down.at[pl.ds(0, head_rows)], down.at[pl.ds(half_d, rows), pl.ds(0, qkv_cols)]]
    chunk += [down.at[pl.ds(0, half_d)], down.at[pl.ds(half_d, half_d)]]
    ring = Ring(
        R,
        [halves_of(a) for a in chunk],
        outs,
        [slots_b.at[0], slots_b.at[1], slots_b.at[0], slots_b.at[1]]
        + [slots_a.at[0], slots_a.at[1]] * 2,
        v.sums, v.spread, v.sent, v.kept,
    )
    copies = Copies(v.send, v.recv)

    def do(work, k, steps):
        count, make = work
        each = -(-count // steps)

        @pl.loop(0, each)
        def _(j):
            i = (k - 1) * each + j

            @pl.when(i < count)
            def _():
                make(i)

    def do_all(work):
        count, make = work

        @pl.loop(0, count)
        def _(i):
            make(i)

    def sum_phase(pair, works=()):
        @pl.loop(1, R)
        def _(k):
            for a in pair:
                ring.sum_step(a, k)
            for work in works:
                do(work, k, R - 1)

    def spread_phase(pair, works=(), before=lambda: None, following=()):
        @pl.loop(1, R - 1)
        def _(k):
            for a in pair:
                ring.spread_step(a, k)
            for work in works:
                do(work, k, R - 2)

        before()
        for a in following:
            ring.start(a)
        for a in pair:
            ring.spread_step(a, R - 1, last=True)
            ring.finish(a)

    def turn_over(source, into):
        @pl.loop(0, source.shape[0] // 128)
        def _(i):
            at = pl.ds(pl.multiple_of(i * 128, 128), 128)
            into[:, at] = source[at].T

    load_down.wait()
    pl.semaphore_wait(barrier, R + 2)
    for a in (6, 7):
        ring.start(a)

    core_b = copies.start(rows_of(h.part, 2 * tok + (1 - c) * tok, tok), got_b, core_dev)
    load_near.wait()
    turn_over(own_two, v.near_t)
    core_a = copies.start(rows_of(h.part, (1 - c) * tok, tok), got_a, core_dev)
    load_b.wait()
    copies.arrived(core_b, got_b)
    mine_b[...] = (mine_b[...].astype(f32) + got_b[...].astype(f32)).astype(bf16)
    far = copies.start(mine_b, got_far, row_dev)
    load_gu.wait()
    core_gu = copies.start(gu_own, gu_near, core_dev)
    quarter = gu_own.shape[0] // 4
    row_gu = [
        copies.start(gu_own.at[pl.ds(i * quarter, quarter)], gu_row.at[pl.ds(i * quarter, quarter)], row_dev)
        for i in (0, 1)
    ]
    small = []
    for j, device in ((2, row_dev), (3, diag_dev), (1, core_dev)):
        for whole, into, size in ((h.ctx, v.in_ctx, head_rows), (h.one, v.in_one, rows)):
            source = columns(whole, shard_of[j], size)
            small.append((copies.start(source, block(into, j), device), block(into, j)))
    own_parts = [
        load(columns(h.ctx, s, head_rows), block(v.in_ctx, 0)),
        load(columns(h.one, s, rows), block(v.in_one, 0)),
    ]

    sum_phase((6, 7), (product(v.near_t, gu_own, chunk[0]),))

    load_a.wait()
    for copy in later:
        copy.wait()
    load_w.wait()
    copies.arrived(core_a, got_a)
    copies.arrived(far, got_far)
    copies.arrived(core_gu, gu_near)
    gain, gain_part = v.gain, v.gain_part
    gain_part[...] = jnp.zeros_like(gain_part)
    step = 32
    groups = step // 8

    def fold(values):
        return jnp.sum(values.reshape(groups, 8, width), axis=0)

    def at_rows(i):
        return pl.ds(pl.multiple_of(i * step, step), step)

    def residual_two(i):
        b = at_rows(i)
        two = mine_a[b].astype(f32) + got_a[b].astype(f32) + got_far[b].astype(f32)
        hidden = hid[b]
        inv = lax.rsqrt(jnp.mean(hidden * hidden, axis=1, keepdims=True) + epsilon)
        gain_part[1] += fold(two * hidden * inv)
        scaled = two * gain[1:2]
        dot = jnp.mean(scaled * hidden, axis=1, keepdims=True)
        out = cot[b].astype(f32) + inv * (scaled - hidden * inv * inv * dot)
        grad_hid[b] = out
        all_gh[b] = out.astype(bf16)

    spread_phase(
        (6, 7),
        ((tok // step, residual_two), product(v.near_t, gu_near, chunk[1])),
        following=(0, 1),
    )
    near_gh = copies.start(block(all_gh, 0), block(all_gh, 1), core_dev)
    row_gh = copies.start(block(all_gh, 0), block(all_gh, 2), row_dev)
    row_gu.append(
        copies.start(gu_own.at[pl.ds(2 * quarter, quarter)], gu_row.at[pl.ds(2 * quarter, quarter)], row_dev)
    )

    for copy in attention:
        copy.wait()
    sum_k, sum_v = v.sum_k, v.sum_v
    sum_k[...] = jnp.zeros_like(sum_k)
    sum_v[...] = jnp.zeros_like(sum_v)
    group = q_cols // kv_cols
    lane = lax.broadcasted_iota(jnp.int32, (tok, 2 * HD), 1)
    front = lane < HD
    lower = lax.rem(lane, HD) < HD // 2

    def turn_back(part):
        other = jnp.where(lower, pltpu.roll(part, 2 * HD - HD // 2, 1), pltpu.roll(part, HD // 2, 1))
        return part * v.cos[...] + other * v.sin[...]

    def head_pair(u):
        lanes = pl.ds(pl.multiple_of(u * 2 * HD, 128), 2 * HD)
        kv = lax.div(2 * u, group)
        grad_ctx = matmul_nt(block(all_gh, 0)[...], weights[pl.ds(pl.multiple_of(u * 2 * HD, 128), 2 * HD)])
        grad_ctx = grad_ctx.astype(bf16)
        query, keys, values = v.q[:, lanes], v.k[kv], v.v[kv]
        shares = grad_ctx.astype(f32) * v.ctx[:, lanes].astype(f32)
        allowed = v.mask[...] > 0
        zero = jnp.zeros_like(query)
        grad_q = jnp.zeros((tok, 2 * HD), f32)
        grad_k = jnp.zeros((tok, 2 * HD), f32)
        grad_v = jnp.zeros((tok, 2 * HD), f32)
        for e in (0, 1):
            own = front if e == 0 else jnp.logical_not(front)
            own_q, own_g = jnp.where(own, query, zero), jnp.where(own, grad_ctx, zero)
            row_dot = jnp.sum(jnp.where(own, shares, 0.0), axis=1, keepdims=True)
            scores = jnp.where(allowed, matmul_nt(own_q, keys) * scaling, neg_large)
            top = jnp.max(scores, axis=1, keepdims=True)
            weight = jnp.exp(scores - top)
            probs = weight / jnp.sum(weight, axis=1, keepdims=True)
            grad_probs = matmul_nt(own_g, values)
            grad_scores = (probs * (grad_probs - row_dot) * scaling).astype(bf16)
            grad_q += matmul(grad_scores, jnp.where(own, keys, zero))
            grad_k += matmul_tn(grad_scores, own_q)
            grad_v += matmul_tn(probs.astype(bf16), own_g)
        all_gq[0:tok, lanes] = turn_back(grad_q).astype(bf16)
        sum_k[kv] += grad_k
        sum_v[kv] += grad_v

    pairs = q_cols // (2 * HD)

    def one_pair(k):
        @pl.when(k <= pairs)
        def _():
            head_pair(k - 1)

    @pl.loop(1, R)
    def _(k):
        for a in (0, 1):
            ring.sum_step(a, k)
        one_pair(k)

    if pairs > R - 1:

        @pl.loop(R - 1, pairs)
        def _(u):
            head_pair(u)

    for j in range(kv_cols // (2 * HD)):
        both = []
        for sums in (sum_k, sum_v):
            one, two = sums[2 * j], sums[2 * j + 1]
            one, two = one + pltpu.roll(one, HD, 1), two + pltpu.roll(two, HD, 1)
            both.append(jnp.where(front, one, two))
        at = q_cols + j * 2 * HD
        all_gq[0:tok, at : at + 2 * HD] = turn_back(both[0]).astype(bf16)
        at += kv_cols
        all_gq[0:tok, at : at + 2 * HD] = both[1].astype(bf16)
    near_gq = copies.start(block(all_gq, 0), block(all_gq, 1), core_dev)
    row_gq = copies.start(block(all_gq, 0), block(all_gq, 2), row_dev)
    row_gu.append(
        copies.start(gu_own.at[pl.ds(3 * quarter, quarter)], gu_row.at[pl.ds(3 * quarter, quarter)], row_dev)
    )

    copies.arrived(near_gh, block(all_gh, 1))
    copies.arrived(row_gh, block(all_gh, 2))
    far_gh = copies.start(block(all_gh, 2), block(all_gh, 3), core_dev)
    for number, landed in small:
        copies.arrived(number, landed)
    for copy in own_parts:
        copy.wait()
    turn_over(v.in_ctx, all_ctx)
    turn_over(v.in_one, all_one)
    copies.arrived(far_gh, block(all_gh, 3))
    tile = q_tiles.shape[1]

    def q_tile(i):
        source = rows_of(h.w_qkv, i * tile, tile)
        at = lax.rem(i, 2)
        return pltpu.make_async_copy(source, q_tiles.at[at], v.tiled.at[at])

    tiles = width // tile
    q_tile(0).start()

    def grad_one(i):
        q_tile(i).wait()

        @pl.when(i + 1 < tiles)
        def _():
            q_tile(i + 1).start()

        hid[:, pl.ds(pl.multiple_of(i * tile, 128), tile)] = matmul_nt(
            block(all_gq, 0)[...], q_tiles[lax.rem(i, 2)]
        )

    load_w = load(h.w_down, weights)

    def before_qkv():
        copies.arrived(near_gq, block(all_gq, 1))
        copies.arrived(row_gq, block(all_gq, 2))
        far_gq = copies.start(block(all_gq, 2), block(all_gq, 3), core_dev)
        copies.arrived(far_gq, block(all_gq, 3))
        do_all(product(all_one, all_gq, chunk[5]))

    spread_phase(
        (0, 1),
        ((tiles, grad_one), product(all_ctx, all_gh, chunk[4])),
        before_qkv,
        (4, 5),
    )

    def residual_one(i):
        b = at_rows(i)
        one, x = hid[b], x_in[b].astype(f32)
        inv = lax.rsqrt(jnp.mean(x * x, axis=1, keepdims=True) + epsilon)
        gain_part[0] += fold(one * x * inv)
        scaled = one * gain[0:1]
        dot = jnp.mean(scaled * x, axis=1, keepdims=True)
        o.tokens[b] = (grad_hid[b] + inv * (scaled - x * inv * inv * dot)).astype(bf16)

    sum_phase((4, 5), ((tok // step, residual_one),))
    load_hid = load(h.hid, hid)

    gain_own, gain_in, gain_all = v.gain_own, v.gain_in, v.gain_all
    for i in (0, 1):
        gain_own[i : i + 1] = jnp.sum(gain_part[i], axis=0, keepdims=True)

    def gain_slice(shard):
        return gain_own.at[:, pl.ds(pl.multiple_of(shard * rows, 128), rows)]

    gains_in = [
        copies.start(gain_slice(shard_of[j]), gain_in.at[j], device)
        for j, device in ((1, core_dev), (2, row_dev), (3, diag_dev))
    ]

    for i, number in enumerate(row_gu):
        copies.arrived(number, gu_row.at[pl.ds(i * quarter, quarter)])
    diag_gu = copies.start(gu_row, gu_near, core_dev)
    copies.arrived(diag_gu, gu_near)
    spread_phase(
        (4, 5),
        (product(v.near_t, gu_row, chunk[2], True), product(v.near_t, gu_near, chunk[3], True)),
        following=(2, 3),
    )

    for j, number in enumerate(gains_in):
        copies.arrived(number, gain_in.at[j + 1])
    gain_all[r] = gain_slice(s)[...] + gain_in[1] + (gain_in[2] + gain_in[3])

    def gain_copy(d):
        return pltpu.make_async_remote_copy(
            src_ref=gain_all.at[r],
            dst_ref=gain_all.at[r],
            send_sem=v.gain_send.at[d],
            recv_sem=v.gain_recv.at[d],
            device_id=(lax.rem(r + d, R), s),
            device_id_type=pl.DeviceIdType.MESH,
        )

    @pl.loop(1, R)
    def _(d):
        gain_copy(d).start()

    copies.finish()
    act = gu_row.at[:, pl.ds(0, ff)]
    load(h.act, act).wait()
    load_w.wait()
    load_hid.wait()
    sum_phase((2, 3), (product(act, weights, gu_own),))
    half = 2 * tok
    core_b = copies.start(rows_of(gu_own, half + (1 - c) * tok, tok), got_b, core_dev)
    core_a = copies.start(rows_of(gu_own, (1 - c) * tok, tok), got_a, core_dev)
    copies.arrived(core_b, got_b)
    mine_b[...] = (
        rows_of(gu_own, half + c * tok, tok)[...].astype(f32) + got_b[...].astype(f32)
    ).astype(bf16)
    far = copies.start(mine_b, got_far, row_dev)
    spread_phase((2, 3))
    copies.arrived(core_a, got_a)
    copies.arrived(far, got_far)

    @pl.loop(0, tok // step)
    def _(i):
        b = at_rows(i)
        own = rows_of(gu_own, c * tok + i * step, step)[...].astype(f32)
        out = hid[b] + own + got_a[b].astype(f32) + got_far[b].astype(f32)
        o.out[b] = out.astype(bf16)

    @pl.loop(1, R)
    def _(d):
        source = lax.rem(r + R - d, R)
        landed = gain_all.at[source]
        pltpu.make_async_copy(landed, landed, v.gain_recv.at[d]).wait()
        gain_copy(d).wait_send()

    total = gain_all[0]
    for q in range(1, R):
        total = total + gain_all[q]
    o.gains[...] = total
    copies.finish()


def backward(R, **given):
    h = types.SimpleNamespace(**given)
    tok, width = h.x.shape
    gu = h.gu.shape
    tokens, S = gu[0], gu[0] // tok
    rows, head_rows = width // S, h.w_o.shape[0] // S
    qkv_cols = h.w_qkv.shape[1]
    half_d = h.down.shape[0] // 2
    down = h.down.shape
    assert half_d >= rows and down[1] >= qkv_cols and gu == (tokens, width), "unsupported sizes"
    slot = slice_shape((max(rows, half_d), width // 2), R)[:2]
    full = (rows, S * gu[1] // 2)
    V = lambda shape, dtype=bf16: pltpu.VMEM(shape, dtype)
    dma = pltpu.SemaphoreType.DMA
    outs = dict(
        gate=(full, bf16, False),
        up=(full, bf16, False),
        o=((head_rows, width), bf16, False),
        qkv=((rows, qkv_cols), bf16, False),
        down=(down, bf16, False),
        tokens=((tok, width), bf16, True),
        out=((tok, width), bf16, True),
        gains=((2, rows), f32, True),
    )
    same = lambda a: V(a.shape, a.dtype)
    scratch = dict(
        down=same(h.down),
        set_one=V((2, rows, width)),
        slots_a=V((2, 2, R - 1) + slot),
        slots_b=V((2, 2, R - 1) + slot),
        gu_own=V(gu),
        gu_near=V(gu),
        gu_row=V(gu),
        near_t=V((rows, tokens)),
        in_ctx=V((tokens, head_rows)),
        in_one=V((tokens, rows)),
        all_gh=V((tokens, width)),
        all_gq=V((tokens, qkv_cols)),
        all_ctx=V((head_rows, tokens)),
        all_one=V((rows, tokens)),
        mine_a=V((tok, width)),
        mine_b=V((tok, width)),
        got_a=V((tok, width)),
        got_b=V((tok, width)),
        got_far=V((tok, width)),
        hid=V((tok, width), f32),
        x_in=V((tok, width)),
        cot=V((tok, width)),
        grad_hid=V((tok, width), f32),
        weights=V(h.w_o.shape),
        q_tiles=V((2, 256, qkv_cols)),
        gain=same(h.gain),
        q=same(h.q),
        k=same(h.k),
        v=same(h.v),
        ctx=same(h.ctx),
        mask=same(h.mask),
        cos=same(h.cos),
        sin=same(h.sin),
        sum_k=V(h.k.shape, f32),
        sum_v=V(h.k.shape, f32),
        gain_part=V((2, 8, width), f32),
        gain_own=V((2, width), f32),
        gain_in=V((S, 2, rows), f32),
        gain_all=V((R, 2, rows), f32),
        sums=dma((8, 2, R - 1)),
        spread=dma((8, 2, R - 1)),
        sent=dma((8, 2, 2)),
        kept=dma((8, 2)),
        send=dma((32,)),
        recv=dma((32,)),
        loaded=dma((32,)),
        tiled=dma((2,)),
        gain_send=dma((R,)),
        gain_recv=dma((R,)),
    )
    keys = tuple(given), tuple(outs), tuple(scratch)
    return pl.pallas_call(
        functools.partial(backward_kernel, R, keys),
        out_shape=[jax.ShapeDtypeStruct(shape, dtype) for shape, dtype, _ in outs.values()],
        in_specs=[pl.BlockSpec(memory_space=pl.ANY)] * len(given),
        out_specs=[
            pl.BlockSpec(memory_space=pltpu.VMEM if near else pl.ANY) for *_, near in outs.values()
        ],
        scratch_shapes=list(scratch.values()),
        compiler_params=pltpu.CompilerParams(
            collective_id=2, has_side_effects=True, vmem_limit_bytes=67043328
        ),
        name="backward",
    )(*given.values())


def widen_kernel(splits, *refs):
    count = len(splits)
    outs = iter(refs[count:])
    for ref, widths in zip(refs, splits):
        at = 0
        for width in widths:
            out = next(outs)
            out[...] = ref[:, at : at + width].astype(out.dtype)
            at += width


def widen(arrays, steps=4):
    in_specs, out_specs, out_shape = [], [], []
    for arr, widths, dtype in arrays:
        h = arr.shape[0] // steps
        in_specs.append(pl.BlockSpec((h, arr.shape[1]), lambda i: (i, 0)))
        for width in widths:
            out_specs.append(pl.BlockSpec((h, width), lambda i: (i, 0)))
            out_shape.append(jax.ShapeDtypeStruct((arr.shape[0], width), dtype))
    return pl.pallas_call(
        functools.partial(widen_kernel, [widths for _, widths, _ in arrays]),
        grid=(steps,),
        in_specs=in_specs,
        out_specs=out_specs,
        out_shape=out_shape,
        name="widen",
    )(*[arr for arr, *_ in arrays])


def per_device(
    R,
    S,
    tokens_in,
    cotangent,
    segment_ids,
    attn_gain,
    w_query,
    w_key,
    w_value,
    w_output,
    mlp_gain,
    w_gate,
    w_up,
    w_down,
):
    batches, length, width = tokens_in.shape
    tokens = batches * length
    assert batches == 1, "unsupported sizes"
    q_cols, kv_cols = w_query.shape[1], w_key.shape[1]
    exponent = jnp.arange(HD // 2).astype(f32) * (2.0 / HD)
    x = tokens_in.reshape(tokens, width)
    cot = cotangent.reshape(tokens, width)
    f = forward(
        S,
        x=x,
        cot=cot,
        gain=jnp.stack([attn_gain, mlp_gain]).astype(f32),
        w_q=w_query,
        w_kv=jnp.concatenate([w_key, w_value], axis=1),
        w_o=w_output,
        w_gate=w_gate,
        w_up=w_up,
        w_down=w_down,
        segments=segment_ids,
        speed=jnp.tile(theta_base ** (-exponent), 4)[None],
    )
    out = backward(
        R,
        down=f.down,
        part=f.part,
        gu=f.gu,
        two=f.two,
        hid=f.hid,
        x=x,
        cot=cot,
        gain=f.gain,
        w_o=f.w_o,
        w_down=w_down,
        w_qkv=f.w_qkv,
        act=f.act,
        q=f.q,
        k=f.k,
        v=f.v,
        ctx=f.ctx,
        mask=f.mask,
        cos=f.cos,
        sin=f.sin,
        one=f.one,
    )
    gate, up, o, qkv, down, grad_tokens, tokens_out, gains = out
    full = gate.shape[1]
    gate, up, o, *qkv, down, grad_tokens, tokens_out = widen(
        [
            (gate, (full,), f32),
            (up, (full,), f32),
            (o, (width,), f32),
            (qkv, (q_cols, kv_cols, kv_cols), f32),
            (down, (width,), f32),
            (grad_tokens, (width,), bf16),
            (tokens_out, (width,), bf16),
        ]
    )
    return (
        tokens_out.reshape(tokens_in.shape),
        grad_tokens.reshape(tokens_in.shape),
        gains[0],
        *qkv,
        o,
        gains[1],
        gate,
        up,
        down,
    )


def solution(mesh):
    R, S = mesh.shape["replica"], mesh.shape["shard"]
    assert S == 4 and R % 4 == 0, "unsupported mesh"
    data = P(AXES, None, None)
    rowwise = P("shard", None)
    flat = P("shard")
    return jax.shard_map(
        functools.partial(per_device, R, S),
        mesh=mesh,
        in_specs=((data, data, P(AXES, None), flat) + (rowwise,) * 4 + (flat,) + (rowwise,) * 3),
        out_specs=(data, data, flat) + (rowwise,) * 4 + (flat,) + (rowwise,) * 3,
        check_vma=False,
    )
```

```python
import functools
import math
import types

import jax
import jax.numpy as jnp
from jax import lax
from jax.experimental import pallas as pl
from jax.experimental.pallas import tpu as pltpu
from jax.sharding import PartitionSpec as P

KV = 4
HD = 64

epsilon = 1e-05
theta_base = 500000.0
neg_large = -1e30


AXES = ("replica", "shard")
f32 = jnp.float32
bf16 = jnp.bfloat16


def matmul(left_arr, right_arr):
    return jnp.dot(left_arr, right_arr, preferred_element_type=f32)


def matmul_nt(left_arr, right_arr):
    return lax.dot_general(
        left_arr, right_arr, (((1,), (1,)), ((), ())), preferred_element_type=f32
    )


def matmul_tn(left_arr, right_arr):
    return lax.dot_general(
        left_arr, right_arr, (((0,), (0,)), ((), ())), preferred_element_type=f32
    )


class Copies:
    def __init__(self, send, recv):
        self.send, self.recv, self.count, self.open = send, recv, 0, []

    def start(self, src, dst, device):
        copy = pltpu.make_async_remote_copy(
            src_ref=src,
            dst_ref=dst,
            send_sem=self.send.at[self.count],
            recv_sem=self.recv.at[self.count],
            device_id=device,
            device_id_type=pl.DeviceIdType.MESH,
        )
        self.count += 1
        copy.start()
        self.open.append(copy)
        return self.count - 1

    def arrived(self, number, landed):
        pltpu.make_async_copy(landed, landed, self.recv.at[number]).wait()

    def finish(self):
        for copy in self.open:
            copy.wait_send()
        self.open = []


def meet(devices):
    barrier = pltpu.get_barrier_semaphore()
    for device in devices:
        pl.semaphore_signal(
            barrier, inc=1, device_id=device, device_id_type=pl.DeviceIdType.MESH
        )
    pl.semaphore_wait(barrier, len(devices))


def forward_kernel(keys, *refs):
    given = iter(refs)
    h, o, v = (types.SimpleNamespace(**{key: next(given) for key in group}) for group in keys)
    r, s = lax.axis_index("replica"), lax.axis_index("shard")
    c, y = lax.rem(s, 2), lax.div(s, 2)
    x = lax.rem(r, 2)
    w = lax.rem(lax.div(r, 2), 2)
    near, row = 2 * y + 1 - c, 2 * (1 - y) + c
    diagonal = 2 * (1 - y) + 1 - c
    core_dev, row_dev, diag_dev = (r, near), (r, row), (r, diagonal)
    x_dev, z_dev = (r + 1 - 2 * x, s), (r + 2 - 4 * w, s)
    copies = Copies(v.send, v.recv)
    loads, saves = [], []

    def move(source, into, kind, sems):
        copy = pltpu.make_async_copy(source, into, sems.at[len(kind)])
        kind.append(copy)
        copy.start()
        return copy

    def load(source, into):
        return move(source, into, loads, v.loaded)

    def save(source, into):
        return move(source, into, saves, v.saved)

    tok, width = h.x.shape
    ff = v.all_gu.shape[1] // 2
    q_cols, kv_cols = v.q.shape[1], v.all_kv.shape[1] // 2
    m_g = h.w_gate.shape[0]
    q_g = m_g // 4

    def rows_of(ref, start, size):
        return ref.at[pl.ds(pl.multiple_of(start, 16), size)]

    def columns_of(ref, start, size, shard):
        return ref.at[
            pl.ds(pl.multiple_of(start, 16), size), pl.ds(pl.multiple_of(shard * ff, 128), ff)
        ]

    def quarter(flip_x, flip_z):
        at_x = (1 - x) if flip_x else x
        at_z = (1 - w) if flip_z else w
        return 2 * at_z + at_x

    here = quarter(0, 0)

    def gu_part(owner, start, size):
        return [
            v.all_gu.at[pl.ds(pl.multiple_of(owner * m_g + start, 16), size), pl.ds(k * ff, ff)]
            for k in (0, 1)
        ]

    load_x = load(h.x, v.x_in)
    load_gain = load(h.gain, v.gain.at[:, pl.ds(pl.multiple_of(s * m_g, 128), m_g)])
    plain = [(h.w_q, v.all_q, True), (h.w_kv, v.all_kv, False), (h.w_o, v.all_o, False)]
    load_own = [load(a, rows_of(b, s * a.shape[0], a.shape[0])) for a, b, _ in plain]
    load_small = [load(h.segments, v.segments), load(h.speed, v.speed)]
    own_cot = rows_of(v.all_cot, c * tok, tok)
    load_gu = [
        load(columns_of(a, 0, m_g, s), part)
        for a, part in zip((h.w_gate, h.w_up), gu_part(s, 0, m_g))
    ]
    load_gu += [load(h.cot, own_cot), load(h.w_down, v.w_down)]

    meet([core_dev, row_dev, diag_dev, x_dev, z_dev])

    gain_parts = []
    for device, owner in ((core_dev, near), (row_dev, row), (diag_dev, diagonal)):
        mine = v.gain.at[:, pl.ds(pl.multiple_of(s * m_g, 128), m_g)]
        landed = v.gain.at[:, pl.ds(pl.multiple_of(owner * m_g, 128), m_g)]
        gain_parts.append((copies.start(h.gain, mine, device), landed))

    flows, first = [], []
    for a, b, x_first in plain:
        m = a.shape[0]
        part = rows_of(a, here * (m // 4), m // 4)
        region = functools.partial(
            lambda b, m, owner, spot: rows_of(b, owner * m + spot * (m // 4), m // 4), b, m
        )
        first.append(copies.start(part, region(s, here), row_dev))
        flows.append((region, row, True, x_first))
    for shard, device in ((row, row_dev), (diagonal, diag_dev)):
        for k, a in enumerate((h.w_gate, h.w_up)):
            region = functools.partial(
                lambda k, owner, spot: v.all_gu.at[
                    pl.ds(pl.multiple_of(owner * m_g + spot * q_g, 16), q_g), pl.ds(k * ff, ff)
                ],
                k,
            )
            part = columns_of(a, here * q_g, q_g, shard)
            first.append(copies.start(part, region(s, here), device))
            flows.append((region, shard, False, k == 0))
    far_cot = rows_of(v.all_cot, 2 * tok + c * tok, tok)
    row_cot = copies.start(h.cot, far_cot, row_dev)

    core_plain = []
    for a, b, _ in plain:
        m = a.shape[0]
        core_plain.append((copies.start(a, rows_of(b, s * m, m), core_dev), rows_of(b, near * m, m)))
    core_gu = [
        (copies.start(columns_of(a, 0, m_g, near), part, core_dev), landed)
        for a, part, landed in zip(
            (h.w_gate, h.w_up), gu_part(s, 0, m_g), gu_part(near, 0, m_g)
        )
    ]
    core_gu.append(
        (copies.start(h.cot, own_cot, core_dev), rows_of(v.all_cot, (1 - c) * tok, tok))
    )

    second, third = {}, {}
    forwarded = {i: [] for i in range(len(flows))}

    def to_core(i, part, spot):
        if flows[i][2]:
            forwarded[i].append((copies.start(part, part, core_dev), spot))

    def stage(i, number):
        region, owner, _, x_first = flows[i]
        flip = (1, 0) if x_first else (0, 1)
        one, two = (x_dev, z_dev) if x_first else (z_dev, x_dev)
        piece, other = region(owner, here), region(owner, quarter(*flip))
        if number == 1:
            copies.arrived(first[i], piece)
            second[i] = copies.start(piece, piece, one)
            to_core(i, piece, (0, 0))
        elif number == 2:
            copies.arrived(second[i], other)
            third[i] = [
                (copies.start(part, part, two), spot)
                for part, spot in ((piece, (0, 0)), (other, flip))
            ]
            to_core(i, other, flip)
        elif number == 3:
            for sent, (fx, fz) in third[i]:
                spot = (fx, 1 - fz) if x_first else (1 - fx, fz)
                part = region(owner, quarter(*spot))
                copies.arrived(sent, part)
                to_core(i, part, spot)
        else:
            for sent, spot in forwarded[i]:
                copies.arrived(sent, region(diagonal, quarter(*spot)))

    step = 32

    def at_rows(i):
        return pl.ds(pl.multiple_of(i * step, step), step)

    def norm(source, which, into):
        @pl.loop(0, tok // step)
        def _(i):
            b = at_rows(i)
            values = source[b].astype(f32)
            inv = lax.rsqrt(jnp.mean(values * values, axis=1, keepdims=True) + epsilon)
            into[b] = (values * inv * v.gain[which : which + 1]).astype(bf16)

    stage(0, 1)
    stage(1, 1)
    for copy in load_small:
        copy.wait()

    along = jnp.broadcast_to(v.segments[...], (tok, tok))
    query_at = lax.broadcasted_iota(jnp.int32, (tok, tok), 0)
    key_at = lax.broadcasted_iota(jnp.int32, (tok, tok), 1)
    allowed = (along.T == along) & (query_at >= key_at)
    v.mask[...] = jnp.where(allowed, 1.0, 0.0)
    position = jnp.sum(v.mask[...], axis=1, keepdims=True) - 1.0
    angle = position * v.speed[...]
    lane = lax.broadcasted_iota(jnp.int32, (tok, 2 * HD), 1)
    front = lane < HD
    lower = lax.rem(lane, HD) < HD // 2
    v.cos[...] = jnp.cos(angle)
    sine = jnp.sin(angle)
    v.sin[...] = jnp.where(lower, sine, -sine)
    save(v.mask, o.mask)
    save(v.cos, o.cos)
    save(v.sin, o.sin)
    for i, number in ((0, 2), (1, 2), (2, 1), (3, 1)):
        stage(i, number)
    load_x.wait()
    load_gain.wait()
    for sent, landed in gain_parts:
        copies.arrived(sent, landed)
    norm(v.x_in, 0, v.one)
    save(v.one, o.one)
    for copy in load_own:
        copy.wait()
    for i, number in ((1, 3), (4, 1), (0, 3), (5, 1), (2, 2), (3, 2), (4, 2)):
        stage(i, number)
    for sent, landed in core_plain:
        copies.arrived(sent, landed)
    stage(0, 4)
    stage(1, 4)

    def turn(part):
        other = jnp.where(lower, pltpu.roll(part, 2 * HD - HD // 2, 1), pltpu.roll(part, HD // 2, 1))
        return part * v.cos[...] - other * v.sin[...]

    def lanes_of(i):
        return pl.ds(pl.multiple_of(i * 2 * HD, 128), 2 * HD)

    @pl.loop(0, q_cols // 256)
    def _(i):
        part = matmul(v.one[...], v.all_q[:, pl.ds(pl.multiple_of(i * 256, 128), 256)])
        for j in (0, 1):
            half = part[:, j * 2 * HD : (j + 1) * 2 * HD]
            v.q[:, lanes_of(2 * i + j)] = turn(half).astype(bf16)

    for which, into in ((0, v.k), (1, v.v)):
        part = matmul(v.one[...], v.all_kv[:, which * kv_cols : (which + 1) * kv_cols])
        for j in range(kv_cols // (2 * HD)):
            half = part[:, j * 2 * HD : (j + 1) * 2 * HD]
            half = turn(half) if which == 0 else half
            swapped = pltpu.roll(half, HD, 1)
            into[2 * j] = jnp.where(front, half, swapped).astype(bf16)
            into[2 * j + 1] = jnp.where(front, swapped, half).astype(bf16)
    save(v.q, o.q)
    save(v.k, o.k)
    save(v.v, o.v)
    save(v.all_q, o.w_qkv.at[:, pl.ds(0, q_cols)])
    save(v.all_kv, o.w_qkv.at[:, pl.ds(q_cols, 2 * kv_cols)])
    stage(6, 1)

    group = q_cols // kv_cols
    scaling = 1.0 / math.sqrt(HD)

    def head_pair(u):
        kv = lax.div(2 * u, group)
        query, keys, values = v.q[:, lanes_of(u)], v.k[kv], v.v[kv]
        allowed = v.mask[...] > 0
        zero = jnp.zeros_like(query)
        context = jnp.zeros((tok, 2 * HD), f32)
        for e in (0, 1):
            own = front if e == 0 else jnp.logical_not(front)
            scores = jnp.where(
                allowed, matmul_nt(jnp.where(own, query, zero), keys) * scaling, neg_large
            )
            top = jnp.max(scores, axis=1, keepdims=True)
            weight = jnp.exp(scores - top)
            probs = (weight / jnp.sum(weight, axis=1, keepdims=True)).astype(bf16)
            context += matmul(probs, jnp.where(own, values, zero))
        v.ctx[:, lanes_of(u)] = context.astype(bf16)

    pairs = q_cols // (2 * HD)

    @pl.loop(0, pairs // 2)
    def _(u):
        head_pair(u)

    stage(5, 2)

    @pl.loop(pairs // 2, pairs)
    def _(u):
        head_pair(u)

    save(v.ctx, o.ctx)
    stage(2, 3)
    stage(2, 4)
    save(v.all_o, o.w_o)

    @pl.loop(0, width // 256)
    def _(i):
        columns = pl.ds(pl.multiple_of(i * 256, 128), 256)
        v.hid[:, columns] = v.x_in[:, columns].astype(f32) + matmul(v.ctx[...], v.all_o[:, columns])

    own_two = rows_of(v.two, c * tok, tok)
    norm(v.hid, 1, own_two)
    far_two = rows_of(v.two, 2 * tok + c * tok, tok)
    near_two = copies.start(own_two, own_two, core_dev)
    row_two = copies.start(own_two, far_two, row_dev)
    stage(6, 2)
    save(v.hid, o.hid)
    save(v.gain, o.gain)

    for copy in load_gu:
        copy.wait()
    for sent, landed in core_gu:
        copies.arrived(sent, landed)
    copies.arrived(near_two, rows_of(v.two, (1 - c) * tok, tok))

    half = 2 * m_g
    early = pl.ds(pl.multiple_of(y * half, 128), half)
    late = pl.ds(pl.multiple_of((1 - y) * half, 128), half)
    low, high = pl.ds(0, 2 * tok), pl.ds(2 * tok, 2 * tok)

    @pl.loop(0, 2 * ff // 256)
    def _(i):
        columns = pl.ds(pl.multiple_of(i * 256, 128), 256)
        v.sums[low, columns] = matmul(v.two[low, early], v.all_gu[early, columns])

    def grads_act(tokens, into):
        @pl.loop(0, ff // 256)
        def _(i):
            columns = pl.ds(pl.multiple_of(i * 256, 128), 256)
            into[:, columns] = matmul_nt(v.all_cot[tokens], v.w_down[columns])

    copies.arrived(row_cot, far_cot)
    last_cot = copies.start(far_cot, far_cot, core_dev)
    act_low, act_high = v.sums.at[high, pl.ds(0, ff)], v.grad_act
    grads_act(low, act_low)
    there = 2 * tok + (1 - c) * tok
    copies.arrived(last_cot, rows_of(v.all_cot, there, tok))
    grads_act(high, act_high)
    for i in (4, 3, 6, 5):
        stage(i, 3)

    def units(end):
        tokens = high if end else low

        @pl.loop(0, ff // 256)
        def _(i):
            columns = pl.ds(pl.multiple_of(i * 256, 128), 256)
            ups = pl.ds(pl.multiple_of(ff + i * 256, 128), 256)
            if end:
                gate = matmul(v.two[tokens], v.all_gu[:, columns])
                up = matmul(v.two[tokens], v.all_gu[:, ups])
            else:
                gate = v.sums[low, columns] + matmul(v.two[tokens, late], v.all_gu[late, columns])
                up = v.sums[low, ups] + matmul(v.two[tokens, late], v.all_gu[late, ups])
            grad_act = (act_high if end else act_low)[:, columns]
            sigmoid = jax.nn.sigmoid(gate)
            silu = gate * sigmoid
            v.act[tokens, columns] = (silu * up).astype(bf16)
            v.gu[tokens, columns] = (
                grad_act * up * sigmoid * (1.0 + gate * (1.0 - sigmoid))
            ).astype(bf16)
            v.gu[tokens, ups] = (grad_act * silu).astype(bf16)

    def partial(end):
        tokens = pl.ds(end * 2 * tok, 2 * tok)

        @pl.loop(0, width // 256)
        def _(i):
            columns = pl.ds(pl.multiple_of(i * 256, 128), 256)
            v.part[tokens, columns] = matmul_nt(
                v.gu[tokens], v.all_gu[pl.ds(pl.multiple_of(i * 256, 128), 256)]
            ).astype(bf16)

    def down(end):
        tokens = pl.ds(end * 2 * tok, 2 * tok)

        @pl.loop(0, ff // 256)
        def _(i):
            units_at = pl.ds(pl.multiple_of(i * 256, 128), 256)
            turned = v.act[tokens, units_at].T

            @pl.loop(0, width // 512)
            def _(j):
                columns = pl.ds(pl.multiple_of(j * 512, 128), 512)
                part = matmul(turned, v.all_cot[tokens, columns])
                if end == 0:
                    v.sums[units_at, columns] = part
                else:
                    v.down[units_at, columns] = (v.sums[units_at, columns] + part).astype(bf16)

    def save_rows(end, *names):
        tokens = pl.ds(end * 2 * tok, 2 * tok)
        for a, b in names:
            save(a.at[tokens], b.at[tokens])

    units(0)
    partial(0)
    save_rows(0, (v.act, o.act), (v.gu, o.gu), (v.part, o.part), (v.two, o.two))
    down(0)
    copies.arrived(row_two, far_two)
    last_two = copies.start(far_two, far_two, core_dev)
    copies.arrived(last_two, rows_of(v.two, there, tok))
    units(1)
    save_rows(1, (v.two, o.two), (v.act, o.act), (v.gu, o.gu))
    down(1)
    save(v.down, o.down)
    partial(1)
    save_rows(1, (v.part, o.part))
    copies.finish()
    for copy in saves:
        copy.wait()


def forward(S, **given):
    h = types.SimpleNamespace(**given)
    tok, width = h.x.shape
    ff, q_cols, kv_cols = h.w_down.shape[0], h.w_q.shape[1], h.w_kv.shape[1] // 2
    V = lambda shape, dtype=bf16: pltpu.VMEM(shape, dtype)
    dma = pltpu.SemaphoreType.DMA
    heads = (kv_cols // HD, tok, 2 * HD)
    many = S * tok
    outs = dict(
        w_qkv=(S * h.w_q.shape[0], q_cols + 2 * kv_cols),
        w_o=(S * h.w_o.shape[0], width),
        gain=(2, width),
        one=(tok, width),
        q=(tok, q_cols),
        k=heads,
        v=heads,
        ctx=(tok, q_cols),
        hid=(tok, width),
        two=(many, width),
        act=(many, ff),
        gu=(many, 2 * ff),
        part=(many, width),
        down=(ff, width),
        mask=(tok, tok),
        cos=(tok, 2 * HD),
        sin=(tok, 2 * HD),
    )
    scratch = dict(
        x_in=V((tok, width)),
        gain=V((2, width), f32),
        all_q=V((S * h.w_q.shape[0], q_cols)),
        all_kv=V((S * h.w_q.shape[0], 2 * kv_cols)),
        all_o=V((S * h.w_o.shape[0], width)),
        all_gu=V((S * h.w_gate.shape[0], 2 * ff)),
        all_cot=V((many, width)),
        w_down=V(h.w_down.shape),
        segments=V(h.segments.shape, h.segments.dtype),
        speed=V(h.speed.shape, f32),
        cos=V((tok, 2 * HD), f32),
        sin=V((tok, 2 * HD), f32),
        mask=V((tok, tok), f32),
        sums=V((ff, width), f32),
        down=V((ff, width)),
        grad_act=V((2 * tok, ff), f32),
        one=V((tok, width)),
        q=V((tok, q_cols)),
        k=V(heads),
        v=V(heads),
        ctx=V((tok, q_cols)),
        hid=V((tok, width), f32),
        two=V((many, width)),
        act=V((many, ff)),
        gu=V((many, 2 * ff)),
        part=V((many, width)),
        send=dma((64,)),
        recv=dma((64,)),
        loaded=dma((24,)),
        saved=dma((32,)),
    )
    wide = ("hid", "gain", "mask", "cos", "sin")
    out = pl.pallas_call(
        functools.partial(forward_kernel, (tuple(given), tuple(outs), tuple(scratch))),
        out_shape=[
            jax.ShapeDtypeStruct(shape, f32 if name in wide else bf16)
            for name, shape in outs.items()
        ],
        in_specs=[pl.BlockSpec(memory_space=pl.ANY)] * len(given),
        out_specs=[pl.BlockSpec(memory_space=pl.ANY)] * len(outs),
        scratch_shapes=list(scratch.values()),
        compiler_params=pltpu.CompilerParams(
            collective_id=1, has_side_effects=True, vmem_limit_bytes=67043328
        ),
        name="forward",
    )(*given.values())
    return types.SimpleNamespace(**dict(zip(outs, out)))


def slice_shape(shape, parts):
    rows, cols = shape
    down = min(parts, rows // 16)
    across = parts // down
    assert rows % down == 0 and cols % (128 * across) == 0, "unsupported sizes"
    return rows // down, cols // across, across


def halves_of(ref):
    w = ref.shape[1] // 2
    return ref.at[:, pl.ds(0, w)], ref.at[:, pl.ds(w, w)]


class Ring:
    def __init__(self, R, chunks, outs, slots, sums, spread, sent, kept):
        self.R, self.chunks, self.outs, self.slots = R, chunks, outs, slots
        self.sums, self.spread, self.sent, self.kept = sums, spread, sent, kept
        r, self.s = lax.axis_index("replica"), lax.axis_index("shard")
        z, x = lax.div(r, 2), lax.rem(r, 2)
        self.place = z * (1 - x) + (R - 1 - z) * x
        self.peers = [self.replica_at(self.place + 1), self.replica_at(self.place + R - 1)]

    def replica_at(self, place):
        R = self.R
        place = lax.rem(place, R)
        back = lax.div(place, R // 2)
        return (1 - back) * 2 * place + back * (2 * (R - 1 - place) + 1)

    def part(self, halves, way, step):
        R, ref = self.R, halves[way]
        number = lax.rem(self.place + (R - step if way == 0 else step), R)
        h, w, across = slice_shape(ref.shape, R)
        return ref.at[
            pl.ds(pl.multiple_of(lax.div(number, across) * h, 16), h),
            pl.ds(pl.multiple_of(lax.rem(number, across) * w, 128), w),
        ]

    def slot(self, a, way, step):
        h, w, _ = slice_shape(self.chunks[a][0].shape, self.R)
        return self.slots[a].at[way, step, pl.ds(0, h), pl.ds(0, w)]

    def copy(self, a, way, step, src, dst, arrival):
        return pltpu.make_async_remote_copy(
            src_ref=src,
            dst_ref=dst,
            send_sem=self.sent.at[a, way, lax.rem(step, 2)],
            recv_sem=arrival,
            device_id=(self.peers[way], self.s),
            device_id_type=pl.DeviceIdType.MESH,
        )

    def start(self, a):
        for way in (0, 1):
            src = self.part(self.chunks[a], way, 0)
            self.copy(a, way, 0, src, self.slot(a, way, 0), self.sums.at[a, way, 0]).start()

    def sum_step(self, a, k):
        last = k == self.R - 1
        for way in (0, 1):
            slot = self.slot(a, way, k - 1)
            self.copy(a, way, 0, slot, slot, self.sums.at[a, way, k - 1]).wait_recv()
            own = self.part(self.chunks[a], way, k)
            slot[...] = (slot[...].astype(f32) + own[...].astype(f32)).astype(bf16)
            dst = self.part(self.outs[a], way, k)
            onward = self.copy(a, way, k, slot, dst, self.spread.at[a, way, 0])

            @pl.when(k >= 2)
            def _():
                self.copy(a, way, k, slot, slot, self.sums.at[a, way, 0]).wait_send()

            @pl.when(last)
            def _():
                onward.start()
                pltpu.make_async_copy(slot, dst, self.kept.at[a, way]).start()

            @pl.when(jnp.logical_not(last))
            def _():
                there = lax.rem(k, self.R - 1)
                self.copy(
                    a, way, k, slot, self.slot(a, way, there), self.sums.at[a, way, there]
                ).start()

    def spread_step(self, a, k, last=False):
        for way in (0, 1):
            dst = self.part(self.outs[a], way, lax.rem(k + self.R - 1, self.R))
            self.copy(a, way, 0, dst, dst, self.spread.at[a, way, k - 1]).wait_recv()
            if not last:
                onward = self.copy(a, way, k + self.R - 1, dst, dst, self.spread.at[a, way, k])
                onward.wait_send()
                onward.start()

    def finish(self, a):
        for way in (0, 1):
            slot = self.slot(a, way, self.R - 2)
            for step in (0, 1):
                self.copy(a, way, step, slot, slot, self.sums.at[a, way, 0]).wait_send()
            dst = self.part(self.outs[a], way, self.R - 1)
            pltpu.make_async_copy(slot, dst, self.kept.at[a, way]).wait()


def product(left, right, out, crossed=False, tile=256):
    half = right.shape[0] // 2

    def make(i):
        columns = pl.ds(pl.multiple_of(i * tile, 128), tile)
        if crossed:
            one = matmul(left[:, 0:half], right[pl.ds(half, half), columns])
            out[:, columns] = (one + matmul(left[:, half:], right[pl.ds(0, half), columns])).astype(bf16)
        else:
            out[:, columns] = matmul(left[...], right[:, columns]).astype(bf16)

    return out.shape[1] // tile, make


def backward_kernel(R, keys, *refs):
    given = iter(refs)
    h, o, v = (types.SimpleNamespace(**{key: next(given) for key in group}) for group in keys)
    r, s = lax.axis_index("replica"), lax.axis_index("shard")
    c, y = lax.rem(s, 2), lax.div(s, 2)
    near, row = 2 * y + 1 - c, 2 * (1 - y) + c
    diagonal = 2 * (1 - y) + 1 - c
    shard_of = (s, near, row, diagonal)
    core_dev, row_dev, diag_dev = (r, near), (r, row), (r, diagonal)

    barrier = pltpu.get_barrier_semaphore()
    for other in (near, row, diagonal):
        pl.semaphore_signal(
            barrier, inc=1, device_id=(r, other), device_id_type=pl.DeviceIdType.MESH
        )

    @pl.loop(1, R)
    def _(d):
        pl.semaphore_signal(
            barrier, inc=1, device_id=(lax.rem(r + d, R), s), device_id_type=pl.DeviceIdType.MESH
        )

    loads = []

    def load(source, into):
        copy = pltpu.make_async_copy(source, into, v.loaded.at[len(loads)])
        loads.append(copy)
        copy.start()
        return copy

    down, set_one, slots_a, slots_b = v.down, v.set_one, v.slots_a, v.slots_b
    gu_own, gu_near, gu_row = v.gu_own, v.gu_near, v.gu_row
    all_gh, all_gq, all_ctx, all_one = v.all_gh, v.all_gq, v.all_ctx, v.all_one
    mine_a, mine_b, got_a, got_b, got_far = v.mine_a, v.mine_b, v.got_a, v.got_b, v.got_far
    hid, x_in, cot, grad_hid = v.hid, v.x_in, v.cot, v.grad_hid
    weights, q_tiles = v.weights, v.q_tiles
    tok, width = x_in.shape
    ff = gu_own.shape[1] // 2
    rows, head_rows = v.near_t.shape[0], weights.shape[0] // len(shard_of)
    q_cols = v.q.shape[1]
    qkv_cols = all_gq.shape[1]
    kv_cols = (qkv_cols - q_cols) // 2
    half_d = down.shape[0] // 2
    scaling = 1.0 / math.sqrt(HD)

    def rows_of(a, start, size):
        return a.at[pl.ds(pl.multiple_of(start, 16), size)]

    def block(a, j):
        return a.at[pl.ds(j * tok, tok)]

    def columns(a, j, size):
        return a.at[:, pl.ds(pl.multiple_of(j * size, 128), size)]

    load_down = load(h.down, down)
    load_b = load(rows_of(h.part, 2 * tok + c * tok, tok), mine_b)
    tokens = gu_own.shape[0]
    load_gu = load(h.gu, gu_own)
    own_two = all_gq.at[:, pl.ds(0, rows)]
    load_near = load(h.two.at[:, pl.ds(pl.multiple_of(s * rows, 128), rows)], own_two)
    load_a = load(rows_of(h.part, c * tok, tok), mine_a)
    later = [
        load(source, into)
        for source, into in ((h.hid, hid), (h.x, x_in), (h.cot, cot), (h.gain, v.gain))
    ]
    load_w = load(h.w_o, weights)
    attention = [
        load(source, into)
        for source, into in (
            (h.q, v.q), (h.k, v.k), (h.v, v.v), (h.ctx, v.ctx),
            (h.mask, v.mask), (h.cos, v.cos), (h.sin, v.sin),
        )
    ]

    units = [pl.ds(pl.multiple_of(shard_of[j] * ff, 128), ff) for j in range(4)]
    outs = [(o.gate.at[:, cols], o.up.at[:, cols]) for cols in units]
    outs += [halves_of(o.o), halves_of(o.qkv)]
    outs += [halves_of(rows_of(o.down, k * half_d, half_d)) for k in (0, 1)]
    chunk = [set_one.at[0], set_one.at[1], set_one.at[0], set_one.at[1]]
    chunk += [down.at[pl.ds(0, head_rows)], down.at[pl.ds(half_d, rows), pl.ds(0, qkv_cols)]]
    chunk += [down.at[pl.ds(0, half_d)], down.at[pl.ds(half_d, half_d)]]
    ring = Ring(
        R,
        [halves_of(a) for a in chunk],
        outs,
        [slots_b.at[0], slots_b.at[1], slots_b.at[0], slots_b.at[1]]
        + [slots_a.at[0], slots_a.at[1]] * 2,
        v.sums, v.spread, v.sent, v.kept,
    )
    copies = Copies(v.send, v.recv)

    def do(work, k, steps):
        count, make = work
        each = -(-count // steps)

        @pl.loop(0, each)
        def _(j):
            i = (k - 1) * each + j

            @pl.when(i < count)
            def _():
                make(i)

    def do_all(work):
        count, make = work

        @pl.loop(0, count)
        def _(i):
            make(i)

    def sum_phase(pair, works=()):
        @pl.loop(1, R)
        def _(k):
            for a in pair:
                ring.sum_step(a, k)
            for work in works:
                do(work, k, R - 1)

    def spread_phase(pair, works=(), before=lambda: None, following=()):
        @pl.loop(1, R - 1)
        def _(k):
            for a in pair:
                ring.spread_step(a, k)
            for work in works:
                do(work, k, R - 2)

        before()
        for a in following:
            ring.start(a)
        for a in pair:
            ring.spread_step(a, R - 1, last=True)
            ring.finish(a)

    def turn_over(source, into):
        @pl.loop(0, source.shape[0] // 128)
        def _(i):
            at = pl.ds(pl.multiple_of(i * 128, 128), 128)
            into[:, at] = source[at].T

    load_down.wait()
    pl.semaphore_wait(barrier, R + 2)
    for a in (6, 7):
        ring.start(a)

    core_b = copies.start(rows_of(h.part, 2 * tok + (1 - c) * tok, tok), got_b, core_dev)
    load_near.wait()
    turn_over(own_two, v.near_t)
    core_a = copies.start(rows_of(h.part, (1 - c) * tok, tok), got_a, core_dev)
    load_b.wait()
    copies.arrived(core_b, got_b)
    mine_b[...] = (mine_b[...].astype(f32) + got_b[...].astype(f32)).astype(bf16)
    far = copies.start(mine_b, got_far, row_dev)
    load_gu.wait()
    core_gu = copies.start(gu_own, gu_near, core_dev)
    quarter = gu_own.shape[0] // 4
    row_gu = [
        copies.start(gu_own.at[pl.ds(i * quarter, quarter)], gu_row.at[pl.ds(i * quarter, quarter)], row_dev)
        for i in (0, 1)
    ]
    small = []
    for j, device in ((2, row_dev), (3, diag_dev), (1, core_dev)):
        for whole, into, size in ((h.ctx, v.in_ctx, head_rows), (h.one, v.in_one, rows)):
            source = columns(whole, shard_of[j], size)
            small.append((copies.start(source, block(into, j), device), block(into, j)))
    own_parts = [
        load(columns(h.ctx, s, head_rows), block(v.in_ctx, 0)),
        load(columns(h.one, s, rows), block(v.in_one, 0)),
    ]

    sum_phase((6, 7), (product(v.near_t, gu_own, chunk[0]),))

    load_a.wait()
    for copy in later:
        copy.wait()
    load_w.wait()
    copies.arrived(core_a, got_a)
    copies.arrived(far, got_far)
    copies.arrived(core_gu, gu_near)
    gain, gain_part = v.gain, v.gain_part
    gain_part[...] = jnp.zeros_like(gain_part)
    step = 32
    groups = step // 8

    def fold(values):
        return jnp.sum(values.reshape(groups, 8, width), axis=0)

    def at_rows(i):
        return pl.ds(pl.multiple_of(i * step, step), step)

    def residual_two(i):
        b = at_rows(i)
        two = mine_a[b].astype(f32) + got_a[b].astype(f32) + got_far[b].astype(f32)
        hidden = hid[b]
        inv = lax.rsqrt(jnp.mean(hidden * hidden, axis=1, keepdims=True) + epsilon)
        gain_part[1] += fold(two * hidden * inv)
        scaled = two * gain[1:2]
        dot = jnp.mean(scaled * hidden, axis=1, keepdims=True)
        out = cot[b].astype(f32) + inv * (scaled - hidden * inv * inv * dot)
        grad_hid[b] = out
        all_gh[b] = out.astype(bf16)

    spread_phase(
        (6, 7),
        ((tok // step, residual_two), product(v.near_t, gu_near, chunk[1])),
        following=(0, 1),
    )
    near_gh = copies.start(block(all_gh, 0), block(all_gh, 1), core_dev)
    row_gh = copies.start(block(all_gh, 0), block(all_gh, 2), row_dev)
    row_gu.append(
        copies.start(gu_own.at[pl.ds(2 * quarter, quarter)], gu_row.at[pl.ds(2 * quarter, quarter)], row_dev)
    )

    for copy in attention:
        copy.wait()
    sum_k, sum_v = v.sum_k, v.sum_v
    sum_k[...] = jnp.zeros_like(sum_k)
    sum_v[...] = jnp.zeros_like(sum_v)
    group = q_cols // kv_cols
    lane = lax.broadcasted_iota(jnp.int32, (tok, 2 * HD), 1)
    front = lane < HD
    lower = lax.rem(lane, HD) < HD // 2

    def turn_back(part):
        other = jnp.where(lower, pltpu.roll(part, 2 * HD - HD // 2, 1), pltpu.roll(part, HD // 2, 1))
        return part * v.cos[...] + other * v.sin[...]

    def head_pair(u):
        lanes = pl.ds(pl.multiple_of(u * 2 * HD, 128), 2 * HD)
        kv = lax.div(2 * u, group)
        grad_ctx = matmul_nt(block(all_gh, 0)[...], weights[pl.ds(pl.multiple_of(u * 2 * HD, 128), 2 * HD)])
        grad_ctx = grad_ctx.astype(bf16)
        query, keys, values = v.q[:, lanes], v.k[kv], v.v[kv]
        shares = grad_ctx.astype(f32) * v.ctx[:, lanes].astype(f32)
        allowed = v.mask[...] > 0
        zero = jnp.zeros_like(query)
        grad_q = jnp.zeros((tok, 2 * HD), f32)
        grad_k = jnp.zeros((tok, 2 * HD), f32)
        grad_v = jnp.zeros((tok, 2 * HD), f32)
        for e in (0, 1):
            own = front if e == 0 else jnp.logical_not(front)
            own_q, own_g = jnp.where(own, query, zero), jnp.where(own, grad_ctx, zero)
            row_dot = jnp.sum(jnp.where(own, shares, 0.0), axis=1, keepdims=True)
            scores = jnp.where(allowed, matmul_nt(own_q, keys) * scaling, neg_large)
            top = jnp.max(scores, axis=1, keepdims=True)
            weight = jnp.exp(scores - top)
            probs = weight / jnp.sum(weight, axis=1, keepdims=True)
            grad_probs = matmul_nt(own_g, values)
            grad_scores = (probs * (grad_probs - row_dot) * scaling).astype(bf16)
            grad_q += matmul(grad_scores, jnp.where(own, keys, zero))
            grad_k += matmul_tn(grad_scores, own_q)
            grad_v += matmul_tn(probs.astype(bf16), own_g)
        all_gq[0:tok, lanes] = turn_back(grad_q).astype(bf16)
        sum_k[kv] += grad_k
        sum_v[kv] += grad_v

    pairs = q_cols // (2 * HD)

    def one_pair(k):
        @pl.when(k <= pairs)
        def _():
            head_pair(k - 1)

    @pl.loop(1, R)
    def _(k):
        for a in (0, 1):
            ring.sum_step(a, k)
        one_pair(k)

    if pairs > R - 1:

        @pl.loop(R - 1, pairs)
        def _(u):
            head_pair(u)

    for j in range(kv_cols // (2 * HD)):
        both = []
        for sums in (sum_k, sum_v):
            one, two = sums[2 * j], sums[2 * j + 1]
            one, two = one + pltpu.roll(one, HD, 1), two + pltpu.roll(two, HD, 1)
            both.append(jnp.where(front, one, two))
        at = q_cols + j * 2 * HD
        all_gq[0:tok, at : at + 2 * HD] = turn_back(both[0]).astype(bf16)
        at += kv_cols
        all_gq[0:tok, at : at + 2 * HD] = both[1].astype(bf16)
    near_gq = copies.start(block(all_gq, 0), block(all_gq, 1), core_dev)
    row_gq = copies.start(block(all_gq, 0), block(all_gq, 2), row_dev)
    row_gu.append(
        copies.start(gu_own.at[pl.ds(3 * quarter, quarter)], gu_row.at[pl.ds(3 * quarter, quarter)], row_dev)
    )

    copies.arrived(near_gh, block(all_gh, 1))
    copies.arrived(row_gh, block(all_gh, 2))
    far_gh = copies.start(block(all_gh, 2), block(all_gh, 3), core_dev)
    for number, landed in small:
        copies.arrived(number, landed)
    for copy in own_parts:
        copy.wait()
    turn_over(v.in_ctx, all_ctx)
    turn_over(v.in_one, all_one)
    copies.arrived(far_gh, block(all_gh, 3))
    tile = q_tiles.shape[1]

    def q_tile(i):
        source = rows_of(h.w_qkv, i * tile, tile)
        at = lax.rem(i, 2)
        return pltpu.make_async_copy(source, q_tiles.at[at], v.tiled.at[at])

    tiles = width // tile
    q_tile(0).start()

    def grad_one(i):
        q_tile(i).wait()

        @pl.when(i + 1 < tiles)
        def _():
            q_tile(i + 1).start()

        hid[:, pl.ds(pl.multiple_of(i * tile, 128), tile)] = matmul_nt(
            block(all_gq, 0)[...], q_tiles[lax.rem(i, 2)]
        )

    load_w = load(h.w_down, weights)

    def before_qkv():
        copies.arrived(near_gq, block(all_gq, 1))
        copies.arrived(row_gq, block(all_gq, 2))
        far_gq = copies.start(block(all_gq, 2), block(all_gq, 3), core_dev)
        copies.arrived(far_gq, block(all_gq, 3))
        do_all(product(all_one, all_gq, chunk[5]))

    spread_phase(
        (0, 1),
        ((tiles, grad_one), product(all_ctx, all_gh, chunk[4])),
        before_qkv,
        (4, 5),
    )

    def residual_one(i):
        b = at_rows(i)
        one, x = hid[b], x_in[b].astype(f32)
        inv = lax.rsqrt(jnp.mean(x * x, axis=1, keepdims=True) + epsilon)
        gain_part[0] += fold(one * x * inv)
        scaled = one * gain[0:1]
        dot = jnp.mean(scaled * x, axis=1, keepdims=True)
        o.tokens[b] = (grad_hid[b] + inv * (scaled - x * inv * inv * dot)).astype(bf16)

    sum_phase((4, 5), ((tok // step, residual_one),))
    load_hid = load(h.hid, hid)

    gain_own, gain_in, gain_all = v.gain_own, v.gain_in, v.gain_all
    for i in (0, 1):
        gain_own[i : i + 1] = jnp.sum(gain_part[i], axis=0, keepdims=True)

    def gain_slice(shard):
        return gain_own.at[:, pl.ds(pl.multiple_of(shard * rows, 128), rows)]

    gains_in = [
        copies.start(gain_slice(shard_of[j]), gain_in.at[j], device)
        for j, device in ((1, core_dev), (2, row_dev), (3, diag_dev))
    ]

    for i, number in enumerate(row_gu):
        copies.arrived(number, gu_row.at[pl.ds(i * quarter, quarter)])
    diag_gu = copies.start(gu_row, gu_near, core_dev)
    copies.arrived(diag_gu, gu_near)
    spread_phase(
        (4, 5),
        (product(v.near_t, gu_row, chunk[2], True), product(v.near_t, gu_near, chunk[3], True)),
        following=(2, 3),
    )

    for j, number in enumerate(gains_in):
        copies.arrived(number, gain_in.at[j + 1])
    gain_all[r] = gain_slice(s)[...] + gain_in[1] + (gain_in[2] + gain_in[3])

    def gain_copy(d):
        return pltpu.make_async_remote_copy(
            src_ref=gain_all.at[r],
            dst_ref=gain_all.at[r],
            send_sem=v.gain_send.at[d],
            recv_sem=v.gain_recv.at[d],
            device_id=(lax.rem(r + d, R), s),
            device_id_type=pl.DeviceIdType.MESH,
        )

    @pl.loop(1, R)
    def _(d):
        gain_copy(d).start()

    copies.finish()
    act = gu_row.at[:, pl.ds(0, ff)]
    load(h.act, act).wait()
    load_w.wait()
    load_hid.wait()
    sum_phase((2, 3), (product(act, weights, gu_own),))
    half = 2 * tok
    core_b = copies.start(rows_of(gu_own, half + (1 - c) * tok, tok), got_b, core_dev)
    core_a = copies.start(rows_of(gu_own, (1 - c) * tok, tok), got_a, core_dev)
    copies.arrived(core_b, got_b)
    mine_b[...] = (
        rows_of(gu_own, half + c * tok, tok)[...].astype(f32) + got_b[...].astype(f32)
    ).astype(bf16)
    far = copies.start(mine_b, got_far, row_dev)
    spread_phase((2, 3))
    copies.arrived(core_a, got_a)
    copies.arrived(far, got_far)

    @pl.loop(0, tok // step)
    def _(i):
        b = at_rows(i)
        own = rows_of(gu_own, c * tok + i * step, step)[...].astype(f32)
        out = hid[b] + own + got_a[b].astype(f32) + got_far[b].astype(f32)
        o.out[b] = out.astype(bf16)

    @pl.loop(1, R)
    def _(d):
        source = lax.rem(r + R - d, R)
        landed = gain_all.at[source]
        pltpu.make_async_copy(landed, landed, v.gain_recv.at[d]).wait()
        gain_copy(d).wait_send()

    total = gain_all[0]
    for q in range(1, R):
        total = total + gain_all[q]
    o.gains[...] = total
    copies.finish()


def backward(R, **given):
    h = types.SimpleNamespace(**given)
    tok, width = h.x.shape
    gu = h.gu.shape
    tokens, S = gu[0], gu[0] // tok
    rows, head_rows = width // S, h.w_o.shape[0] // S
    qkv_cols = h.w_qkv.shape[1]
    half_d = h.down.shape[0] // 2
    down = h.down.shape
    assert half_d >= rows and down[1] >= qkv_cols and gu == (tokens, width), "unsupported sizes"
    slot = slice_shape((max(rows, half_d), width // 2), R)[:2]
    full = (rows, S * gu[1] // 2)
    V = lambda shape, dtype=bf16: pltpu.VMEM(shape, dtype)
    dma = pltpu.SemaphoreType.DMA
    outs = dict(
        gate=(full, bf16, False),
        up=(full, bf16, False),
        o=((head_rows, width), bf16, False),
        qkv=((rows, qkv_cols), bf16, False),
        down=(down, bf16, False),
        tokens=((tok, width), bf16, True),
        out=((tok, width), bf16, True),
        gains=((2, rows), f32, True),
    )
    same = lambda a: V(a.shape, a.dtype)
    scratch = dict(
        down=same(h.down),
        set_one=V((2, rows, width)),
        slots_a=V((2, 2, R - 1) + slot),
        slots_b=V((2, 2, R - 1) + slot),
        gu_own=V(gu),
        gu_near=V(gu),
        gu_row=V(gu),
        near_t=V((rows, tokens)),
        in_ctx=V((tokens, head_rows)),
        in_one=V((tokens, rows)),
        all_gh=V((tokens, width)),
        all_gq=V((tokens, qkv_cols)),
        all_ctx=V((head_rows, tokens)),
        all_one=V((rows, tokens)),
        mine_a=V((tok, width)),
        mine_b=V((tok, width)),
        got_a=V((tok, width)),
        got_b=V((tok, width)),
        got_far=V((tok, width)),
        hid=V((tok, width), f32),
        x_in=V((tok, width)),
        cot=V((tok, width)),
        grad_hid=V((tok, width), f32),
        weights=V(h.w_o.shape),
        q_tiles=V((2, 256, qkv_cols)),
        gain=same(h.gain),
        q=same(h.q),
        k=same(h.k),
        v=same(h.v),
        ctx=same(h.ctx),
        mask=same(h.mask),
        cos=same(h.cos),
        sin=same(h.sin),
        sum_k=V(h.k.shape, f32),
        sum_v=V(h.k.shape, f32),
        gain_part=V((2, 8, width), f32),
        gain_own=V((2, width), f32),
        gain_in=V((S, 2, rows), f32),
        gain_all=V((R, 2, rows), f32),
        sums=dma((8, 2, R - 1)),
        spread=dma((8, 2, R - 1)),
        sent=dma((8, 2, 2)),
        kept=dma((8, 2)),
        send=dma((32,)),
        recv=dma((32,)),
        loaded=dma((32,)),
        tiled=dma((2,)),
        gain_send=dma((R,)),
        gain_recv=dma((R,)),
    )
    keys = tuple(given), tuple(outs), tuple(scratch)
    return pl.pallas_call(
        functools.partial(backward_kernel, R, keys),
        out_shape=[jax.ShapeDtypeStruct(shape, dtype) for shape, dtype, _ in outs.values()],
        in_specs=[pl.BlockSpec(memory_space=pl.ANY)] * len(given),
        out_specs=[
            pl.BlockSpec(memory_space=pltpu.VMEM if near else pl.ANY) for *_, near in outs.values()
        ],
        scratch_shapes=list(scratch.values()),
        compiler_params=pltpu.CompilerParams(
            collective_id=2, has_side_effects=True, vmem_limit_bytes=67043328
        ),
        name="backward",
    )(*given.values())


def widen_kernel(splits, *refs):
    count = len(splits)
    outs = iter(refs[count:])
    for ref, widths in zip(refs, splits):
        at = 0
        for width in widths:
            out = next(outs)
            out[...] = ref[:, at : at + width].astype(out.dtype)
            at += width


def widen(arrays, steps=4):
    in_specs, out_specs, out_shape = [], [], []
    for arr, widths, dtype in arrays:
        h = arr.shape[0] // steps
        in_specs.append(pl.BlockSpec((h, arr.shape[1]), lambda i: (i, 0)))
        for width in widths:
            out_specs.append(pl.BlockSpec((h, width), lambda i: (i, 0)))
            out_shape.append(jax.ShapeDtypeStruct((arr.shape[0], width), dtype))
    return pl.pallas_call(
        functools.partial(widen_kernel, [widths for _, widths, _ in arrays]),
        grid=(steps,),
        in_specs=in_specs,
        out_specs=out_specs,
        out_shape=out_shape,
        name="widen",
    )(*[arr for arr, *_ in arrays])


def per_device(
    R,
    S,
    tokens_in,
    cotangent,
    segment_ids,
    attn_gain,
    w_query,
    w_key,
    w_value,
    w_output,
    mlp_gain,
    w_gate,
    w_up,
    w_down,
):
    batches, length, width = tokens_in.shape
    tokens = batches * length
    assert batches == 1, "unsupported sizes"
    q_cols, kv_cols = w_query.shape[1], w_key.shape[1]
    exponent = jnp.arange(HD // 2).astype(f32) * (2.0 / HD)
    x = tokens_in.reshape(tokens, width)
    cot = cotangent.reshape(tokens, width)
    f = forward(
        S,
        x=x,
        cot=cot,
        gain=jnp.stack([attn_gain, mlp_gain]).astype(f32),
        w_q=w_query,
        w_kv=jnp.concatenate([w_key, w_value], axis=1),
        w_o=w_output,
        w_gate=w_gate,
        w_up=w_up,
        w_down=w_down,
        segments=segment_ids,
        speed=jnp.tile(theta_base ** (-exponent), 4)[None],
    )
    out = backward(
        R,
        down=f.down,
        part=f.part,
        gu=f.gu,
        two=f.two,
        hid=f.hid,
        x=x,
        cot=cot,
        gain=f.gain,
        w_o=f.w_o,
        w_down=w_down,
        w_qkv=f.w_qkv,
        act=f.act,
        q=f.q,
        k=f.k,
        v=f.v,
        ctx=f.ctx,
        mask=f.mask,
        cos=f.cos,
        sin=f.sin,
        one=f.one,
    )
    gate, up, o, qkv, down, grad_tokens, tokens_out, gains = out
    full = gate.shape[1]
    gate, up, o, *qkv, down, grad_tokens, tokens_out = widen(
        [
            (gate, (full,), f32),
            (up, (full,), f32),
            (o, (width,), f32),
            (qkv, (q_cols, kv_cols, kv_cols), f32),
            (down, (width,), f32),
            (grad_tokens, (width,), bf16),
            (tokens_out, (width,), bf16),
        ]
    )
    return (
        tokens_out.reshape(tokens_in.shape),
        grad_tokens.reshape(tokens_in.shape),
        gains[0],
        *qkv,
        o,
        gains[1],
        gate,
        up,
        down,
    )


def solution(mesh):
    R, S = mesh.shape["replica"], mesh.shape["shard"]
    assert S == 4 and R % 4 == 0, "unsupported mesh"
    data = P(AXES, None, None)
    rowwise = P("shard", None)
    flat = P("shard")
    return jax.shard_map(
        functools.partial(per_device, R, S),
        mesh=mesh,
        in_specs=((data, data, P(AXES, None), flat) + (rowwise,) * 4 + (flat,) + (rowwise,) * 3),
        out_specs=(data, data, flat) + (rowwise,) * 4 + (flat,) + (rowwise,) * 3,
        check_vma=False,
    )
```

```python
import functools
import math
import types

import jax
import jax.numpy as jnp
from jax import lax
from jax.experimental import pallas as pl
from jax.experimental.pallas import tpu as pltpu
from jax.sharding import PartitionSpec as P

KV = 4
HD = 64

epsilon = 1e-05
theta_base = 500000.0
neg_large = -1e30


AXES = ("replica", "shard")
f32 = jnp.float32
bf16 = jnp.bfloat16


def matmul(left_arr, right_arr):
    return jnp.dot(left_arr, right_arr, preferred_element_type=f32)


def matmul_nt(left_arr, right_arr):
    return lax.dot_general(
        left_arr, right_arr, (((1,), (1,)), ((), ())), preferred_element_type=f32
    )


def matmul_tn(left_arr, right_arr):
    return lax.dot_general(
        left_arr, right_arr, (((0,), (0,)), ((), ())), preferred_element_type=f32
    )


class Copies:
    def __init__(self, send, recv):
        self.send, self.recv, self.count, self.open = send, recv, 0, {}

    def start(self, src, dst, device):
        copy = pltpu.make_async_remote_copy(
            src_ref=src,
            dst_ref=dst,
            send_sem=self.send.at[self.count],
            recv_sem=self.recv.at[self.count],
            device_id=device,
            device_id_type=pl.DeviceIdType.MESH,
        )
        self.count += 1
        copy.start()
        self.open[self.count - 1] = copy
        return self.count - 1

    def sent(self, number):
        self.open.pop(number).wait_send()

    def arrived(self, number, landed):
        pltpu.make_async_copy(landed, landed, self.recv.at[number]).wait()

    def finish(self):
        for number in tuple(self.open):
            self.sent(number)


def meet(devices):
    barrier = pltpu.get_barrier_semaphore()
    for device in devices:
        pl.semaphore_signal(
            barrier, inc=1, device_id=device, device_id_type=pl.DeviceIdType.MESH
        )
    pl.semaphore_wait(barrier, len(devices))


def forward_kernel(keys, *refs):
    given = iter(refs)
    h, o, v = (types.SimpleNamespace(**{key: next(given) for key in group}) for group in keys)
    r, s = lax.axis_index("replica"), lax.axis_index("shard")
    c, y = lax.rem(s, 2), lax.div(s, 2)
    x = lax.rem(r, 2)
    w = lax.rem(lax.div(r, 2), 2)
    near, row = 2 * y + 1 - c, 2 * (1 - y) + c
    diagonal = 2 * (1 - y) + 1 - c
    core_dev, row_dev, diag_dev = (r, near), (r, row), (r, diagonal)
    x_dev, z_dev = (r + 1 - 2 * x, s), (r + 2 - 4 * w, s)
    copies = Copies(v.send, v.recv)
    loads, saves = [], []

    def move(source, into, kind, sems):
        copy = pltpu.make_async_copy(source, into, sems.at[len(kind)])
        kind.append(copy)
        copy.start()
        return copy

    def load(source, into):
        return move(source, into, loads, v.loaded)

    def save(source, into):
        return move(source, into, saves, v.saved)

    tok, width = h.x.shape
    ff = v.all_gu.shape[1] // 2
    q_cols, kv_cols = v.q.shape[1], v.all_kv.shape[1] // 2
    m_g = h.w_gate.shape[0]
    q_g = m_g // 4

    def rows_of(ref, start, size):
        return ref.at[pl.ds(pl.multiple_of(start, 16), size)]

    def columns_of(ref, start, size, shard):
        return ref.at[
            pl.ds(pl.multiple_of(start, 16), size), pl.ds(pl.multiple_of(shard * ff, 128), ff)
        ]

    def quarter(flip_x, flip_z):
        at_x = (1 - x) if flip_x else x
        at_z = (1 - w) if flip_z else w
        return 2 * at_z + at_x

    here = quarter(0, 0)

    def gu_part(owner, start, size):
        return [
            v.all_gu.at[pl.ds(pl.multiple_of(owner * m_g + start, 16), size), pl.ds(k * ff, ff)]
            for k in (0, 1)
        ]

    load_x = load(h.x, v.x_in)
    gains = [(h.gain_one, v.gain_one), (h.gain_two, v.gain_two)]

    def gain_at(ref, shard):
        return ref.at[:, pl.ds(pl.multiple_of(shard * m_g, 128), m_g)]

    load_gain = [load(a, gain_at(b, s)) for a, b in gains]
    keys, values = (v.all_kv.at[:, pl.ds(k * kv_cols, kv_cols)] for k in (0, 1))
    plain = [(h.w_q, v.all_q, True), (h.w_k, keys, False), (h.w_v, values, False), (h.w_o, v.all_o, False)]
    load_own = [load(a, rows_of(b, s * a.shape[0], a.shape[0])) for a, b, _ in plain]
    load_small = [load(h.segments, v.segments)]
    own_cot = rows_of(v.all_cot, c * tok, tok)
    load_gu = [
        load(columns_of(a, 0, m_g, s), part)
        for a, part in zip((h.w_gate, h.w_up), gu_part(s, 0, m_g))
    ]
    load_gu += [load(h.cot, own_cot), load(h.w_down, v.w_down)]

    meet([core_dev, row_dev, diag_dev, x_dev, z_dev])

    gain_parts = []
    for device, owner in ((core_dev, near), (row_dev, row), (diag_dev, diagonal)):
        for a, b in gains:
            gain_parts.append((copies.start(a, gain_at(b, s), device), gain_at(b, owner)))

    flows, first = [], []
    for a, b, x_first in plain:
        m = a.shape[0]
        part = rows_of(a, here * (m // 4), m // 4)
        region = functools.partial(
            lambda b, m, owner, spot: rows_of(b, owner * m + spot * (m // 4), m // 4), b, m
        )
        first.append(copies.start(part, region(s, here), row_dev))
        flows.append((region, row, True, x_first))
    for shard, device in ((row, row_dev), (diagonal, diag_dev)):
        for k, a in enumerate((h.w_gate, h.w_up)):
            region = functools.partial(
                lambda k, owner, spot: v.all_gu.at[
                    pl.ds(pl.multiple_of(owner * m_g + spot * q_g, 16), q_g), pl.ds(k * ff, ff)
                ],
                k,
            )
            part = columns_of(a, here * q_g, q_g, shard)
            first.append(copies.start(part, region(s, here), device))
            flows.append((region, shard, False, k == 0))
    far_cot = rows_of(v.all_cot, 2 * tok + c * tok, tok)
    row_cot = copies.start(h.cot, far_cot, row_dev)

    core_plain = []
    for a, b, _ in plain:
        m = a.shape[0]
        core_plain.append((copies.start(a, rows_of(b, s * m, m), core_dev), rows_of(b, near * m, m)))
    core_gu = [
        (copies.start(columns_of(a, 0, m_g, near), part, core_dev), landed)
        for a, part, landed in zip(
            (h.w_gate, h.w_up), gu_part(s, 0, m_g), gu_part(near, 0, m_g)
        )
    ]
    core_gu.append(
        (copies.start(h.cot, own_cot, core_dev), rows_of(v.all_cot, (1 - c) * tok, tok))
    )

    second, third = {}, {}
    forwarded = {i: [] for i in range(len(flows))}

    def to_core(i, part, spot):
        if flows[i][2]:
            forwarded[i].append((copies.start(part, part, core_dev), spot))

    def stage(i, number):
        region, owner, _, x_first = flows[i]
        flip = (1, 0) if x_first else (0, 1)
        one, two = (x_dev, z_dev) if x_first else (z_dev, x_dev)
        piece, other = region(owner, here), region(owner, quarter(*flip))
        if number == 1:
            copies.arrived(first[i], piece)
            second[i] = copies.start(piece, piece, one)
            to_core(i, piece, (0, 0))
        elif number == 2:
            copies.arrived(second[i], other)
            third[i] = [
                (copies.start(part, part, two), spot)
                for part, spot in ((piece, (0, 0)), (other, flip))
            ]
            to_core(i, other, flip)
        elif number == 3:
            for sent, (fx, fz) in third[i]:
                spot = (fx, 1 - fz) if x_first else (1 - fx, fz)
                part = region(owner, quarter(*spot))
                copies.arrived(sent, part)
                to_core(i, part, spot)
        else:
            for sent, spot in forwarded[i]:
                copies.arrived(sent, region(diagonal, quarter(*spot)))

    step = 32

    def at_rows(i):
        return pl.ds(pl.multiple_of(i * step, step), step)

    def norm(source, which, into):
        @pl.loop(0, tok // step)
        def _(i):
            b = at_rows(i)
            values = source[b].astype(f32)
            inv = lax.rsqrt(jnp.mean(values * values, axis=1, keepdims=True) + epsilon)
            into[b] = (values * inv * v.gain[which : which + 1]).astype(bf16)

    for i in (0, 1, 2):
        stage(i, 1)
    for copy in load_small:
        copy.wait()

    along = jnp.broadcast_to(v.segments[...], (tok, tok))
    query_at = lax.broadcasted_iota(jnp.int32, (tok, tok), 0)
    key_at = lax.broadcasted_iota(jnp.int32, (tok, tok), 1)
    allowed = (along.T == along) & (query_at >= key_at)
    v.mask[...] = jnp.where(allowed, 1.0, 0.0)
    position = jnp.sum(v.mask[...], axis=1, keepdims=True) - 1.0
    lane = lax.broadcasted_iota(jnp.int32, (tok, 2 * HD), 1)
    front = lane < HD
    lower = lax.rem(lane, HD) < HD // 2
    turn_of = lax.rem(lane[0:8], HD // 2).astype(f32) * (2.0 / HD)
    speed = jnp.exp(turn_of * -math.log(theta_base))[0:1]
    angle = position * speed
    v.cos[...] = jnp.cos(angle)
    sine = jnp.sin(angle)
    v.sin[...] = jnp.where(lower, sine, -sine)
    save(v.mask, o.mask)
    save(v.cos, o.cos)
    save(v.sin, o.sin)
    for i, number in ((0, 2), (1, 2), (2, 2), (3, 1), (4, 1)):
        stage(i, number)
    load_x.wait()
    for copy in load_gain:
        copy.wait()
    for sent, landed in gain_parts:
        copies.arrived(sent, landed)
    for i, (_, b) in enumerate(gains):
        v.gain[i : i + 1] = b[...].astype(f32)
    norm(v.x_in, 0, v.one)
    save(v.one, o.one)
    for copy in load_own:
        copy.wait()
    for i, number in ((1, 3), (2, 3), (5, 1), (0, 3), (6, 1), (3, 2), (4, 2), (5, 2)):
        stage(i, number)
    for sent, landed in core_plain:
        copies.arrived(sent, landed)
    for i in (0, 1, 2):
        stage(i, 4)

    def turn(part):
        other = jnp.where(lower, pltpu.roll(part, 2 * HD - HD // 2, 1), pltpu.roll(part, HD // 2, 1))
        return part * v.cos[...] - other * v.sin[...]

    def lanes_of(i):
        return pl.ds(pl.multiple_of(i * 2 * HD, 128), 2 * HD)

    @pl.loop(0, q_cols // 256)
    def _(i):
        part = matmul(v.one[...], v.all_q[:, pl.ds(pl.multiple_of(i * 256, 128), 256)])
        for j in (0, 1):
            half = part[:, j * 2 * HD : (j + 1) * 2 * HD]
            v.q[:, lanes_of(2 * i + j)] = turn(half).astype(bf16)

    for which, into in ((0, v.k), (1, v.v)):
        part = matmul(v.one[...], v.all_kv[:, which * kv_cols : (which + 1) * kv_cols])
        for j in range(kv_cols // (2 * HD)):
            half = part[:, j * 2 * HD : (j + 1) * 2 * HD]
            half = turn(half) if which == 0 else half
            swapped = pltpu.roll(half, HD, 1)
            into[2 * j] = jnp.where(front, half, swapped).astype(bf16)
            into[2 * j + 1] = jnp.where(front, swapped, half).astype(bf16)
    save(v.q, o.q)
    save(v.k, o.k)
    save(v.v, o.v)
    save(v.all_q, o.w_qkv.at[:, pl.ds(0, q_cols)])
    save(v.all_kv, o.w_qkv.at[:, pl.ds(q_cols, 2 * kv_cols)])
    stage(7, 1)

    group = q_cols // kv_cols
    scaling = 1.0 / math.sqrt(HD)

    def head_pair(u):
        kv = lax.div(2 * u, group)
        query, keys, values = v.q[:, lanes_of(u)], v.k[kv], v.v[kv]
        allowed = v.mask[...] > 0
        zero = jnp.zeros_like(query)
        context = jnp.zeros((tok, 2 * HD), f32)
        for e in (0, 1):
            own = front if e == 0 else jnp.logical_not(front)
            scores = jnp.where(
                allowed, matmul_nt(jnp.where(own, query, zero), keys) * scaling, neg_large
            )
            top = jnp.max(scores, axis=1, keepdims=True)
            weight = jnp.exp(scores - top)
            probs = (weight / jnp.sum(weight, axis=1, keepdims=True)).astype(bf16)
            context += matmul(probs, jnp.where(own, values, zero))
        v.ctx[:, lanes_of(u)] = context.astype(bf16)

    pairs = q_cols // (2 * HD)

    @pl.loop(0, pairs // 2)
    def _(u):
        head_pair(u)

    stage(6, 2)

    @pl.loop(pairs // 2, pairs)
    def _(u):
        head_pair(u)

    save(v.ctx, o.ctx)
    stage(3, 3)
    stage(3, 4)
    save(v.all_o, o.w_o)

    @pl.loop(0, width // 256)
    def _(i):
        columns = pl.ds(pl.multiple_of(i * 256, 128), 256)
        v.hid[:, columns] = v.x_in[:, columns].astype(f32) + matmul(v.ctx[...], v.all_o[:, columns])

    own_two = rows_of(v.two, c * tok, tok)
    norm(v.hid, 1, own_two)
    far_two = rows_of(v.two, 2 * tok + c * tok, tok)
    near_two = copies.start(own_two, own_two, core_dev)
    row_two = copies.start(own_two, far_two, row_dev)
    stage(7, 2)
    save(v.hid, o.hid)
    save(v.gain, o.gain)

    for copy in load_gu:
        copy.wait()
    for sent, landed in core_gu:
        copies.arrived(sent, landed)
    copies.arrived(near_two, rows_of(v.two, (1 - c) * tok, tok))

    half = 2 * m_g
    early = pl.ds(pl.multiple_of(y * half, 128), half)
    late = pl.ds(pl.multiple_of((1 - y) * half, 128), half)
    low, high = pl.ds(0, 2 * tok), pl.ds(2 * tok, 2 * tok)

    @pl.loop(0, 2 * ff // 256)
    def _(i):
        columns = pl.ds(pl.multiple_of(i * 256, 128), 256)
        v.sums[low, columns] = matmul(v.two[low, early], v.all_gu[early, columns])

    def grads_act(tokens, into):
        @pl.loop(0, ff // 256)
        def _(i):
            columns = pl.ds(pl.multiple_of(i * 256, 128), 256)
            into[:, columns] = matmul_nt(v.all_cot[tokens], v.w_down[columns])

    copies.arrived(row_cot, far_cot)
    last_cot = copies.start(far_cot, far_cot, core_dev)
    act_low, act_high = v.sums.at[high, pl.ds(0, ff)], v.grad_act
    grads_act(low, act_low)
    there = 2 * tok + (1 - c) * tok
    copies.arrived(last_cot, rows_of(v.all_cot, there, tok))
    grads_act(high, act_high)
    for i in (5, 4, 7, 6):
        stage(i, 3)
    save(v.all_gu, o.w_gu)

    def units(end):
        tokens = high if end else low

        @pl.loop(0, ff // 256)
        def _(i):
            columns = pl.ds(pl.multiple_of(i * 256, 128), 256)
            ups = pl.ds(pl.multiple_of(ff + i * 256, 128), 256)
            if end:
                gate = matmul(v.two[tokens], v.all_gu[:, columns])
                up = matmul(v.two[tokens], v.all_gu[:, ups])
            else:
                gate = v.sums[low, columns] + matmul(v.two[tokens, late], v.all_gu[late, columns])
                up = v.sums[low, ups] + matmul(v.two[tokens, late], v.all_gu[late, ups])
            grad_act = (act_high if end else act_low)[:, columns]
            sigmoid = jax.nn.sigmoid(gate)
            silu = gate * sigmoid
            v.act[tokens, columns] = (silu * up).astype(bf16)
            v.gu[tokens, columns] = (
                grad_act * up * sigmoid * (1.0 + gate * (1.0 - sigmoid))
            ).astype(bf16)
            v.gu[tokens, ups] = (grad_act * silu).astype(bf16)

    def down(end):
        tokens = pl.ds(end * 2 * tok, 2 * tok)

        @pl.loop(0, ff // 256)
        def _(i):
            units_at = pl.ds(pl.multiple_of(i * 256, 128), 256)
            turned = v.act[tokens, units_at].T

            @pl.loop(0, width // 512)
            def _(j):
                columns = pl.ds(pl.multiple_of(j * 512, 128), 512)
                part = matmul(turned, v.all_cot[tokens, columns])
                if end == 0:
                    v.sums[units_at, columns] = part
                else:
                    v.down[units_at, columns] = (v.sums[units_at, columns] + part).astype(bf16)

    def save_rows(end, *names):
        tokens = pl.ds(end * 2 * tok, 2 * tok)
        for a, b in names:
            save(a.at[tokens], b.at[tokens])

    units(0)
    save_rows(0, (v.act, o.act), (v.gu, o.gu), (v.two, o.two))
    down(0)
    copies.arrived(row_two, far_two)
    last_two = copies.start(far_two, far_two, core_dev)
    copies.arrived(last_two, rows_of(v.two, there, tok))
    units(1)
    save_rows(1, (v.two, o.two), (v.act, o.act), (v.gu, o.gu))
    down(1)
    save(v.down, o.down)
    copies.finish()
    for copy in saves:
        copy.wait()


def forward(S, **given):
    h = types.SimpleNamespace(**given)
    tok, width = h.x.shape
    ff, q_cols, kv_cols = h.w_down.shape[0], h.w_q.shape[1], h.w_k.shape[1]
    V = lambda shape, dtype=bf16: pltpu.VMEM(shape, dtype)
    dma = pltpu.SemaphoreType.DMA
    heads = (kv_cols // HD, tok, 2 * HD)
    many = S * tok
    outs = dict(
        w_qkv=(S * h.w_q.shape[0], q_cols + 2 * kv_cols),
        w_o=(S * h.w_o.shape[0], width),
        w_gu=(S * h.w_gate.shape[0], 2 * ff),
        gain=(2, width),
        one=(tok, width),
        q=(tok, q_cols),
        k=heads,
        v=heads,
        ctx=(tok, q_cols),
        hid=(tok, width),
        two=(many, width),
        act=(many, ff),
        gu=(many, 2 * ff),
        down=(ff, width),
        mask=(tok, tok),
        cos=(tok, 2 * HD),
        sin=(tok, 2 * HD),
    )
    scratch = dict(
        x_in=V((tok, width)),
        gain=V((2, width), f32),
        gain_one=V((1, width)),
        gain_two=V((1, width)),
        all_q=V((S * h.w_q.shape[0], q_cols)),
        all_kv=V((S * h.w_q.shape[0], 2 * kv_cols)),
        all_o=V((S * h.w_o.shape[0], width)),
        all_gu=V((S * h.w_gate.shape[0], 2 * ff)),
        all_cot=V((many, width)),
        w_down=V(h.w_down.shape),
        segments=V(h.segments.shape, h.segments.dtype),
        cos=V((tok, 2 * HD), f32),
        sin=V((tok, 2 * HD), f32),
        mask=V((tok, tok), f32),
        sums=V((ff, width), f32),
        down=V((ff, width)),
        grad_act=V((2 * tok, ff), f32),
        one=V((tok, width)),
        q=V((tok, q_cols)),
        k=V(heads),
        v=V(heads),
        ctx=V((tok, q_cols)),
        hid=V((tok, width), f32),
        two=V((many, width)),
        act=V((many, ff)),
        gu=V((many, 2 * ff)),
        send=dma((80,)),
        recv=dma((80,)),
        loaded=dma((24,)),
        saved=dma((32,)),
    )
    wide = ("hid", "gain", "mask", "cos", "sin")
    out = pl.pallas_call(
        functools.partial(forward_kernel, (tuple(given), tuple(outs), tuple(scratch))),
        out_shape=[
            jax.ShapeDtypeStruct(shape, f32 if name in wide else bf16)
            for name, shape in outs.items()
        ],
        in_specs=[pl.BlockSpec(memory_space=pl.ANY)] * len(given),
        out_specs=[pl.BlockSpec(memory_space=pl.ANY)] * len(outs),
        scratch_shapes=list(scratch.values()),
        compiler_params=pltpu.CompilerParams(
            collective_id=1, has_side_effects=True, vmem_limit_bytes=67043328
        ),
        name="forward",
    )(*given.values())
    return types.SimpleNamespace(**dict(zip(outs, out)))


def slice_shape(shape, parts):
    rows, cols = shape
    down = min(parts, rows // 16)
    across = parts // down
    assert rows % down == 0 and cols % (128 * across) == 0, "unsupported sizes"
    return rows // down, cols // across, across


def halves_of(ref):
    w = ref.shape[1] // 2
    return ref.at[:, pl.ds(0, w)], ref.at[:, pl.ds(w, w)]


class Ring:
    def __init__(self, R, chunks, outs, slots, sums, spread, sent, kept):
        self.R, self.chunks, self.outs, self.slots = R, chunks, outs, slots
        self.sums, self.spread, self.sent, self.kept = sums, spread, sent, kept
        r, self.s = lax.axis_index("replica"), lax.axis_index("shard")
        z, x = lax.div(r, 2), lax.rem(r, 2)
        self.place = z * (1 - x) + (R - 1 - z) * x
        self.peers = [self.replica_at(self.place + 1), self.replica_at(self.place + R - 1)]

    def replica_at(self, place):
        R = self.R
        place = lax.rem(place, R)
        back = lax.div(place, R // 2)
        return (1 - back) * 2 * place + back * (2 * (R - 1 - place) + 1)

    def part(self, halves, way, step):
        R, ref = self.R, halves[way]
        number = lax.rem(self.place + (R - step if way == 0 else step), R)
        h, w, across = slice_shape(ref.shape, R)
        return ref.at[
            pl.ds(pl.multiple_of(lax.div(number, across) * h, 16), h),
            pl.ds(pl.multiple_of(lax.rem(number, across) * w, 128), w),
        ]

    def slot(self, a, way, step):
        h, w, _ = slice_shape(self.chunks[a][0].shape, self.R)
        return self.slots[a].at[way, step, pl.ds(0, h), pl.ds(0, w)]

    def copy(self, a, way, step, src, dst, arrival):
        return pltpu.make_async_remote_copy(
            src_ref=src,
            dst_ref=dst,
            send_sem=self.sent.at[a, way, lax.rem(step, 2)],
            recv_sem=arrival,
            device_id=(self.peers[way], self.s),
            device_id_type=pl.DeviceIdType.MESH,
        )

    def start(self, a):
        for way in (0, 1):
            src = self.part(self.chunks[a], way, 0)
            self.copy(a, way, 0, src, self.slot(a, way, 0), self.sums.at[a, way, 0]).start()

    def sum_step(self, a, k):
        last = k == self.R - 1
        for way in (0, 1):
            slot = self.slot(a, way, k - 1)
            self.copy(a, way, 0, slot, slot, self.sums.at[a, way, k - 1]).wait_recv()
            own = self.part(self.chunks[a], way, k)
            slot[...] = (slot[...].astype(f32) + own[...].astype(f32)).astype(bf16)
            dst = self.part(self.outs[a], way, k)
            onward = self.copy(a, way, k, slot, dst, self.spread.at[a, way, 0])

            @pl.when(k >= 2)
            def _():
                self.copy(a, way, k, slot, slot, self.sums.at[a, way, 0]).wait_send()

            @pl.when(last)
            def _():
                onward.start()
                pltpu.make_async_copy(slot, dst, self.kept.at[a, way]).start()

            @pl.when(jnp.logical_not(last))
            def _():
                there = lax.rem(k, self.R - 1)
                self.copy(
                    a, way, k, slot, self.slot(a, way, there), self.sums.at[a, way, there]
                ).start()

    def spread_step(self, a, k, last=False):
        for way in (0, 1):
            dst = self.part(self.outs[a], way, lax.rem(k + self.R - 1, self.R))
            self.copy(a, way, 0, dst, dst, self.spread.at[a, way, k - 1]).wait_recv()
            if not last:
                onward = self.copy(a, way, k + self.R - 1, dst, dst, self.spread.at[a, way, k])
                onward.wait_send()
                onward.start()

    def finish(self, a):
        for way in (0, 1):
            slot = self.slot(a, way, self.R - 2)
            for step in (0, 1):
                self.copy(a, way, step, slot, slot, self.sums.at[a, way, 0]).wait_send()
            dst = self.part(self.outs[a], way, self.R - 1)
            pltpu.make_async_copy(slot, dst, self.kept.at[a, way]).wait()


def product(left, right, out, crossed=False, tile=256):
    half = right.shape[0] // 2

    def make(i):
        columns = pl.ds(pl.multiple_of(i * tile, 128), tile)
        if crossed:
            one = matmul(left[:, 0:half], right[pl.ds(half, half), columns])
            out[:, columns] = (one + matmul(left[:, half:], right[pl.ds(0, half), columns])).astype(bf16)
        else:
            out[:, columns] = matmul(left[...], right[:, columns]).astype(bf16)

    return out.shape[1] // tile, make


def backward_kernel(R, keys, *refs):
    given = iter(refs)
    h, o, v = (types.SimpleNamespace(**{key: next(given) for key in group}) for group in keys)
    r, s = lax.axis_index("replica"), lax.axis_index("shard")
    c, y = lax.rem(s, 2), lax.div(s, 2)
    near, row = 2 * y + 1 - c, 2 * (1 - y) + c
    diagonal = 2 * (1 - y) + 1 - c
    shard_of = (s, near, row, diagonal)
    core_dev, row_dev, diag_dev = (r, near), (r, row), (r, diagonal)

    barrier = pltpu.get_barrier_semaphore()
    for other in (near, row, diagonal):
        pl.semaphore_signal(
            barrier, inc=1, device_id=(r, other), device_id_type=pl.DeviceIdType.MESH
        )

    @pl.loop(1, R)
    def _(d):
        pl.semaphore_signal(
            barrier, inc=1, device_id=(lax.rem(r + d, R), s), device_id_type=pl.DeviceIdType.MESH
        )

    loads = []

    def load(source, into):
        copy = pltpu.make_async_copy(source, into, v.loaded.at[len(loads)])
        loads.append(copy)
        copy.start()
        return copy

    down, set_one, slots_a, slots_b = v.down, v.set_one, v.slots_a, v.slots_b
    gu_own, gu_near, gu_row = v.gu_own, v.gu_near, v.gu_row
    all_gh, all_gq, all_ctx, all_one = v.all_gh, v.all_gq, v.all_ctx, v.all_one
    mine_a, mine_b, got_a, got_b, got_far = v.mine_a, v.mine_b, v.got_a, v.got_b, v.got_far
    hid, x_in, cot, grad_hid = v.hid, v.x_in, v.cot, v.grad_hid
    weights = v.weights
    q_tiles = v.w_tiles.at[:, :, pl.ds(0, v.all_gq.shape[1])]
    tok, width = x_in.shape
    ff = gu_own.shape[1] // 2
    rows, head_rows = v.near_t.shape[0], weights.shape[0] // len(shard_of)
    q_cols = v.q.shape[1]
    qkv_cols = all_gq.shape[1]
    kv_cols = (qkv_cols - q_cols) // 2
    half_d = down.shape[0] // 2
    scaling = 1.0 / math.sqrt(HD)

    def rows_of(a, start, size):
        return a.at[pl.ds(pl.multiple_of(start, 16), size)]

    def block(a, j):
        return a.at[pl.ds(j * tok, tok)]

    def columns(a, j, size):
        return a.at[:, pl.ds(pl.multiple_of(j * size, 128), size)]

    load_down = load(h.down, down)
    tokens = gu_own.shape[0]
    load_gu = load(h.gu, gu_own)
    own_two = all_gq.at[:, pl.ds(0, rows)]
    load_near = load(h.two.at[:, pl.ds(pl.multiple_of(s * rows, 128), rows)], own_two)
    later = [
        load(source, into)
        for source, into in ((h.hid, hid), (h.x, x_in), (h.cot, cot), (h.gain, v.gain))
    ]
    load_w = load(h.w_o, weights)
    attention = [
        load(source, into)
        for source, into in (
            (h.q, v.q), (h.k, v.k), (h.v, v.v), (h.ctx, v.ctx),
            (h.mask, v.mask), (h.cos, v.cos), (h.sin, v.sin),
        )
    ]

    units = [pl.ds(pl.multiple_of(shard_of[j] * ff, 128), ff) for j in range(4)]
    outs = [(o.gate.at[:, cols], o.up.at[:, cols]) for cols in units]
    outs += [halves_of(o.o), halves_of(o.qkv)]
    outs += [halves_of(rows_of(o.down, k * half_d, half_d)) for k in (0, 1)]
    chunk = [set_one.at[0], set_one.at[1], set_one.at[0], set_one.at[1]]
    chunk += [down.at[pl.ds(0, head_rows)], down.at[pl.ds(half_d, rows), pl.ds(0, qkv_cols)]]
    chunk += [down.at[pl.ds(0, half_d)], down.at[pl.ds(half_d, half_d)]]
    ring = Ring(
        R,
        [halves_of(a) for a in chunk],
        outs,
        [slots_b.at[0], slots_b.at[1], slots_b.at[0], slots_b.at[1]]
        + [slots_a.at[0], slots_a.at[1]] * 2,
        v.sums, v.spread, v.sent, v.kept,
    )
    copies = Copies(v.send, v.recv)

    def do(work, k, steps):
        count, make = work
        each = -(-count // steps)

        @pl.loop(0, each)
        def _(j):
            i = (k - 1) * each + j

            @pl.when(i < count)
            def _():
                make(i)

    def do_all(work):
        count, make = work

        @pl.loop(0, count)
        def _(i):
            make(i)

    def sum_phase(pair, works=()):
        @pl.loop(1, R)
        def _(k):
            for a in pair:
                ring.sum_step(a, k)
            for work in works:
                do(work, k, R - 1)

    def spread_phase(pair, works=(), before=lambda: None, following=()):
        @pl.loop(1, R - 1)
        def _(k):
            for a in pair:
                ring.spread_step(a, k)
            for work in works:
                do(work, k, R - 2)

        before()
        for a in following:
            ring.start(a)
        for a in pair:
            ring.spread_step(a, R - 1, last=True)
            ring.finish(a)

    def turned(source, into):
        def make(i):
            at = pl.ds(pl.multiple_of(i * 128, 128), 128)
            into[:, at] = source[at].T

        return source.shape[0] // 128, make

    load_down.wait()
    pl.semaphore_wait(barrier, R + 2)
    for a in (6, 7):
        ring.start(a)

    load_near.wait()
    do_all(turned(own_two, v.near_t))
    load_gu.wait()
    core_gu = copies.start(gu_own, gu_near, core_dev)
    small = []
    for j, device in ((2, row_dev), (3, diag_dev), (1, core_dev)):
        for whole, into, size in ((h.ctx, v.in_ctx, head_rows), (h.one, v.in_one, rows)):
            source = columns(whole, shard_of[j], size)
            small.append((copies.start(source, block(into, j), device), block(into, j)))
    quarter = gu_own.shape[0] // 4

    def row_piece(i):
        at = pl.ds(i * quarter, quarter)
        return copies.start(gu_own.at[at], gu_row.at[at], row_dev)

    row_gu = [row_piece(0)]
    own_parts = [
        load(columns(h.ctx, s, head_rows), block(v.in_ctx, 0)),
        load(columns(h.one, s, rows), block(v.in_one, 0)),
    ]

    w_tiles = v.w_tiles
    w_tile = w_tiles.shape[1]

    def gu_tile(i):
        at = lax.rem(i, 2)
        return pltpu.make_async_copy(rows_of(h.w_gu, i * w_tile, w_tile), w_tiles.at[at], v.w_tiled.at[at])

    def grad_two(i):
        gu_tile(i).wait()

        @pl.when(i + 1 < width // w_tile)
        def _():
            gu_tile(i + 1).start()

        part = matmul_nt(gu_own[...], w_tiles[lax.rem(i, 2)]).astype(bf16)
        at = pl.ds(pl.multiple_of(i * w_tile, 128), w_tile)
        set_one[0, :, at] = part[: 2 * tok]
        set_one[1, :, at] = part[2 * tok :]

    gu_tile(0).start()
    sum_phase((6, 7), ((width // w_tile, grad_two),))

    core_b = copies.start(rows_of(set_one.at[1], (1 - c) * tok, tok), got_b, core_dev)
    core_a = copies.start(rows_of(set_one.at[0], (1 - c) * tok, tok), got_a, core_dev)
    mine_a[...] = rows_of(set_one.at[0], c * tok, tok)[...]
    copies.arrived(core_b, got_b)
    own_b = rows_of(set_one.at[1], c * tok, tok)[...]
    mine_b[...] = (own_b.astype(f32) + got_b[...].astype(f32)).astype(bf16)
    far = copies.start(mine_b, got_far, row_dev)
    row_gu.append(row_piece(1))
    copies.sent(core_b)
    copies.sent(core_a)

    for copy in later:
        copy.wait()
    load_w.wait()
    copies.arrived(core_a, got_a)
    copies.arrived(core_gu, gu_near)
    gain, gain_part = v.gain, v.gain_part
    gain_part[...] = jnp.zeros_like(gain_part)
    step = 32
    groups = step // 8

    def fold(values):
        return jnp.sum(values.reshape(groups, 8, width), axis=0)

    def at_rows(i):
        return pl.ds(pl.multiple_of(i * step, step), step)

    def residual_two(i):
        b = at_rows(i)
        two = mine_a[b].astype(f32) + got_a[b].astype(f32) + got_far[b].astype(f32)
        hidden = hid[b]
        inv = lax.rsqrt(jnp.mean(hidden * hidden, axis=1, keepdims=True) + epsilon)
        gain_part[1] += fold(two * hidden * inv)
        scaled = two * gain[1:2]
        dot = jnp.mean(scaled * hidden, axis=1, keepdims=True)
        out = cot[b].astype(f32) + inv * (scaled - hidden * inv * inv * dot)
        grad_hid[b] = out
        all_gh[b] = out.astype(bf16)

    def before_gh():
        copies.arrived(far, got_far)
        do_all((tok // step, residual_two))

    spread_phase(
        (6, 7),
        (product(v.near_t, gu_own, chunk[0]), product(v.near_t, gu_near, chunk[1])),
        before_gh,
        (0, 1),
    )
    near_gh = copies.start(block(all_gh, 0), block(all_gh, 1), core_dev)
    row_gh = copies.start(block(all_gh, 0), block(all_gh, 2), row_dev)
    row_gu.append(row_piece(2))

    for copy in attention:
        copy.wait()
    sum_k, sum_v = v.sum_k, v.sum_v
    sum_k[...] = jnp.zeros_like(sum_k)
    sum_v[...] = jnp.zeros_like(sum_v)
    group = q_cols // kv_cols
    lane = lax.broadcasted_iota(jnp.int32, (tok, 2 * HD), 1)
    front = lane < HD
    lower = lax.rem(lane, HD) < HD // 2

    def turn_back(part):
        other = jnp.where(lower, pltpu.roll(part, 2 * HD - HD // 2, 1), pltpu.roll(part, HD // 2, 1))
        return part * v.cos[...] + other * v.sin[...]

    def head_pair(u):
        lanes = pl.ds(pl.multiple_of(u * 2 * HD, 128), 2 * HD)
        kv = lax.div(2 * u, group)
        grad_ctx = matmul_nt(block(all_gh, 0)[...], weights[pl.ds(pl.multiple_of(u * 2 * HD, 128), 2 * HD)])
        grad_ctx = grad_ctx.astype(bf16)
        query, keys, values = v.q[:, lanes], v.k[kv], v.v[kv]
        shares = grad_ctx.astype(f32) * v.ctx[:, lanes].astype(f32)
        allowed = v.mask[...] > 0
        zero = jnp.zeros_like(query)
        grad_q = jnp.zeros((tok, 2 * HD), f32)
        grad_k = jnp.zeros((tok, 2 * HD), f32)
        grad_v = jnp.zeros((tok, 2 * HD), f32)
        for e in (0, 1):
            own = front if e == 0 else jnp.logical_not(front)
            own_q, own_g = jnp.where(own, query, zero), jnp.where(own, grad_ctx, zero)
            row_dot = jnp.sum(jnp.where(own, shares, 0.0), axis=1, keepdims=True)
            scores = jnp.where(allowed, matmul_nt(own_q, keys) * scaling, neg_large)
            top = jnp.max(scores, axis=1, keepdims=True)
            weight = jnp.exp(scores - top)
            probs = weight / jnp.sum(weight, axis=1, keepdims=True)
            grad_probs = matmul_nt(own_g, values)
            grad_scores = (probs * (grad_probs - row_dot) * scaling).astype(bf16)
            grad_q += matmul(grad_scores, jnp.where(own, keys, zero))
            grad_k += matmul_tn(grad_scores, own_q)
            grad_v += matmul_tn(probs.astype(bf16), own_g)
        all_gq[0:tok, lanes] = turn_back(grad_q).astype(bf16)
        sum_k[kv] += grad_k
        sum_v[kv] += grad_v

    pairs = q_cols // (2 * HD)
    for number, landed in small:
        copies.arrived(number, landed)
    for copy in own_parts:
        copy.wait()
    turns = turned(v.in_ctx, all_ctx), turned(v.in_one, all_one)

    def one_pair(k):
        @pl.when(k <= pairs)
        def _():
            head_pair(k - 1)

    @pl.loop(1, R)
    def _(k):
        for a in (0, 1):
            ring.sum_step(a, k)
        one_pair(k)
        for work in turns:
            do(work, k, R - 1)

    if pairs > R - 1:

        @pl.loop(R - 1, pairs)
        def _(u):
            head_pair(u)

    for j in range(kv_cols // (2 * HD)):
        both = []
        for sums in (sum_k, sum_v):
            one, two = sums[2 * j], sums[2 * j + 1]
            one, two = one + pltpu.roll(one, HD, 1), two + pltpu.roll(two, HD, 1)
            both.append(jnp.where(front, one, two))
        at = q_cols + j * 2 * HD
        all_gq[0:tok, at : at + 2 * HD] = turn_back(both[0]).astype(bf16)
        at += kv_cols
        all_gq[0:tok, at : at + 2 * HD] = both[1].astype(bf16)
    near_gq = copies.start(block(all_gq, 0), block(all_gq, 1), core_dev)
    row_gq = copies.start(block(all_gq, 0), block(all_gq, 2), row_dev)
    row_gu.append(row_piece(3))

    copies.arrived(near_gh, block(all_gh, 1))
    copies.arrived(row_gh, block(all_gh, 2))
    far_gh = copies.start(block(all_gh, 2), block(all_gh, 3), core_dev)
    copies.arrived(far_gh, block(all_gh, 3))
    tile = q_tiles.shape[1]

    def q_tile(i):
        source = rows_of(h.w_qkv, i * tile, tile)
        at = lax.rem(i, 2)
        return pltpu.make_async_copy(source, q_tiles.at[at], v.tiled.at[at])

    tiles = width // tile
    q_tile(0).start()

    def grad_one(i):
        q_tile(i).wait()

        @pl.when(i + 1 < tiles)
        def _():
            q_tile(i + 1).start()

        hid[:, pl.ds(pl.multiple_of(i * tile, 128), tile)] = matmul_nt(
            block(all_gq, 0)[...], q_tiles[lax.rem(i, 2)]
        )

    load_w = load(h.w_down, weights)

    def before_qkv():
        copies.arrived(near_gq, block(all_gq, 1))
        copies.arrived(row_gq, block(all_gq, 2))
        far_gq = copies.start(block(all_gq, 2), block(all_gq, 3), core_dev)
        copies.arrived(far_gq, block(all_gq, 3))
        do_all(product(all_one, all_gq, chunk[5]))

    spread_phase(
        (0, 1),
        ((tiles, grad_one), product(all_ctx, all_gh, chunk[4])),
        before_qkv,
        (4, 5),
    )

    def residual_one(i):
        b = at_rows(i)
        one, x = hid[b], x_in[b].astype(f32)
        inv = lax.rsqrt(jnp.mean(x * x, axis=1, keepdims=True) + epsilon)
        gain_part[0] += fold(one * x * inv)
        scaled = one * gain[0:1]
        dot = jnp.mean(scaled * x, axis=1, keepdims=True)
        o.tokens[b] = (grad_hid[b] + inv * (scaled - x * inv * inv * dot)).astype(bf16)

    sum_phase((4, 5), ((tok // step, residual_one),))
    load_hid = load(h.hid, hid)

    gain_own, gain_in, gain_all = v.gain_own, v.gain_in, v.gain_all
    for i in (0, 1):
        gain_own[i : i + 1] = jnp.sum(gain_part[i], axis=0, keepdims=True)

    def gain_slice(shard):
        return gain_own.at[:, pl.ds(pl.multiple_of(shard * rows, 128), rows)]

    gains_in = [
        copies.start(gain_slice(shard_of[j]), gain_in.at[j], device)
        for j, device in ((1, core_dev), (2, row_dev), (3, diag_dev))
    ]

    for i, number in enumerate(row_gu):
        copies.arrived(number, gu_row.at[pl.ds(i * quarter, quarter)])
    diag_gu = copies.start(gu_row, gu_near, core_dev)
    copies.arrived(diag_gu, gu_near)
    spread_phase(
        (4, 5),
        (product(v.near_t, gu_row, chunk[2], True), product(v.near_t, gu_near, chunk[3], True)),
        following=(2, 3),
    )

    for j, number in enumerate(gains_in):
        copies.arrived(number, gain_in.at[j + 1])
    gain_all[r] = gain_slice(s)[...] + gain_in[1] + (gain_in[2] + gain_in[3])

    def gain_copy(d):
        return pltpu.make_async_remote_copy(
            src_ref=gain_all.at[r],
            dst_ref=gain_all.at[r],
            send_sem=v.gain_send.at[d],
            recv_sem=v.gain_recv.at[d],
            device_id=(lax.rem(r + d, R), s),
            device_id_type=pl.DeviceIdType.MESH,
        )

    @pl.loop(1, R)
    def _(d):
        gain_copy(d).start()

    copies.finish()
    act = gu_row.at[:, pl.ds(0, ff)]
    load(h.act, act).wait()
    load_w.wait()
    load_hid.wait()
    sum_phase((2, 3), (product(act, weights, gu_own),))
    half = 2 * tok
    core_b = copies.start(rows_of(gu_own, half + (1 - c) * tok, tok), got_b, core_dev)
    core_a = copies.start(rows_of(gu_own, (1 - c) * tok, tok), got_a, core_dev)
    copies.arrived(core_b, got_b)
    mine_b[...] = (
        rows_of(gu_own, half + c * tok, tok)[...].astype(f32) + got_b[...].astype(f32)
    ).astype(bf16)
    far = copies.start(mine_b, got_far, row_dev)

    def last():
        copies.arrived(core_a, got_a)
        copies.arrived(far, got_far)

        @pl.loop(0, tok // step)
        def _(i):
            b = at_rows(i)
            own = rows_of(gu_own, c * tok + i * step, step)[...].astype(f32)
            out = hid[b] + own + got_a[b].astype(f32) + got_far[b].astype(f32)
            o.out[b] = out.astype(bf16)

        @pl.loop(1, R)
        def _(d):
            source = lax.rem(r + R - d, R)
            landed = gain_all.at[source]
            pltpu.make_async_copy(landed, landed, v.gain_recv.at[d]).wait()
            gain_copy(d).wait_send()

        total = gain_all[0]
        for q in range(1, R):
            total = total + gain_all[q]
        o.gains[...] = total

    spread_phase((2, 3), before=last)
    copies.finish()


def backward(R, **given):
    h = types.SimpleNamespace(**given)
    tok, width = h.x.shape
    gu = h.gu.shape
    tokens, S = gu[0], gu[0] // tok
    rows, head_rows = width // S, h.w_o.shape[0] // S
    qkv_cols = h.w_qkv.shape[1]
    half_d = h.down.shape[0] // 2
    down = h.down.shape
    assert half_d >= rows and down[1] >= qkv_cols and gu == (tokens, width), "unsupported sizes"
    slot = slice_shape((max(rows, half_d), width // 2), R)[:2]
    full = (rows, S * gu[1] // 2)
    V = lambda shape, dtype=bf16: pltpu.VMEM(shape, dtype)
    dma = pltpu.SemaphoreType.DMA
    outs = dict(
        gate=(full, bf16, False),
        up=(full, bf16, False),
        o=((head_rows, width), bf16, False),
        qkv=((rows, qkv_cols), bf16, False),
        down=(down, bf16, False),
        tokens=((tok, width), bf16, True),
        out=((tok, width), bf16, True),
        gains=((2, rows), f32, True),
    )
    same = lambda a: V(a.shape, a.dtype)
    scratch = dict(
        down=same(h.down),
        set_one=V((2, rows, width)),
        slots_a=V((2, 2, R - 1) + slot),
        slots_b=V((2, 2, R - 1) + slot),
        gu_own=V(gu),
        gu_near=V(gu),
        gu_row=V(gu),
        near_t=V((rows, tokens)),
        in_ctx=V((tokens, head_rows)),
        in_one=V((tokens, rows)),
        all_gh=V((tokens, width)),
        all_gq=V((tokens, qkv_cols)),
        all_ctx=V((head_rows, tokens)),
        all_one=V((rows, tokens)),
        mine_a=V((tok, width)),
        mine_b=V((tok, width)),
        got_a=V((tok, width)),
        got_b=V((tok, width)),
        got_far=V((tok, width)),
        hid=V((tok, width), f32),
        x_in=V((tok, width)),
        cot=V((tok, width)),
        grad_hid=V((tok, width), f32),
        weights=V(h.w_o.shape),
        w_tiles=V((2, 256, gu[1])),
        gain=same(h.gain),
        q=same(h.q),
        k=same(h.k),
        v=same(h.v),
        ctx=same(h.ctx),
        mask=same(h.mask),
        cos=same(h.cos),
        sin=same(h.sin),
        sum_k=V(h.k.shape, f32),
        sum_v=V(h.k.shape, f32),
        gain_part=V((2, 8, width), f32),
        gain_own=V((2, width), f32),
        gain_in=V((S, 2, rows), f32),
        gain_all=V((R, 2, rows), f32),
        sums=dma((8, 2, R - 1)),
        spread=dma((8, 2, R - 1)),
        sent=dma((8, 2, 2)),
        kept=dma((8, 2)),
        send=dma((32,)),
        recv=dma((32,)),
        loaded=dma((32,)),
        tiled=dma((2,)),
        w_tiled=dma((2,)),
        gain_send=dma((R,)),
        gain_recv=dma((R,)),
    )
    keys = tuple(given), tuple(outs), tuple(scratch)
    return pl.pallas_call(
        functools.partial(backward_kernel, R, keys),
        out_shape=[jax.ShapeDtypeStruct(shape, dtype) for shape, dtype, _ in outs.values()],
        in_specs=[pl.BlockSpec(memory_space=pl.ANY)] * len(given),
        out_specs=[
            pl.BlockSpec(memory_space=pltpu.VMEM if near else pl.ANY) for *_, near in outs.values()
        ],
        scratch_shapes=list(scratch.values()),
        compiler_params=pltpu.CompilerParams(
            collective_id=2, has_side_effects=True, vmem_limit_bytes=67043328
        ),
        name="backward",
    )(*given.values())


def widen_kernel(splits, *refs):
    count = len(splits)
    outs = iter(refs[count:])
    for ref, widths in zip(refs, splits):
        at = 0
        for width in widths:
            out = next(outs)
            out[...] = ref[:, at : at + width].astype(out.dtype)
            at += width


def widen(arrays, steps=4):
    in_specs, out_specs, out_shape = [], [], []
    for arr, widths, dtype in arrays:
        h = arr.shape[0] // steps
        in_specs.append(pl.BlockSpec((h, arr.shape[1]), lambda i: (i, 0)))
        for width in widths:
            out_specs.append(pl.BlockSpec((h, width), lambda i: (i, 0)))
            out_shape.append(jax.ShapeDtypeStruct((arr.shape[0], width), dtype))
    return pl.pallas_call(
        functools.partial(widen_kernel, [widths for _, widths, _ in arrays]),
        grid=(steps,),
        in_specs=in_specs,
        out_specs=out_specs,
        out_shape=out_shape,
        name="widen",
    )(*[arr for arr, *_ in arrays])


def per_device(
    R,
    S,
    tokens_in,
    cotangent,
    segment_ids,
    attn_gain,
    w_query,
    w_key,
    w_value,
    w_output,
    mlp_gain,
    w_gate,
    w_up,
    w_down,
):
    batches, length, width = tokens_in.shape
    tokens = batches * length
    assert batches == 1, "unsupported sizes"
    q_cols, kv_cols = w_query.shape[1], w_key.shape[1]
    x = tokens_in.reshape(tokens, width)
    cot = cotangent.reshape(tokens, width)
    f = forward(
        S,
        x=x,
        cot=cot,
        gain_one=attn_gain[None],
        gain_two=mlp_gain[None],
        w_q=w_query,
        w_k=w_key,
        w_v=w_value,
        w_o=w_output,
        w_gate=w_gate,
        w_up=w_up,
        w_down=w_down,
        segments=segment_ids,
    )
    out = backward(
        R,
        down=f.down,
        w_gu=f.w_gu,
        gu=f.gu,
        two=f.two,
        hid=f.hid,
        x=x,
        cot=cot,
        gain=f.gain,
        w_o=f.w_o,
        w_down=w_down,
        w_qkv=f.w_qkv,
        act=f.act,
        q=f.q,
        k=f.k,
        v=f.v,
        ctx=f.ctx,
        mask=f.mask,
        cos=f.cos,
        sin=f.sin,
        one=f.one,
    )
    gate, up, o, qkv, down, grad_tokens, tokens_out, gains = out
    full = gate.shape[1]
    gate, up, o, *qkv, down, grad_tokens, tokens_out = widen(
        [
            (gate, (full,), f32),
            (up, (full,), f32),
            (o, (width,), f32),
            (qkv, (q_cols, kv_cols, kv_cols), f32),
            (down, (width,), f32),
            (grad_tokens, (width,), bf16),
            (tokens_out, (width,), bf16),
        ]
    )
    return (
        tokens_out.reshape(tokens_in.shape),
        grad_tokens.reshape(tokens_in.shape),
        gains[0],
        *qkv,
        o,
        gains[1],
        gate,
        up,
        down,
    )


def solution(mesh):
    R, S = mesh.shape["replica"], mesh.shape["shard"]
    assert S == 4 and R % 4 == 0, "unsupported mesh"
    data = P(AXES, None, None)
    rowwise = P("shard", None)
    flat = P("shard")
    return jax.shard_map(
        functools.partial(per_device, R, S),
        mesh=mesh,
        in_specs=((data, data, P(AXES, None), flat) + (rowwise,) * 4 + (flat,) + (rowwise,) * 3),
        out_specs=(data, data, flat) + (rowwise,) * 4 + (flat,) + (rowwise,) * 3,
        check_vma=False,
    )
```

```python
import functools
import math
import types

import jax
import jax.numpy as jnp
from jax import lax
from jax.experimental import pallas as pl
from jax.experimental.pallas import tpu as pltpu
from jax.sharding import PartitionSpec as P

KV = 4
HD = 64

epsilon = 1e-05
theta_base = 500000.0
neg_large = -1e30


AXES = ("replica", "shard")
f32 = jnp.float32
bf16 = jnp.bfloat16


def matmul(left_arr, right_arr):
    return jnp.dot(left_arr, right_arr, preferred_element_type=f32)


def matmul_nt(left_arr, right_arr):
    return lax.dot_general(
        left_arr, right_arr, (((1,), (1,)), ((), ())), preferred_element_type=f32
    )


def matmul_tn(left_arr, right_arr):
    return lax.dot_general(
        left_arr, right_arr, (((0,), (0,)), ((), ())), preferred_element_type=f32
    )


class Copies:
    def __init__(self, send, recv):
        self.send, self.recv, self.count, self.open = send, recv, 0, {}

    def start(self, src, dst, device):
        copy = pltpu.make_async_remote_copy(
            src_ref=src,
            dst_ref=dst,
            send_sem=self.send.at[self.count],
            recv_sem=self.recv.at[self.count],
            device_id=device,
            device_id_type=pl.DeviceIdType.MESH,
        )
        self.count += 1
        copy.start()
        self.open[self.count - 1] = copy
        return self.count - 1

    def sent(self, number):
        self.open.pop(number).wait_send()

    def arrived(self, number, landed):
        pltpu.make_async_copy(landed, landed, self.recv.at[number]).wait()

    def finish(self):
        for number in tuple(self.open):
            self.sent(number)


def meet(devices):
    barrier = pltpu.get_barrier_semaphore()
    for device in devices:
        pl.semaphore_signal(
            barrier, inc=1, device_id=device, device_id_type=pl.DeviceIdType.MESH
        )
    pl.semaphore_wait(barrier, len(devices))


def forward_kernel(keys, *refs):
    given = iter(refs)
    h, o, v = (types.SimpleNamespace(**{key: next(given) for key in group}) for group in keys)
    r, s = lax.axis_index("replica"), lax.axis_index("shard")
    c, y = lax.rem(s, 2), lax.div(s, 2)
    x = lax.rem(r, 2)
    w = lax.rem(lax.div(r, 2), 2)
    near, row = 2 * y + 1 - c, 2 * (1 - y) + c
    diagonal = 2 * (1 - y) + 1 - c
    core_dev, row_dev, diag_dev = (r, near), (r, row), (r, diagonal)
    x_dev, z_dev = (r + 1 - 2 * x, s), (r + 2 - 4 * w, s)
    copies = Copies(v.send, v.recv)
    loads, saves = [], []

    def move(source, into, kind, sems):
        copy = pltpu.make_async_copy(source, into, sems.at[len(kind)])
        kind.append(copy)
        copy.start()
        return copy

    def load(source, into):
        return move(source, into, loads, v.loaded)

    def save(source, into):
        return move(source, into, saves, v.saved)

    tok, width = h.x.shape
    ff = v.all_gu.shape[1] // 2
    q_cols, kv_cols = v.q.shape[1], v.all_kv.shape[1] // 2
    m_g = h.w_gate.shape[0]
    q_g = m_g // 4

    def rows_of(ref, start, size):
        return ref.at[pl.ds(pl.multiple_of(start, 16), size)]

    def columns_of(ref, start, size, shard):
        return ref.at[
            pl.ds(pl.multiple_of(start, 16), size), pl.ds(pl.multiple_of(shard * ff, 128), ff)
        ]

    def quarter(flip_x, flip_z):
        at_x = (1 - x) if flip_x else x
        at_z = (1 - w) if flip_z else w
        return 2 * at_z + at_x

    here = quarter(0, 0)

    def gu_part(owner, start, size):
        return [
            v.all_gu.at[pl.ds(pl.multiple_of(owner * m_g + start, 16), size), pl.ds(k * ff, ff)]
            for k in (0, 1)
        ]

    load_x = load(h.x, v.x_in)
    gains = [(h.gain_one, v.gain_one), (h.gain_two, v.gain_two)]

    def gain_at(ref, shard):
        return ref.at[:, pl.ds(pl.multiple_of(shard * m_g, 128), m_g)]

    load_gain = [load(a, gain_at(b, s)) for a, b in gains]
    keys, values = (v.all_kv.at[:, pl.ds(k * kv_cols, kv_cols)] for k in (0, 1))
    plain = [(h.w_q, v.all_q, True), (h.w_k, keys, False), (h.w_v, values, False), (h.w_o, v.all_o, False)]
    load_own = [load(a, rows_of(b, s * a.shape[0], a.shape[0])) for a, b, _ in plain]
    load_small = [load(h.segments, v.segments)]
    own_cot = rows_of(v.all_cot, c * tok, tok)
    load_gu = [
        load(columns_of(a, 0, m_g, s), part)
        for a, part in zip((h.w_gate, h.w_up), gu_part(s, 0, m_g))
    ]
    load_gu += [load(h.cot, own_cot), load(h.w_down, v.w_down)]

    meet([core_dev, row_dev, diag_dev, x_dev, z_dev])

    gain_parts = []
    for device, owner in ((core_dev, near), (row_dev, row), (diag_dev, diagonal)):
        for a, b in gains:
            gain_parts.append((copies.start(a, gain_at(b, s), device), gain_at(b, owner)))

    flows, first = [], []
    for a, b, x_first in plain:
        m = a.shape[0]
        part = rows_of(a, here * (m // 4), m // 4)
        region = functools.partial(
            lambda b, m, owner, spot: rows_of(b, owner * m + spot * (m // 4), m // 4), b, m
        )
        first.append(copies.start(part, region(s, here), row_dev))
        flows.append((region, row, True, x_first))
    for shard, device in ((row, row_dev), (diagonal, diag_dev)):
        for k, a in enumerate((h.w_gate, h.w_up)):
            region = functools.partial(
                lambda k, owner, spot: v.all_gu.at[
                    pl.ds(pl.multiple_of(owner * m_g + spot * q_g, 16), q_g), pl.ds(k * ff, ff)
                ],
                k,
            )
            part = columns_of(a, here * q_g, q_g, shard)
            first.append(copies.start(part, region(s, here), device))
            flows.append((region, shard, False, k == 0))
    far_cot = rows_of(v.all_cot, 2 * tok + c * tok, tok)
    row_cot = copies.start(h.cot, far_cot, row_dev)

    core_plain = []
    for a, b, _ in plain:
        m = a.shape[0]
        core_plain.append((copies.start(a, rows_of(b, s * m, m), core_dev), rows_of(b, near * m, m)))
    core_gu = [
        (copies.start(columns_of(a, 0, m_g, near), part, core_dev), landed)
        for a, part, landed in zip(
            (h.w_gate, h.w_up), gu_part(s, 0, m_g), gu_part(near, 0, m_g)
        )
    ]
    core_gu.append(
        (copies.start(h.cot, own_cot, core_dev), rows_of(v.all_cot, (1 - c) * tok, tok))
    )

    second, third = {}, {}
    forwarded = {i: [] for i in range(len(flows))}

    def to_core(i, part, spot):
        if flows[i][2]:
            forwarded[i].append((copies.start(part, part, core_dev), spot))

    def stage(i, number):
        region, owner, _, x_first = flows[i]
        flip = (1, 0) if x_first else (0, 1)
        one, two = (x_dev, z_dev) if x_first else (z_dev, x_dev)
        piece, other = region(owner, here), region(owner, quarter(*flip))
        if number == 1:
            copies.arrived(first[i], piece)
            second[i] = copies.start(piece, piece, one)
            to_core(i, piece, (0, 0))
        elif number == 2:
            copies.arrived(second[i], other)
            third[i] = [
                (copies.start(part, part, two), spot)
                for part, spot in ((piece, (0, 0)), (other, flip))
            ]
            to_core(i, other, flip)
        elif number == 3:
            for sent, (fx, fz) in third[i]:
                spot = (fx, 1 - fz) if x_first else (1 - fx, fz)
                part = region(owner, quarter(*spot))
                copies.arrived(sent, part)
                to_core(i, part, spot)
        else:
            for sent, spot in forwarded[i]:
                copies.arrived(sent, region(diagonal, quarter(*spot)))

    step = 32

    def at_rows(i):
        return pl.ds(pl.multiple_of(i * step, step), step)

    def norm(source, which, into):
        @pl.loop(0, tok // step)
        def _(i):
            b = at_rows(i)
            values = source[b].astype(f32)
            inv = lax.rsqrt(jnp.mean(values * values, axis=1, keepdims=True) + epsilon)
            into[b] = (values * inv * v.gain[which : which + 1]).astype(bf16)

    for i in (0, 1, 2):
        stage(i, 1)
    for copy in load_small:
        copy.wait()

    along = jnp.broadcast_to(v.segments[...], (tok, tok))
    query_at = lax.broadcasted_iota(jnp.int32, (tok, tok), 0)
    key_at = lax.broadcasted_iota(jnp.int32, (tok, tok), 1)
    allowed = (along.T == along) & (query_at >= key_at)
    v.mask[...] = jnp.where(allowed, 1.0, 0.0)
    position = jnp.sum(v.mask[...], axis=1, keepdims=True) - 1.0
    lane = lax.broadcasted_iota(jnp.int32, (tok, 2 * HD), 1)
    front = lane < HD
    lower = lax.rem(lane, HD) < HD // 2
    turn_of = lax.rem(lane[0:8], HD // 2).astype(f32) * (2.0 / HD)
    speed = jnp.exp(turn_of * -math.log(theta_base))[0:1]
    angle = position * speed
    v.cos[...] = jnp.cos(angle)
    sine = jnp.sin(angle)
    v.sin[...] = jnp.where(lower, sine, -sine)
    save(v.mask, o.mask)
    save(v.cos, o.cos)
    save(v.sin, o.sin)
    for i, number in ((0, 2), (1, 2), (2, 2), (3, 1), (4, 1)):
        stage(i, number)
    load_x.wait()
    for copy in load_gain:
        copy.wait()
    for sent, landed in gain_parts:
        copies.arrived(sent, landed)
    for i, (_, b) in enumerate(gains):
        v.gain[i : i + 1] = b[...].astype(f32)
    norm(v.x_in, 0, v.one)
    save(v.one, o.one)
    for copy in load_own:
        copy.wait()
    for i, number in ((1, 3), (2, 3), (5, 1), (0, 3), (6, 1), (3, 2), (4, 2), (5, 2)):
        stage(i, number)
    for sent, landed in core_plain:
        copies.arrived(sent, landed)
    for i in (0, 1, 2):
        stage(i, 4)

    def turn(part):
        other = jnp.where(lower, pltpu.roll(part, 2 * HD - HD // 2, 1), pltpu.roll(part, HD // 2, 1))
        return part * v.cos[...] - other * v.sin[...]

    def lanes_of(i):
        return pl.ds(pl.multiple_of(i * 2 * HD, 128), 2 * HD)

    @pl.loop(0, q_cols // 256)
    def _(i):
        part = matmul(v.one[...], v.all_q[:, pl.ds(pl.multiple_of(i * 256, 128), 256)])
        for j in (0, 1):
            half = part[:, j * 2 * HD : (j + 1) * 2 * HD]
            v.q[:, lanes_of(2 * i + j)] = turn(half).astype(bf16)

    for which, into in ((0, v.k), (1, v.v)):
        part = matmul(v.one[...], v.all_kv[:, which * kv_cols : (which + 1) * kv_cols])
        for j in range(kv_cols // (2 * HD)):
            half = part[:, j * 2 * HD : (j + 1) * 2 * HD]
            half = turn(half) if which == 0 else half
            swapped = pltpu.roll(half, HD, 1)
            into[2 * j] = jnp.where(front, half, swapped).astype(bf16)
            into[2 * j + 1] = jnp.where(front, swapped, half).astype(bf16)
    save(v.q, o.q)
    save(v.k, o.k)
    save(v.v, o.v)
    save(v.all_q, o.w_qkv.at[:, pl.ds(0, q_cols)])
    save(v.all_kv, o.w_qkv.at[:, pl.ds(q_cols, 2 * kv_cols)])
    stage(7, 1)

    group = q_cols // kv_cols
    scaling = 1.0 / math.sqrt(HD)

    def head_pair(u):
        kv = lax.div(2 * u, group)
        query, keys, values = v.q[:, lanes_of(u)], v.k[kv], v.v[kv]
        allowed = v.mask[...] > 0
        zero = jnp.zeros_like(query)
        context = jnp.zeros((tok, 2 * HD), f32)
        for e in (0, 1):
            own = front if e == 0 else jnp.logical_not(front)
            scores = jnp.where(
                allowed, matmul_nt(jnp.where(own, query, zero), keys) * scaling, neg_large
            )
            top = jnp.max(scores, axis=1, keepdims=True)
            weight = jnp.exp(scores - top)
            probs = (weight / jnp.sum(weight, axis=1, keepdims=True)).astype(bf16)
            context += matmul(probs, jnp.where(own, values, zero))
        v.ctx[:, lanes_of(u)] = context.astype(bf16)

    pairs = q_cols // (2 * HD)

    @pl.loop(0, pairs // 2)
    def _(u):
        head_pair(u)

    stage(6, 2)

    @pl.loop(pairs // 2, pairs)
    def _(u):
        head_pair(u)

    save(v.ctx, o.ctx)
    stage(3, 3)
    stage(3, 4)
    save(v.all_o, o.w_o)

    @pl.loop(0, width // 256)
    def _(i):
        columns = pl.ds(pl.multiple_of(i * 256, 128), 256)
        v.hid[:, columns] = v.x_in[:, columns].astype(f32) + matmul(v.ctx[...], v.all_o[:, columns])

    own_two = rows_of(v.two, c * tok, tok)
    norm(v.hid, 1, own_two)
    far_two = rows_of(v.two, 2 * tok + c * tok, tok)
    near_two = copies.start(own_two, own_two, core_dev)
    row_two = copies.start(own_two, far_two, row_dev)
    stage(7, 2)
    save(v.hid, o.hid)
    save(v.gain, o.gain)

    for copy in load_gu:
        copy.wait()
    for sent, landed in core_gu:
        copies.arrived(sent, landed)
    copies.arrived(near_two, rows_of(v.two, (1 - c) * tok, tok))

    half = 2 * m_g
    early = pl.ds(pl.multiple_of(y * half, 128), half)
    late = pl.ds(pl.multiple_of((1 - y) * half, 128), half)
    low, high = pl.ds(0, 2 * tok), pl.ds(2 * tok, 2 * tok)

    @pl.loop(0, 2 * ff // 256)
    def _(i):
        columns = pl.ds(pl.multiple_of(i * 256, 128), 256)
        v.sums[low, columns] = matmul(v.two[low, early], v.all_gu[early, columns])

    def grads_act(tokens, into):
        @pl.loop(0, ff // 256)
        def _(i):
            columns = pl.ds(pl.multiple_of(i * 256, 128), 256)
            into[:, columns] = matmul_nt(v.all_cot[tokens], v.w_down[columns])

    copies.arrived(row_cot, far_cot)
    last_cot = copies.start(far_cot, far_cot, core_dev)
    act_low, act_high = v.sums.at[high, pl.ds(0, ff)], v.grad_act
    grads_act(low, act_low)
    there = 2 * tok + (1 - c) * tok
    copies.arrived(last_cot, rows_of(v.all_cot, there, tok))
    grads_act(high, act_high)
    for i in (5, 4, 7, 6):
        stage(i, 3)
    save(v.all_gu, o.w_gu)

    def units(end):
        tokens = high if end else low

        @pl.loop(0, ff // 256)
        def _(i):
            columns = pl.ds(pl.multiple_of(i * 256, 128), 256)
            ups = pl.ds(pl.multiple_of(ff + i * 256, 128), 256)
            if end:
                gate = matmul(v.two[tokens], v.all_gu[:, columns])
                up = matmul(v.two[tokens], v.all_gu[:, ups])
            else:
                gate = v.sums[low, columns] + matmul(v.two[tokens, late], v.all_gu[late, columns])
                up = v.sums[low, ups] + matmul(v.two[tokens, late], v.all_gu[late, ups])
            grad_act = (act_high if end else act_low)[:, columns]
            sigmoid = jax.nn.sigmoid(gate)
            silu = gate * sigmoid
            v.act[tokens, columns] = (silu * up).astype(bf16)
            v.gu[tokens, columns] = (
                grad_act * up * sigmoid * (1.0 + gate * (1.0 - sigmoid))
            ).astype(bf16)
            v.gu[tokens, ups] = (grad_act * silu).astype(bf16)

    def down(end):
        tokens = pl.ds(end * 2 * tok, 2 * tok)

        @pl.loop(0, ff // 256)
        def _(i):
            units_at = pl.ds(pl.multiple_of(i * 256, 128), 256)
            turned = v.act[tokens, units_at].T

            @pl.loop(0, width // 512)
            def _(j):
                columns = pl.ds(pl.multiple_of(j * 512, 128), 512)
                part = matmul(turned, v.all_cot[tokens, columns])
                if end == 0:
                    v.sums[units_at, columns] = part
                else:
                    v.down[units_at, columns] = (v.sums[units_at, columns] + part).astype(bf16)

    def save_rows(end, *names):
        tokens = pl.ds(end * 2 * tok, 2 * tok)
        for a, b in names:
            save(a.at[tokens], b.at[tokens])

    units(0)
    save_rows(0, (v.act, o.act), (v.gu, o.gu), (v.two, o.two))
    down(0)
    copies.arrived(row_two, far_two)
    last_two = copies.start(far_two, far_two, core_dev)
    copies.arrived(last_two, rows_of(v.two, there, tok))
    units(1)
    save_rows(1, (v.two, o.two), (v.act, o.act), (v.gu, o.gu))
    down(1)
    save(v.down, o.down)
    copies.finish()
    for copy in saves:
        copy.wait()


def forward(S, **given):
    h = types.SimpleNamespace(**given)
    tok, width = h.x.shape
    ff, q_cols, kv_cols = h.w_down.shape[0], h.w_q.shape[1], h.w_k.shape[1]
    V = lambda shape, dtype=bf16: pltpu.VMEM(shape, dtype)
    dma = pltpu.SemaphoreType.DMA
    heads = (kv_cols // HD, tok, 2 * HD)
    many = S * tok
    outs = dict(
        w_qkv=(S * h.w_q.shape[0], q_cols + 2 * kv_cols),
        w_o=(S * h.w_o.shape[0], width),
        w_gu=(S * h.w_gate.shape[0], 2 * ff),
        gain=(2, width),
        one=(tok, width),
        q=(tok, q_cols),
        k=heads,
        v=heads,
        ctx=(tok, q_cols),
        hid=(tok, width),
        two=(many, width),
        act=(many, ff),
        gu=(many, 2 * ff),
        down=(ff, width),
        mask=(tok, tok),
        cos=(tok, 2 * HD),
        sin=(tok, 2 * HD),
    )
    scratch = dict(
        x_in=V((tok, width)),
        gain=V((2, width), f32),
        gain_one=V((1, width)),
        gain_two=V((1, width)),
        all_q=V((S * h.w_q.shape[0], q_cols)),
        all_kv=V((S * h.w_q.shape[0], 2 * kv_cols)),
        all_o=V((S * h.w_o.shape[0], width)),
        all_gu=V((S * h.w_gate.shape[0], 2 * ff)),
        all_cot=V((many, width)),
        w_down=V(h.w_down.shape),
        segments=V(h.segments.shape, h.segments.dtype),
        cos=V((tok, 2 * HD), f32),
        sin=V((tok, 2 * HD), f32),
        mask=V((tok, tok), f32),
        sums=V((ff, width), f32),
        down=V((ff, width)),
        grad_act=V((2 * tok, ff), f32),
        one=V((tok, width)),
        q=V((tok, q_cols)),
        k=V(heads),
        v=V(heads),
        ctx=V((tok, q_cols)),
        hid=V((tok, width), f32),
        two=V((many, width)),
        act=V((many, ff)),
        gu=V((many, 2 * ff)),
        send=dma((80,)),
        recv=dma((80,)),
        loaded=dma((24,)),
        saved=dma((32,)),
    )
    wide = ("hid", "gain", "mask", "cos", "sin")
    out = pl.pallas_call(
        functools.partial(forward_kernel, (tuple(given), tuple(outs), tuple(scratch))),
        out_shape=[
            jax.ShapeDtypeStruct(shape, f32 if name in wide else bf16)
            for name, shape in outs.items()
        ],
        in_specs=[pl.BlockSpec(memory_space=pl.ANY)] * len(given),
        out_specs=[pl.BlockSpec(memory_space=pl.ANY)] * len(outs),
        scratch_shapes=list(scratch.values()),
        compiler_params=pltpu.CompilerParams(
            collective_id=1, has_side_effects=True, vmem_limit_bytes=67043328
        ),
        name="forward",
    )(*given.values())
    return types.SimpleNamespace(**dict(zip(outs, out)))


def slice_shape(shape, parts):
    rows, cols = shape
    down = min(parts, rows // 16)
    across = parts // down
    assert rows % down == 0 and cols % (128 * across) == 0, "unsupported sizes"
    return rows // down, cols // across, across


def halves_of(ref):
    w = ref.shape[1] // 2
    return ref.at[:, pl.ds(0, w)], ref.at[:, pl.ds(w, w)]


class Ring:
    def __init__(self, R, chunks, outs, slots, sums, spread, sent, kept):
        self.R, self.chunks, self.outs, self.slots = R, chunks, outs, slots
        self.sums, self.spread, self.sent, self.kept = sums, spread, sent, kept
        r, self.s = lax.axis_index("replica"), lax.axis_index("shard")
        z, x = lax.div(r, 2), lax.rem(r, 2)
        self.place = z * (1 - x) + (R - 1 - z) * x
        self.peers = [self.replica_at(self.place + 1), self.replica_at(self.place + R - 1)]

    def replica_at(self, place):
        R = self.R
        place = lax.rem(place, R)
        back = lax.div(place, R // 2)
        return (1 - back) * 2 * place + back * (2 * (R - 1 - place) + 1)

    def part(self, halves, way, step):
        R, ref = self.R, halves[way]
        number = lax.rem(self.place + (R - step if way == 0 else step), R)
        h, w, across = slice_shape(ref.shape, R)
        return ref.at[
            pl.ds(pl.multiple_of(lax.div(number, across) * h, 16), h),
            pl.ds(pl.multiple_of(lax.rem(number, across) * w, 128), w),
        ]

    def slot(self, a, way, step):
        h, w, _ = slice_shape(self.chunks[a][0].shape, self.R)
        return self.slots[a].at[way, step, pl.ds(0, h), pl.ds(0, w)]

    def copy(self, a, way, step, src, dst, arrival):
        return pltpu.make_async_remote_copy(
            src_ref=src,
            dst_ref=dst,
            send_sem=self.sent.at[a, way, lax.rem(step, 2)],
            recv_sem=arrival,
            device_id=(self.peers[way], self.s),
            device_id_type=pl.DeviceIdType.MESH,
        )

    def start(self, a):
        for way in (0, 1):
            src = self.part(self.chunks[a], way, 0)
            self.copy(a, way, 0, src, self.slot(a, way, 0), self.sums.at[a, way, 0]).start()

    def sum_step(self, a, k):
        last = k == self.R - 1
        for way in (0, 1):
            slot = self.slot(a, way, k - 1)
            self.copy(a, way, 0, slot, slot, self.sums.at[a, way, k - 1]).wait_recv()
            own = self.part(self.chunks[a], way, k)
            slot[...] = (slot[...].astype(f32) + own[...].astype(f32)).astype(bf16)
            dst = self.part(self.outs[a], way, k)
            onward = self.copy(a, way, k, slot, dst, self.spread.at[a, way, 0])

            @pl.when(k >= 2)
            def _():
                self.copy(a, way, k, slot, slot, self.sums.at[a, way, 0]).wait_send()

            @pl.when(last)
            def _():
                onward.start()
                pltpu.make_async_copy(slot, dst, self.kept.at[a, way]).start()

            @pl.when(jnp.logical_not(last))
            def _():
                there = lax.rem(k, self.R - 1)
                self.copy(
                    a, way, k, slot, self.slot(a, way, there), self.sums.at[a, way, there]
                ).start()

    def spread_step(self, a, k, last=False):
        for way in (0, 1):
            dst = self.part(self.outs[a], way, lax.rem(k + self.R - 1, self.R))
            self.copy(a, way, 0, dst, dst, self.spread.at[a, way, k - 1]).wait_recv()
            if not last:
                onward = self.copy(a, way, k + self.R - 1, dst, dst, self.spread.at[a, way, k])
                onward.wait_send()
                onward.start()

    def finish(self, a):
        for way in (0, 1):
            slot = self.slot(a, way, self.R - 2)
            for step in (0, 1):
                self.copy(a, way, step, slot, slot, self.sums.at[a, way, 0]).wait_send()
            dst = self.part(self.outs[a], way, self.R - 1)
            pltpu.make_async_copy(slot, dst, self.kept.at[a, way]).wait()


def product(left, right, out, crossed=False, tile=256):
    half = right.shape[0] // 2

    def make(i):
        columns = pl.ds(pl.multiple_of(i * tile, 128), tile)
        if crossed:
            one = matmul(left[:, 0:half], right[pl.ds(half, half), columns])
            out[:, columns] = (one + matmul(left[:, half:], right[pl.ds(0, half), columns])).astype(bf16)
        else:
            out[:, columns] = matmul(left[...], right[:, columns]).astype(bf16)

    return out.shape[1] // tile, make


def backward_kernel(R, keys, *refs):
    given = iter(refs)
    h, o, v = (types.SimpleNamespace(**{key: next(given) for key in group}) for group in keys)
    r, s = lax.axis_index("replica"), lax.axis_index("shard")
    c, y = lax.rem(s, 2), lax.div(s, 2)
    near, row = 2 * y + 1 - c, 2 * (1 - y) + c
    diagonal = 2 * (1 - y) + 1 - c
    shard_of = (s, near, row, diagonal)
    core_dev, row_dev, diag_dev = (r, near), (r, row), (r, diagonal)

    barrier = pltpu.get_barrier_semaphore()
    for other in (near, row, diagonal):
        pl.semaphore_signal(
            barrier, inc=1, device_id=(r, other), device_id_type=pl.DeviceIdType.MESH
        )

    @pl.loop(1, R)
    def _(d):
        pl.semaphore_signal(
            barrier, inc=1, device_id=(lax.rem(r + d, R), s), device_id_type=pl.DeviceIdType.MESH
        )

    loads = []

    def load(source, into):
        copy = pltpu.make_async_copy(source, into, v.loaded.at[len(loads)])
        loads.append(copy)
        copy.start()
        return copy

    down, set_one, slots_a, slots_b = v.down, v.set_one, v.slots_a, v.slots_b
    gu_own, gu_near, gu_row = v.gu_own, v.gu_near, v.gu_row
    all_gh, all_gq, all_ctx, all_one = v.all_gh, v.all_gq, v.all_ctx, v.all_one
    mine_a, mine_b, got_a, got_b, got_far = v.mine_a, v.mine_b, v.got_a, v.got_b, v.got_far
    hid, x_in, cot, grad_hid = v.hid, v.x_in, v.cot, v.grad_hid
    weights = v.weights
    q_tiles = v.w_tiles.at[:, :, pl.ds(0, v.all_gq.shape[1])]
    tok, width = x_in.shape
    ff = gu_own.shape[1] // 2
    rows, head_rows = v.near_t.shape[0], weights.shape[0] // len(shard_of)
    q_cols = v.q.shape[1]
    qkv_cols = all_gq.shape[1]
    kv_cols = (qkv_cols - q_cols) // 2
    half_d = down.shape[0] // 2
    scaling = 1.0 / math.sqrt(HD)

    def rows_of(a, start, size):
        return a.at[pl.ds(pl.multiple_of(start, 16), size)]

    def block(a, j):
        return a.at[pl.ds(j * tok, tok)]

    def columns(a, j, size):
        return a.at[:, pl.ds(pl.multiple_of(j * size, 128), size)]

    load_down = load(h.down, down)
    tokens = gu_own.shape[0]
    load_gu = load(h.gu, gu_own)
    own_two = all_gq.at[:, pl.ds(0, rows)]
    load_near = load(h.two.at[:, pl.ds(pl.multiple_of(s * rows, 128), rows)], own_two)
    later = [
        load(source, into)
        for source, into in ((h.hid, hid), (h.x, x_in), (h.cot, cot), (h.gain, v.gain))
    ]
    load_w = load(h.w_o, weights)
    attention = [
        load(source, into)
        for source, into in (
            (h.q, v.q), (h.k, v.k), (h.v, v.v), (h.ctx, v.ctx),
            (h.mask, v.mask), (h.cos, v.cos), (h.sin, v.sin),
        )
    ]

    units = [pl.ds(pl.multiple_of(shard_of[j] * ff, 128), ff) for j in range(4)]
    outs = [(o.gate.at[:, cols], o.up.at[:, cols]) for cols in units]
    outs += [halves_of(o.o), halves_of(o.qkv)]
    outs += [halves_of(rows_of(o.down, k * half_d, half_d)) for k in (0, 1)]
    chunk = [set_one.at[0], set_one.at[1], set_one.at[0], set_one.at[1]]
    chunk += [down.at[pl.ds(0, head_rows)], down.at[pl.ds(half_d, rows), pl.ds(0, qkv_cols)]]
    chunk += [down.at[pl.ds(0, half_d)], down.at[pl.ds(half_d, half_d)]]
    def parts_of(whole):
        h = whole.shape[0] // 2
        return [whole.at[pl.ds(k * h, h)] for k in (0, 1)]

    slots = [slots_b.at[0], slots_b.at[1]] * 2 + [slots_a.at[0], slots_a.at[1]] * 2
    ring = Ring(
        R,
        [halves_of(part) for a in chunk for part in parts_of(a)],
        [both for one, two in outs for both in zip(parts_of(one), parts_of(two))],
        [slot.at[k] for slot in slots for k in (0, 1)],
        v.sums, v.spread, v.sent, v.kept,
    )

    def parts(pair):
        return [2 * a + k for a in pair for k in (0, 1)]

    copies = Copies(v.send, v.recv)

    def do(work, k, steps):
        count, make = work
        each = -(-count // steps)

        @pl.loop(0, each)
        def _(j):
            i = (k - 1) * each + j

            @pl.when(i < count)
            def _():
                make(i)

    def do_all(work):
        count, make = work

        @pl.loop(0, count)
        def _(i):
            make(i)

    def sum_phase(pair, works=()):
        pair = parts(pair)

        @pl.loop(1, R)
        def _(k):
            for a in pair:
                ring.sum_step(a, k)
            for work in works:
                do(work, k, R - 1)

    def spread_phase(pair, works=(), before=lambda: None, following=()):
        pair, following = parts(pair), parts(following)

        @pl.loop(1, R - 1)
        def _(k):
            for a in pair:
                ring.spread_step(a, k)
            for work in works:
                do(work, k, R - 2)

        before()
        for a in following:
            ring.start(a)
        for a in pair:
            ring.spread_step(a, R - 1, last=True)
            ring.finish(a)

    def turned(source, into):
        def make(i):
            at = pl.ds(pl.multiple_of(i * 128, 128), 128)
            into[:, at] = source[at].T

        return source.shape[0] // 128, make

    load_down.wait()
    pl.semaphore_wait(barrier, R + 2)
    for a in parts((6, 7)):
        ring.start(a)

    load_near.wait()
    do_all(turned(own_two, v.near_t))
    load_gu.wait()
    core_gu = copies.start(gu_own, gu_near, core_dev)
    small = []
    for j, device in ((2, row_dev), (3, diag_dev), (1, core_dev)):
        for whole, into, size in ((h.ctx, v.in_ctx, head_rows), (h.one, v.in_one, rows)):
            source = columns(whole, shard_of[j], size)
            small.append((copies.start(source, block(into, j), device), block(into, j)))
    quarter = gu_own.shape[0] // 4

    def row_piece(i):
        at = pl.ds(i * quarter, quarter)
        return copies.start(gu_own.at[at], gu_row.at[at], row_dev)

    row_gu = [row_piece(0)]
    own_parts = [
        load(columns(h.ctx, s, head_rows), block(v.in_ctx, 0)),
        load(columns(h.one, s, rows), block(v.in_one, 0)),
    ]

    w_tiles = v.w_tiles
    w_tile = w_tiles.shape[1]

    def gu_tile(i):
        at = lax.rem(i, 2)
        return pltpu.make_async_copy(rows_of(h.w_gu, i * w_tile, w_tile), w_tiles.at[at], v.w_tiled.at[at])

    def grad_two(i):
        gu_tile(i).wait()

        @pl.when(i + 1 < width // w_tile)
        def _():
            gu_tile(i + 1).start()

        part = matmul_nt(gu_own[...], w_tiles[lax.rem(i, 2)]).astype(bf16)
        at = pl.ds(pl.multiple_of(i * w_tile, 128), w_tile)
        set_one[0, :, at] = part[: 2 * tok]
        set_one[1, :, at] = part[2 * tok :]

    gu_tile(0).start()
    sum_phase((6, 7), ((width // w_tile, grad_two),))

    core_b = copies.start(rows_of(set_one.at[1], (1 - c) * tok, tok), got_b, core_dev)
    core_a = copies.start(rows_of(set_one.at[0], (1 - c) * tok, tok), got_a, core_dev)
    mine_a[...] = rows_of(set_one.at[0], c * tok, tok)[...]
    copies.arrived(core_b, got_b)
    own_b = rows_of(set_one.at[1], c * tok, tok)[...]
    mine_b[...] = (own_b.astype(f32) + got_b[...].astype(f32)).astype(bf16)
    far = copies.start(mine_b, got_far, row_dev)
    row_gu.append(row_piece(1))
    copies.sent(core_b)
    copies.sent(core_a)

    for copy in later:
        copy.wait()
    load_w.wait()
    copies.arrived(core_a, got_a)
    copies.arrived(core_gu, gu_near)
    gain, gain_part = v.gain, v.gain_part
    gain_part[...] = jnp.zeros_like(gain_part)
    step = 32
    groups = step // 8

    def fold(values):
        return jnp.sum(values.reshape(groups, 8, width), axis=0)

    def at_rows(i):
        return pl.ds(pl.multiple_of(i * step, step), step)

    def residual_two(i):
        b = at_rows(i)
        two = mine_a[b].astype(f32) + got_a[b].astype(f32) + got_far[b].astype(f32)
        hidden = hid[b]
        inv = lax.rsqrt(jnp.mean(hidden * hidden, axis=1, keepdims=True) + epsilon)
        gain_part[1] += fold(two * hidden * inv)
        scaled = two * gain[1:2]
        dot = jnp.mean(scaled * hidden, axis=1, keepdims=True)
        out = cot[b].astype(f32) + inv * (scaled - hidden * inv * inv * dot)
        grad_hid[b] = out
        all_gh[b] = out.astype(bf16)

    def before_gh():
        copies.arrived(far, got_far)
        do_all((tok // step, residual_two))

    spread_phase(
        (6, 7),
        (product(v.near_t, gu_own, chunk[0]), product(v.near_t, gu_near, chunk[1])),
        before_gh,
        (0, 1),
    )
    near_gh = copies.start(block(all_gh, 0), block(all_gh, 1), core_dev)
    row_gh = copies.start(block(all_gh, 0), block(all_gh, 2), row_dev)
    row_gu.append(row_piece(2))

    for copy in attention:
        copy.wait()
    sum_k, sum_v = v.sum_k, v.sum_v
    sum_k[...] = jnp.zeros_like(sum_k)
    sum_v[...] = jnp.zeros_like(sum_v)
    group = q_cols // kv_cols
    lane = lax.broadcasted_iota(jnp.int32, (tok, 2 * HD), 1)
    front = lane < HD
    lower = lax.rem(lane, HD) < HD // 2

    def turn_back(part):
        other = jnp.where(lower, pltpu.roll(part, 2 * HD - HD // 2, 1), pltpu.roll(part, HD // 2, 1))
        return part * v.cos[...] + other * v.sin[...]

    def head_pair(u):
        lanes = pl.ds(pl.multiple_of(u * 2 * HD, 128), 2 * HD)
        kv = lax.div(2 * u, group)
        grad_ctx = matmul_nt(block(all_gh, 0)[...], weights[pl.ds(pl.multiple_of(u * 2 * HD, 128), 2 * HD)])
        grad_ctx = grad_ctx.astype(bf16)
        query, keys, values = v.q[:, lanes], v.k[kv], v.v[kv]
        shares = grad_ctx.astype(f32) * v.ctx[:, lanes].astype(f32)
        allowed = v.mask[...] > 0
        zero = jnp.zeros_like(query)
        grad_q = jnp.zeros((tok, 2 * HD), f32)
        grad_k = jnp.zeros((tok, 2 * HD), f32)
        grad_v = jnp.zeros((tok, 2 * HD), f32)
        for e in (0, 1):
            own = front if e == 0 else jnp.logical_not(front)
            own_q, own_g = jnp.where(own, query, zero), jnp.where(own, grad_ctx, zero)
            row_dot = jnp.sum(jnp.where(own, shares, 0.0), axis=1, keepdims=True)
            scores = jnp.where(allowed, matmul_nt(own_q, keys) * scaling, neg_large)
            top = jnp.max(scores, axis=1, keepdims=True)
            weight = jnp.exp(scores - top)
            probs = weight / jnp.sum(weight, axis=1, keepdims=True)
            grad_probs = matmul_nt(own_g, values)
            grad_scores = (probs * (grad_probs - row_dot) * scaling).astype(bf16)
            grad_q += matmul(grad_scores, jnp.where(own, keys, zero))
            grad_k += matmul_tn(grad_scores, own_q)
            grad_v += matmul_tn(probs.astype(bf16), own_g)
        all_gq[0:tok, lanes] = turn_back(grad_q).astype(bf16)
        sum_k[kv] += grad_k
        sum_v[kv] += grad_v

    pairs = q_cols // (2 * HD)
    for number, landed in small:
        copies.arrived(number, landed)
    for copy in own_parts:
        copy.wait()
    turns = turned(v.in_ctx, all_ctx), turned(v.in_one, all_one)

    def one_pair(k):
        @pl.when(k <= pairs)
        def _():
            head_pair(k - 1)

    @pl.loop(1, R)
    def _(k):
        for a in parts((0, 1)):
            ring.sum_step(a, k)
        one_pair(k)
        for work in turns:
            do(work, k, R - 1)

    if pairs > R - 1:

        @pl.loop(R - 1, pairs)
        def _(u):
            head_pair(u)

    for j in range(kv_cols // (2 * HD)):
        both = []
        for sums in (sum_k, sum_v):
            one, two = sums[2 * j], sums[2 * j + 1]
            one, two = one + pltpu.roll(one, HD, 1), two + pltpu.roll(two, HD, 1)
            both.append(jnp.where(front, one, two))
        at = q_cols + j * 2 * HD
        all_gq[0:tok, at : at + 2 * HD] = turn_back(both[0]).astype(bf16)
        at += kv_cols
        all_gq[0:tok, at : at + 2 * HD] = both[1].astype(bf16)
    near_gq = copies.start(block(all_gq, 0), block(all_gq, 1), core_dev)
    row_gq = copies.start(block(all_gq, 0), block(all_gq, 2), row_dev)
    row_gu.append(row_piece(3))

    copies.arrived(near_gh, block(all_gh, 1))
    copies.arrived(row_gh, block(all_gh, 2))
    far_gh = copies.start(block(all_gh, 2), block(all_gh, 3), core_dev)
    copies.arrived(far_gh, block(all_gh, 3))
    tile = q_tiles.shape[1]

    def q_tile(i):
        source = rows_of(h.w_qkv, i * tile, tile)
        at = lax.rem(i, 2)
        return pltpu.make_async_copy(source, q_tiles.at[at], v.tiled.at[at])

    tiles = width // tile
    q_tile(0).start()

    def grad_one(i):
        q_tile(i).wait()

        @pl.when(i + 1 < tiles)
        def _():
            q_tile(i + 1).start()

        hid[:, pl.ds(pl.multiple_of(i * tile, 128), tile)] = matmul_nt(
            block(all_gq, 0)[...], q_tiles[lax.rem(i, 2)]
        )

    load_w = load(h.w_down, weights)

    def before_qkv():
        copies.arrived(near_gq, block(all_gq, 1))
        copies.arrived(row_gq, block(all_gq, 2))
        far_gq = copies.start(block(all_gq, 2), block(all_gq, 3), core_dev)
        copies.arrived(far_gq, block(all_gq, 3))
        do_all(product(all_one, all_gq, chunk[5]))

    spread_phase(
        (0, 1),
        ((tiles, grad_one), product(all_ctx, all_gh, chunk[4])),
        before_qkv,
        (4, 5),
    )

    def residual_one(i):
        b = at_rows(i)
        one, x = hid[b], x_in[b].astype(f32)
        inv = lax.rsqrt(jnp.mean(x * x, axis=1, keepdims=True) + epsilon)
        gain_part[0] += fold(one * x * inv)
        scaled = one * gain[0:1]
        dot = jnp.mean(scaled * x, axis=1, keepdims=True)
        o.tokens[b] = (grad_hid[b] + inv * (scaled - x * inv * inv * dot)).astype(bf16)

    sum_phase((4, 5), ((tok // step, residual_one),))
    load_hid = load(h.hid, hid)

    gain_own, gain_in, gain_all = v.gain_own, v.gain_in, v.gain_all
    for i in (0, 1):
        gain_own[i : i + 1] = jnp.sum(gain_part[i], axis=0, keepdims=True)

    def gain_slice(shard):
        return gain_own.at[:, pl.ds(pl.multiple_of(shard * rows, 128), rows)]

    gains_in = [
        copies.start(gain_slice(shard_of[j]), gain_in.at[j], device)
        for j, device in ((1, core_dev), (2, row_dev), (3, diag_dev))
    ]

    for i, number in enumerate(row_gu):
        copies.arrived(number, gu_row.at[pl.ds(i * quarter, quarter)])
    diag_gu = copies.start(gu_row, gu_near, core_dev)
    copies.arrived(diag_gu, gu_near)
    spread_phase(
        (4, 5),
        (product(v.near_t, gu_row, chunk[2], True), product(v.near_t, gu_near, chunk[3], True)),
        following=(2, 3),
    )

    for j, number in enumerate(gains_in):
        copies.arrived(number, gain_in.at[j + 1])
    gain_all[r] = gain_slice(s)[...] + gain_in[1] + (gain_in[2] + gain_in[3])

    def gain_copy(d):
        return pltpu.make_async_remote_copy(
            src_ref=gain_all.at[r],
            dst_ref=gain_all.at[r],
            send_sem=v.gain_send.at[d],
            recv_sem=v.gain_recv.at[d],
            device_id=(lax.rem(r + d, R), s),
            device_id_type=pl.DeviceIdType.MESH,
        )

    @pl.loop(1, R)
    def _(d):
        gain_copy(d).start()

    copies.finish()
    act = gu_row.at[:, pl.ds(0, ff)]
    load(h.act, act).wait()
    load_w.wait()
    load_hid.wait()
    sum_phase((2, 3), (product(act, weights, gu_own),))
    half = 2 * tok
    core_b = copies.start(rows_of(gu_own, half + (1 - c) * tok, tok), got_b, core_dev)
    core_a = copies.start(rows_of(gu_own, (1 - c) * tok, tok), got_a, core_dev)
    copies.arrived(core_b, got_b)
    mine_b[...] = (
        rows_of(gu_own, half + c * tok, tok)[...].astype(f32) + got_b[...].astype(f32)
    ).astype(bf16)
    far = copies.start(mine_b, got_far, row_dev)

    def last():
        copies.arrived(core_a, got_a)
        copies.arrived(far, got_far)

        @pl.loop(0, tok // step)
        def _(i):
            b = at_rows(i)
            own = rows_of(gu_own, c * tok + i * step, step)[...].astype(f32)
            out = hid[b] + own + got_a[b].astype(f32) + got_far[b].astype(f32)
            o.out[b] = out.astype(bf16)

        @pl.loop(1, R)
        def _(d):
            source = lax.rem(r + R - d, R)
            landed = gain_all.at[source]
            pltpu.make_async_copy(landed, landed, v.gain_recv.at[d]).wait()
            gain_copy(d).wait_send()

        total = gain_all[0]
        for q in range(1, R):
            total = total + gain_all[q]
        o.gains[...] = total

    spread_phase((2, 3), before=last)
    copies.finish()


def backward(R, **given):
    h = types.SimpleNamespace(**given)
    tok, width = h.x.shape
    gu = h.gu.shape
    tokens, S = gu[0], gu[0] // tok
    rows, head_rows = width // S, h.w_o.shape[0] // S
    qkv_cols = h.w_qkv.shape[1]
    half_d = h.down.shape[0] // 2
    down = h.down.shape
    assert half_d >= rows and down[1] >= qkv_cols and gu == (tokens, width), "unsupported sizes"
    slot = slice_shape((max(rows, half_d) // 2, width // 2), R)[:2]
    full = (rows, S * gu[1] // 2)
    V = lambda shape, dtype=bf16: pltpu.VMEM(shape, dtype)
    dma = pltpu.SemaphoreType.DMA
    outs = dict(
        gate=(full, bf16, False),
        up=(full, bf16, False),
        o=((head_rows, width), bf16, False),
        qkv=((rows, qkv_cols), bf16, False),
        down=(down, bf16, False),
        tokens=((tok, width), bf16, True),
        out=((tok, width), bf16, True),
        gains=((2, rows), f32, True),
    )
    same = lambda a: V(a.shape, a.dtype)
    scratch = dict(
        down=same(h.down),
        set_one=V((2, rows, width)),
        slots_a=V((2, 2, 2, R - 1) + slot),
        slots_b=V((2, 2, 2, R - 1) + slot),
        gu_own=V(gu),
        gu_near=V(gu),
        gu_row=V(gu),
        near_t=V((rows, tokens)),
        in_ctx=V((tokens, head_rows)),
        in_one=V((tokens, rows)),
        all_gh=V((tokens, width)),
        all_gq=V((tokens, qkv_cols)),
        all_ctx=V((head_rows, tokens)),
        all_one=V((rows, tokens)),
        mine_a=V((tok, width)),
        mine_b=V((tok, width)),
        got_a=V((tok, width)),
        got_b=V((tok, width)),
        got_far=V((tok, width)),
        hid=V((tok, width), f32),
        x_in=V((tok, width)),
        cot=V((tok, width)),
        grad_hid=V((tok, width), f32),
        weights=V(h.w_o.shape),
        w_tiles=V((2, 256, gu[1])),
        gain=same(h.gain),
        q=same(h.q),
        k=same(h.k),
        v=same(h.v),
        ctx=same(h.ctx),
        mask=same(h.mask),
        cos=same(h.cos),
        sin=same(h.sin),
        sum_k=V(h.k.shape, f32),
        sum_v=V(h.k.shape, f32),
        gain_part=V((2, 8, width), f32),
        gain_own=V((2, width), f32),
        gain_in=V((S, 2, rows), f32),
        gain_all=V((R, 2, rows), f32),
        sums=dma((16, 2, R - 1)),
        spread=dma((16, 2, R - 1)),
        sent=dma((16, 2, 2)),
        kept=dma((16, 2)),
        send=dma((32,)),
        recv=dma((32,)),
        loaded=dma((32,)),
        tiled=dma((2,)),
        w_tiled=dma((2,)),
        gain_send=dma((R,)),
        gain_recv=dma((R,)),
    )
    keys = tuple(given), tuple(outs), tuple(scratch)
    return pl.pallas_call(
        functools.partial(backward_kernel, R, keys),
        out_shape=[jax.ShapeDtypeStruct(shape, dtype) for shape, dtype, _ in outs.values()],
        in_specs=[pl.BlockSpec(memory_space=pl.ANY)] * len(given),
        out_specs=[
            pl.BlockSpec(memory_space=pltpu.VMEM if near else pl.ANY) for *_, near in outs.values()
        ],
        scratch_shapes=list(scratch.values()),
        compiler_params=pltpu.CompilerParams(
            collective_id=2, has_side_effects=True, vmem_limit_bytes=67043328
        ),
        name="backward",
    )(*given.values())


def widen_kernel(splits, *refs):
    count = len(splits)
    outs = iter(refs[count:])
    for ref, widths in zip(refs, splits):
        at = 0
        for width in widths:
            out = next(outs)
            out[...] = ref[:, at : at + width].astype(out.dtype)
            at += width


def widen(arrays, steps=4):
    in_specs, out_specs, out_shape = [], [], []
    for arr, widths, dtype in arrays:
        h = arr.shape[0] // steps
        in_specs.append(pl.BlockSpec((h, arr.shape[1]), lambda i: (i, 0)))
        for width in widths:
            out_specs.append(pl.BlockSpec((h, width), lambda i: (i, 0)))
            out_shape.append(jax.ShapeDtypeStruct((arr.shape[0], width), dtype))
    return pl.pallas_call(
        functools.partial(widen_kernel, [widths for _, widths, _ in arrays]),
        grid=(steps,),
        in_specs=in_specs,
        out_specs=out_specs,
        out_shape=out_shape,
        name="widen",
    )(*[arr for arr, *_ in arrays])


def per_device(
    R,
    S,
    tokens_in,
    cotangent,
    segment_ids,
    attn_gain,
    w_query,
    w_key,
    w_value,
    w_output,
    mlp_gain,
    w_gate,
    w_up,
    w_down,
):
    batches, length, width = tokens_in.shape
    tokens = batches * length
    assert batches == 1, "unsupported sizes"
    q_cols, kv_cols = w_query.shape[1], w_key.shape[1]
    x = tokens_in.reshape(tokens, width)
    cot = cotangent.reshape(tokens, width)
    f = forward(
        S,
        x=x,
        cot=cot,
        gain_one=attn_gain[None],
        gain_two=mlp_gain[None],
        w_q=w_query,
        w_k=w_key,
        w_v=w_value,
        w_o=w_output,
        w_gate=w_gate,
        w_up=w_up,
        w_down=w_down,
        segments=segment_ids,
    )
    out = backward(
        R,
        down=f.down,
        w_gu=f.w_gu,
        gu=f.gu,
        two=f.two,
        hid=f.hid,
        x=x,
        cot=cot,
        gain=f.gain,
        w_o=f.w_o,
        w_down=w_down,
        w_qkv=f.w_qkv,
        act=f.act,
        q=f.q,
        k=f.k,
        v=f.v,
        ctx=f.ctx,
        mask=f.mask,
        cos=f.cos,
        sin=f.sin,
        one=f.one,
    )
    gate, up, o, qkv, down, grad_tokens, tokens_out, gains = out
    full = gate.shape[1]
    gate, up, o, *qkv, down, grad_tokens, tokens_out = widen(
        [
            (gate, (full,), f32),
            (up, (full,), f32),
            (o, (width,), f32),
            (qkv, (q_cols, kv_cols, kv_cols), f32),
            (down, (width,), f32),
            (grad_tokens, (width,), bf16),
            (tokens_out, (width,), bf16),
        ]
    )
    return (
        tokens_out.reshape(tokens_in.shape),
        grad_tokens.reshape(tokens_in.shape),
        gains[0],
        *qkv,
        o,
        gains[1],
        gate,
        up,
        down,
    )


def solution(mesh):
    R, S = mesh.shape["replica"], mesh.shape["shard"]
    assert S == 4 and R % 4 == 0, "unsupported mesh"
    data = P(AXES, None, None)
    rowwise = P("shard", None)
    flat = P("shard")
    return jax.shard_map(
        functools.partial(per_device, R, S),
        mesh=mesh,
        in_specs=((data, data, P(AXES, None), flat) + (rowwise,) * 4 + (flat,) + (rowwise,) * 3),
        out_specs=(data, data, flat) + (rowwise,) * 4 + (flat,) + (rowwise,) * 3,
        check_vma=False,
    )
```
